32 devices in a mesh: wa: 16 (over z, y, core), ha: 2 (over x).
Axes of the slice: x: 2, y: 2, z: 4, core: 2. Of those that a mesh axis runs over, the one named last changes fastest.
Arguments:
- tokens: bfloat16 [16384, 4096], P('wa'), may hold values from -6 to 6
- expert_ids: int32 [16384, 8], P('wa'), may hold values from 0 to 127, as said below
- keep_mask: int32 [16384, 8], P('wa'), may hold values from 0 to 1, as said below
- route_weight: float32 [16384, 8], P('wa'), may hold values from 0.2 to 1
- gate_weight: bfloat16 [4096, 1536], P('wa', 'ha'), may hold values from -0.09375 to 0.09375
- up_weight: bfloat16 [4096, 1536], P('wa', 'ha'), may hold values from -0.09375 to 0.09375
- down_weight: bfloat16 [4096, 1536], P('wa', 'ha'), may hold values from -0.15625 to 0.15625
Outputs:
- mixed: bfloat16 [16384, 4096], P('wa', 'ha')
The draws below stay inside these ranges and needn't reach their ends.
Inputs may be any that keep to these rules, and one draw needn't show every extreme that they name: `expert_ids`: each row names 8 different experts. keep_mask[t, k] is 1 exactly where fewer than 128 earlier tokens of the same block of 1024 rows name expert_ids[t, k]; in some block 128 tokens naming expert 0 are kept.
All inputs are finite; a program needn't handle non-finite values.
Results may differ from the reference program's by a relative error of at most 0.005.
Values may be sent and summed in bfloat16 or wider, within the bound.
A program may use at most 128 MiB of HBM per device.

```python
import math
import jax
import jax.numpy as jnp
from jax import lax

D = 4096
HID = 1536
EXPERTS = 128
TOP = 8
TOK_DEV = 1024
CAP = 128
TOKENS = 16384
GLOBAL_CAP = 1024


def routing(key):
    block_count = TOKENS // TOK_DEV
    keys = jax.random.split(jax.random.fold_in(key, 11), 4)
    columns = jnp.arange(EXPERTS, dtype=jnp.int32)
    scores = jax.random.randint(keys[0], (TOKENS, EXPERTS), 0, 65536, dtype=jnp.int32) * EXPERTS + columns[None, :]
    boost_rate = jax.random.randint(keys[1], (block_count,), 1, 9, dtype=jnp.int32)
    forced = jax.random.randint(keys[2], (), 0, block_count, dtype=jnp.int32)
    boost_rate = jnp.where(jnp.arange(block_count, dtype=jnp.int32) == forced, 32, boost_rate)
    coin_flip = jax.random.randint(keys[3], (TOKENS,), 0, 32, dtype=jnp.int32)
    favoured = (coin_flip < jnp.repeat(boost_rate, TOK_DEV)).astype(jnp.int32)
    scores = scores.at[:, 0].add(favoured * 16777216)
    chosen_ids = lax.top_k(scores, TOP)[1].astype(jnp.int32)
    counts = jnp.zeros((TOKENS, EXPERTS), jnp.int32)
    for column in range(TOP):
        counts = counts + (chosen_ids[:, column:column + 1] == columns[None, :]).astype(jnp.int32)
    blocked = counts.reshape(block_count, TOK_DEV, EXPERTS)
    earlier = (jnp.cumsum(blocked, axis=1).astype(jnp.int32) - blocked).reshape(TOKENS, EXPERTS)
    position = jnp.take_along_axis(earlier, chosen_ids, axis=1)
    keeping = (position < CAP).astype(jnp.int32)
    return (chosen_ids, keeping)


def draw_expert_ids(key, part):
    return routing(key)[0]


def draw_keep_mask(key, part):
    return routing(key)[1]


def block_levels(own_key, dims, cuts, low, top_value):
    level, own = 1.0, jax.random.fold_in(own_key, 6)
    for axis_at, blocks in cuts:
        heights = jnp.exp(jax.random.uniform(jax.random.fold_in(own, axis_at), (blocks,), jnp.float32, low / len(cuts), top_value / len(cuts)))
        level = level * jnp.repeat(heights, dims[axis_at] // blocks).reshape([-1 if axis == axis_at else 1 for axis in range(len(dims))])
    return level


def normal_values(own_key, dims, spread, limit, cuts=(), kind=jnp.bfloat16):
    drawn = jax.random.normal(own_key, dims, jnp.float32) * spread
    if len(cuts) > 0:
        drawn = block_levels(own_key, dims, cuts, -0.22, 0.18) * drawn
    return jnp.clip(drawn, min=-limit, max=limit).astype(kind)


def setup_inputs(seed: int = 0) -> dict:
    splits = jax.random.split(jax.random.key(seed), 8)
    tokens = normal_values(splits[0], (TOKENS, D), 1.0, 6.0, ((0, 16),))
    expert_ids = draw_expert_ids(jax.random.fold_in(splits[7], 71), 0)
    keep_mask = draw_keep_mask(jax.random.fold_in(splits[7], 71), 0)
    route_weight = jnp.clip(jnp.exp(math.log(1.0) - 1.609438 * jax.random.uniform(splits[3], (TOKENS, TOP), jnp.float32) ** block_levels(splits[3], (TOKENS, TOP), ((0, 16),), -0.2, 0.2)), 0.2, 1.0)
    gate_weight = normal_values(splits[4], (D, HID), D ** -0.5, 0.09375, ((0, 16), (1, 2)))
    up_weight = normal_values(splits[5], (D, HID), D ** -0.5, 0.09375, ((0, 16), (1, 2)))
    down_weight = normal_values(splits[6], (D, HID), HID ** -0.5, 0.15625, ((0, 16), (1, 2)))
    return dict(tokens=tokens, expert_ids=expert_ids, keep_mask=keep_mask, route_weight=route_weight, gate_weight=gate_weight, up_weight=up_weight, down_weight=down_weight)


def reference(tokens, expert_ids, keep_mask, route_weight, gate_weight, up_weight, down_weight):
    block_count = TOKENS // TOK_DEV
    matches = (expert_ids == 0) & (keep_mask == 1)
    chosen = jnp.any(matches, axis=1).astype(jnp.int32).reshape(block_count, TOK_DEV)
    route_sum = jnp.sum(jnp.where(matches, route_weight, jnp.float32(0.0)), axis=1).astype(jnp.float32)
    route_sum = route_sum.reshape(block_count, TOK_DEV)
    position = (jnp.cumsum(chosen, axis=1).astype(jnp.int32) - chosen).astype(jnp.int32)
    counted = jnp.sum(chosen, axis=1).astype(jnp.int32)
    earlier = (jnp.cumsum(counted).astype(jnp.int32) - counted).astype(jnp.int32)
    admitted = chosen * ((earlier[:, None] + position) < GLOBAL_CAP).astype(jnp.int32)
    slot_ids = jnp.arange(CAP, dtype=jnp.int32)

    def one_block(packed):
        block_rows, block_pos, block_adm, block_route = packed
        dispatch = (block_pos[None, :] == slot_ids[:, None]) & (block_adm[None, :] == 1)
        slot_rows = jnp.dot(dispatch.astype(jnp.bfloat16), block_rows, preferred_element_type=jnp.float32).astype(jnp.bfloat16)
        gate_sum = jnp.dot(slot_rows, gate_weight, preferred_element_type=jnp.float32)
        up_sum = jnp.dot(slot_rows, up_weight, preferred_element_type=jnp.float32)
        hidden = (jax.nn.silu(gate_sum) * up_sum).astype(jnp.bfloat16)
        expert_out = jnp.dot(hidden, down_weight.T, preferred_element_type=jnp.float32)
        combine_map = jnp.where(dispatch.T, block_route[:, None], jnp.float32(0.0)).astype(jnp.float32)
        mixed_block = jnp.dot(combine_map, expert_out, precision=lax.Precision.HIGHEST, preferred_element_type=jnp.float32)
        return mixed_block.astype(jnp.bfloat16)

    mixed = lax.map(one_block, (tokens.reshape(block_count, TOK_DEV, D), position, admitted, route_sum))
    return mixed.reshape(TOKENS, D)
```

```python
import functools

import jax
import jax.numpy as jnp
from jax import lax
from jax.experimental import pallas as pl
from jax.experimental.pallas import tpu as pltpu
from jax.sharding import PartitionSpec as P

CAP = 128
MESH = pl.DeviceIdType.MESH


def expert_kernel(
    n,
    pos_ref, route_ref, tok_ref, gate_ref, up_ref, down_ref,
    y_ref,
    w1, w2, stage, tok_buf, guest_out, own_rows, guest_rows, own_acc, guest_acc, part_out, part_in, hidden,
    x_own, x_out, x_in, y_own, y_out, y_in, xy_own, xy_out, xy_in, yx_out, yx_in, count, counts, route,
    load_sem, tok_sem, c_send, c_recv, e_send, e_recv, l1_send, l1_recv, b1_send, b1_recv,
    l2_send, l2_recv, b2_send, b2_recv, g_send, g_recv, p_send, p_recv,
    x_send, x_recv, y_send, y_recv, xy_send, xy_recv, yx_send, yx_recv,
):
    zs = n // 4
    span = zs // 2
    sub = span // 2
    me = lax.axis_index("wa")
    ha = lax.axis_index("ha")
    core = lax.rem(me, 2)
    y = lax.rem(me // 2, 2)
    z = me // 4
    half = z // span
    zl = z - half * span
    sibling = me + 1 - 2 * core
    beside = me + 2 - 4 * y
    mirror = lax.rem(me + n // 2, n)
    q = hidden.shape[2]
    fd = stage.shape[1]
    group = 4 * fd

    def remote(ref, dst, send, recv, **where):
        return pltpu.make_async_remote_copy(
            src_ref=ref, dst_ref=dst, send_sem=send, recv_sem=recv, device_id=where, device_id_type=MESH
        )

    def same(ref, send, recv, **where):
        return remote(ref, ref, send, recv, **where)

    def order(e, at, size):
        short = jnp.minimum(at, size - 1 - at)
        paired = jnp.where(e % 2 == 1, at + (e + 1) // 2, at - e // 2)
        rest = jnp.where(at < size - 1 - at, at + (e - short), at - (e - short))
        return jnp.where(e <= 2 * short, paired, rest)

    class Line:
        def __init__(self, ref_of, at, size, sems):
            self.ref_of, self.at, self.size = ref_of, at, size
            self.l_send, self.l_recv, self.b_send, self.b_recv = sems

        def hop(self, way, *unit):
            to = me + 4 * (1 - 2 * way)
            return same(self.ref_of(core, *unit), self.l_send.at[(way, *unit)], self.l_recv.at[unit], wa=to)

        def up(self, zi):
            return (zi <= self.at) & (self.at + 1 < self.size)

        def down(self, zi):
            return (zi >= self.at) & (self.at > 0)

        def push(self, t, zi, yy):
            @pl.when(self.up(zi))
            def _():
                self.hop(0, t, zi, yy).start()

            @pl.when(self.down(zi))
            def _():
                self.hop(1, t, zi, yy).start()

        def arrive(self, t, zi, yy):
            self.hop(0, t, zi, yy).wait_recv()

        def give(self, t, zi, yy):
            return same(self.ref_of(core, t, zi, yy), self.b_send.at[t, zi, yy], self.b_recv.at[t, zi, yy], wa=sibling)

        def given(self, t, zi, yy):
            return same(
                self.ref_of(1 - core, t, zi, yy), self.b_send.at[t, zi, yy], self.b_recv.at[t, zi, yy], wa=sibling
            )

        def spread(self, t, zi, yy):
            self.push(t, zi, yy)
            self.give(t, zi, yy).start()

        def serve(self, t, zi, yy):
            self.arrive(t, zi, yy)
            self.spread(t, zi, yy)

        def drain(self, kinds):
            @pl.loop(0, self.size)
            def _(zi):
                for t in kinds:
                    for yy in (0, 1):
                        @pl.when(self.up(zi))
                        def _():
                            self.hop(0, t, zi, yy).wait_send()

                        @pl.when(self.down(zi))
                        def _():
                            self.hop(1, t, zi, yy).wait_send()

                        self.give(t, zi, yy).wait_send()

    first = Line(lambda c, t, zi, yy: w1.at[t, zi, yy, c], zl, span, (l1_send, l1_recv, b1_send, b1_recv))
    second = Line(lambda c, t, zi, yy: w2.at[zi, yy, c], z, zs, (l2_send, l2_recv, b2_send, b2_recv))

    def exchange(t):
        dst, recv = (w2.at[z, y, core], l2_recv.at[0, z, y]) if t == 2 else (w1.at[t, zl, y, core], l1_recv.at[t, zl, y])
        return remote(stage.at[t], dst, e_send.at[t], recv, wa=beside)

    def count_copy(k):
        return remote(count, counts.at[me], c_send.at[k], c_recv.at[k], wa=lax.rem(me + k, n))

    def count_got(k):
        return remote(count, counts.at[lax.rem(me - k + n, n)], c_send.at[k], c_recv.at[k], wa=lax.rem(me + k, n))

    def columns(ref, index):
        return ref.at[:, pl.ds(pl.multiple_of(index * q, 128), q)]

    weights = (gate_ref, up_ref, down_ref)
    homes = (w1.at[0, zl, y, core], w1.at[1, zl, y, core], w2.at[z, y, core])
    loads = []
    for t in range(3):
        loads.append((
            pltpu.make_async_copy(columns(weights[t], 1 - y), stage.at[t], load_sem.at[t, 0]),
            pltpu.make_async_copy(columns(weights[t], y), homes[t], load_sem.at[t, 1]),
        ))

    def tok_load(i):
        column = (1 - half) * span + ha * sub + i if i < sub else half * span + i - sub
        return pltpu.make_async_copy(
            tok_ref.at[:, pl.ds(pl.multiple_of(column * group, 128), group)], tok_buf.at[i], tok_sem.at[i]
        )

    for load in loads[0]:
        load.start()
    for i in range(sub):
        tok_load(i).start()
    for load in (*loads[1], *loads[2]):
        load.start()
    for i in range(sub, sub + span):
        tok_load(i).start()

    place = pos_ref[...]
    chosen = jnp.sum(jnp.where(place >= 0, 1, 0), axis=1, keepdims=True)
    count[...] = jnp.broadcast_to(chosen, count.shape)

    barrier = pltpu.get_barrier_semaphore()

    @pl.loop(1, n)
    def _(k):
        pl.semaphore_signal(barrier, inc=1, device_id={"wa": lax.rem(me + k, n)}, device_id_type=MESH)

    pl.semaphore_signal(barrier, inc=1, device_id={"ha": 1 - ha}, device_id_type=MESH)

    slot_ids = lax.broadcasted_iota(jnp.int32, (CAP, pos_ref.shape[1]), 0)
    table = jnp.where(place == slot_ids, jnp.float32(1.0), jnp.float32(0.0)).astype(jnp.bfloat16)
    slot_route = jnp.sum(jnp.where(place == slot_ids, route_ref[...], jnp.float32(0.0)), axis=1, keepdims=True)
    route[...] = jnp.broadcast_to(slot_route, route.shape)

    pl.semaphore_wait(barrier, n)

    def slots(i):
        tok_load(i).wait()
        return jnp.dot(table, tok_buf[i], preferred_element_type=jnp.float32).astype(jnp.bfloat16)

    def direct(ref, yy, sems, k, **where):
        return same(ref.at[pl.ds(ha * sub, sub), yy], sems[0].at[k], sems[1].at[k], **where)

    def other(ref, yy, sems, k, **where):
        return same(ref.at[pl.ds((1 - ha) * sub, sub), yy], sems[0].at[k], sems[1].at[k], **where)

    g_sems = (g_send, g_recv)
    to_x = {"ha": 1 - ha}
    to_y = {"wa": beside}
    guest_send = remote(guest_out, guest_rows.at[pl.ds(ha * sub, sub), y], g_send.at[0], g_recv.at[0], wa=mirror)
    guest_y, guest_y_got = direct(guest_rows, y, g_sems, 1, **to_y), direct(guest_rows, 1 - y, g_sems, 1, **to_y)
    guest_x, guest_x_got = direct(guest_rows, y, g_sems, 2, **to_x), other(guest_rows, y, g_sems, 2, **to_x)
    guest_d, guest_d_got = direct(guest_rows, 1 - y, g_sems, 3, **to_x), other(guest_rows, 1 - y, g_sems, 3, **to_x)
    own_y, own_y_got = direct(own_rows, y, g_sems, 4, **to_y), direct(own_rows, 1 - y, g_sems, 4, **to_y)
    own_d, own_d_got = direct(own_rows, 1 - y, g_sems, 5, **to_x), other(own_rows, 1 - y, g_sems, 5, **to_x)

    for load in loads[0]:
        load.wait()
    exchange(0).start()
    first.spread(0, zl, y)
    for i in range(sub):
        guest_out[i] = slots(i)
    guest_send.start()
    for load in loads[1]:
        load.wait()
    exchange(1).start()
    first.spread(1, zl, y)
    for i in range(span):
        own_rows[i, y] = slots(sub + i)
    own_y.start()
    for load in loads[2]:
        load.wait()
    exchange(2).start()

    @pl.loop(1, n)
    def _(k):
        count_copy(k).start()

    for t in (0, 1):
        first.serve(t, zl, 1 - y)
    second.spread(0, z, y)

    guest_send.wait_recv()
    guest_y.start()
    guest_x.start()
    own_y_got.wait_recv()
    own_d.start()

    def line_in(e):
        zi = order(e, zl, span)
        for yy in (y, 1 - y):
            for t in (0, 1):
                first.serve(t, zi, yy)

    def line_all(e):
        zi = order(e, zl, span)
        for t in (0, 1):
            for yy in (0, 1):
                first.given(t, zi, yy).wait_recv()

    line_all(0)
    second.serve(0, z, 1 - y)
    own_d_got.wait_recv()

    def project(rows, e, t):
        zi = order(e, zl, span)
        return jnp.dot(rows(zi), w1[t, zi].reshape(group, q), preferred_element_type=jnp.float32)

    def guests(yy):
        return lambda zi: guest_rows[zi, yy]

    def mine(zi):
        return own_rows[zi].reshape(2 * CAP, group)

    for t in (0, 1):
        own_acc[t] = project(mine, 0, t)
    guest_y_got.wait_recv()
    guest_d.start()
    guest_x_got.wait_recv()
    for t in (0, 1):
        guest_acc[t] = project(guests(y), 0, t)
    for e in range(1, span):
        line_in(e)
        line_all(e)
        if e + 1 < span:
            for t in (0, 1):
                guest_acc[t] = guest_acc[t] + project(guests(y), e, t)

    def partial(yy):
        return remote(part_out.at[yy], part_in.at[yy], p_send.at[yy], p_recv.at[yy], wa=mirror)

    for t in (0, 1):
        part_out[y, t] = (guest_acc[t] + project(guests(y), span - 1, t)).astype(jnp.bfloat16)
    partial(y).start()
    guest_d_got.wait_recv()
    for t in (0, 1):
        total = project(guests(1 - y), 0, t)
        for e in range(1, span):
            total = total + project(guests(1 - y), e, t)
        part_out[1 - y, t] = total.astype(jnp.bfloat16)
    partial(1 - y).start()

    def line2_in(e):
        zi = order(e, z, zs)
        for yy in (y, 1 - y):
            second.serve(0, zi, yy)

    line2_in(1)
    for t in (0, 1):
        for e in range(1, span):
            own_acc[t] = own_acc[t] + project(mine, e, t)

    @pl.loop(2, span + 1)
    def _(e):
        line2_in(e)

    for yy in (0, 1):
        partial(yy).wait_recv()
    for yy in (0, 1):
        gate = own_acc[0, yy * CAP:(yy + 1) * CAP] + part_in[yy, 0].astype(jnp.float32)
        up = own_acc[1, yy * CAP:(yy + 1) * CAP] + part_in[yy, 1].astype(jnp.float32)
        hidden[yy] = (gate / (1.0 + jnp.exp(-gate)) * up).astype(jnp.bfloat16)

    def swap_x(j):
        return remote(x_out.at[j], x_in.at[j], x_send.at[j], x_recv.at[j], ha=1 - ha)

    def swap_y(zi):
        return remote(y_out.at[zi], y_in.at[zi], y_send.at[zi], y_recv.at[zi], wa=beside)

    def swap_xy(j):
        return remote(xy_out.at[j], xy_in.at[j], xy_send.at[j], xy_recv.at[j], wa=beside)

    def swap_yx(j):
        return remote(yx_out.at[j], yx_in.at[j], yx_send.at[j], yx_recv.at[j], ha=1 - ha)

    def mine_rows(v):
        return jnp.where(y == 0, v[:CAP], v[CAP:]), jnp.where(y == 0, v[CAP:], v[:CAP])

    def down(zi, yy):
        return lax.dot_general(
            hidden[...].reshape(2 * CAP, q), w2[zi, yy].reshape(2 * fd, q), (((1,), (1,)), ((), ())),
            preferred_element_type=jnp.float32,
        )

    def finish(e):
        zi = order(e, z, zs)
        out = zi // span
        j = zi - out * span
        for yy in (0, 1):
            second.given(0, zi, yy).wait_recv()
        part = down(zi, 0)

        @pl.when(out == ha)
        def _():
            x_own[j] = part

        @pl.when(out != ha)
        def _():
            x_out[j] = part.astype(jnp.bfloat16)
            swap_x(j).start()

        keep, leave = mine_rows(down(zi, 1))
        y_out[zi] = leave.astype(jnp.bfloat16)
        swap_y(zi).start()
        y_own[zi] = keep

    def combine(e):
        zi = order(e, z, zs)
        out = zi // span
        j = zi - out * span
        swap_y(zi).wait_recv()
        total = y_own[zi] + y_in[zi].astype(jnp.float32)

        @pl.when(out != ha)
        def _():
            yx_out[j] = total.astype(jnp.bfloat16)
            swap_yx(j).start()

        @pl.when(out == ha)
        def _():
            y_own[zi] = total
            swap_x(j).wait_recv()
            keep, leave = mine_rows(x_own[j] + x_in[j].astype(jnp.float32))
            xy_own[j] = keep
            xy_out[j] = leave.astype(jnp.bfloat16)
            swap_xy(j).start()

    @pl.loop(0, zs)
    def _(e):
        @pl.when(e > span)
        def _():
            line2_in(e)

        finish(e)

        @pl.when(e > 0)
        def _():
            combine(e - 1)

    combine(zs - 1)

    @pl.loop(1, n)
    def _(k):
        count_got(k).wait_recv()

    counts[me] = jnp.zeros(counts.shape[1:], jnp.int32)

    def add_count(i, total):
        return total + jnp.where(i < me, counts[i], 0)

    earlier = lax.fori_loop(0, n, add_count, jnp.zeros(counts.shape[1:], jnp.int32))
    slot = lax.broadcasted_iota(jnp.int32, (CAP, 1), 0)
    scale = jnp.where(slot + earlier[0:1, 0:1] < n // 2 * CAP, route[:, 0:1], jnp.float32(0.0))
    wide = 2 * fd

    for j in range(span):
        swap_xy(j).wait_recv()
        total = xy_own[j] + xy_in[j].astype(jnp.float32)
        y_ref[:, 2 * j * wide:(2 * j + 1) * wide] = (total * scale).astype(jnp.bfloat16)
        swap_yx(j).wait_recv()
        total = y_own[ha * span + j] + yx_in[j].astype(jnp.float32)
        y_ref[:, (2 * j + 1) * wide:(2 * j + 2) * wide] = (total * scale).astype(jnp.bfloat16)

    @pl.loop(1, n)
    def _(k):
        count_copy(k).wait_send()

    for t in range(3):
        exchange(t).wait_send()
    for copy in (guest_send, guest_y, guest_x, guest_d, own_y, own_d, partial(0), partial(1)):
        copy.wait_send()
    first.drain((0, 1))
    second.drain((0,))

    @pl.loop(0, span)
    def _(j):
        swap_x(j).wait_send()
        swap_xy(j).wait_send()
        swap_yx(j).wait_send()

    @pl.loop(0, zs)
    def _(zi):
        swap_y(zi).wait_send()


def expert(pos, route_sum, tokens, gate, up, down):
    n = lax.axis_size("wa")
    fd, hid = gate.shape
    q = hid // 2
    zs = n // 4
    span = zs // 2
    sub = span // 2
    group = 4 * fd
    wide = 2 * fd
    any_spec = pl.BlockSpec(memory_space=pl.ANY)
    vmem = pl.BlockSpec(memory_space=pltpu.VMEM)
    dma = pltpu.SemaphoreType.DMA
    bf16, f32 = jnp.bfloat16, jnp.float32
    return pl.pallas_call(
        functools.partial(expert_kernel, n),
        out_shape=jax.ShapeDtypeStruct((CAP, span * group), bf16),
        in_specs=[vmem, vmem, any_spec, any_spec, any_spec, any_spec],
        out_specs=vmem,
        scratch_shapes=[
            pltpu.VMEM((2, span, 2, 2, fd, q), bf16),
            pltpu.VMEM((zs, 2, 2, fd, q), bf16),
            pltpu.VMEM((3, fd, q), bf16),
            pltpu.VMEM((sub + span, tokens.shape[0], group), bf16),
            pltpu.VMEM((sub, CAP, group), bf16),
            pltpu.VMEM((span, 2, CAP, group), bf16),
            pltpu.VMEM((span, 2, CAP, group), bf16),
            pltpu.VMEM((2, 2 * CAP, q), f32),
            pltpu.VMEM((2, CAP, q), f32),
            pltpu.VMEM((2, 2, CAP, q), bf16),
            pltpu.VMEM((2, 2, CAP, q), bf16),
            pltpu.VMEM((2, CAP, q), bf16),
            pltpu.VMEM((span, 2 * CAP, wide), f32),
            pltpu.VMEM((span, 2 * CAP, wide), bf16),
            pltpu.VMEM((span, 2 * CAP, wide), bf16),
            pltpu.VMEM((zs, CAP, wide), f32),
            pltpu.VMEM((zs, CAP, wide), bf16),
            pltpu.VMEM((zs, CAP, wide), bf16),
            pltpu.VMEM((span, CAP, wide), f32),
            pltpu.VMEM((span, CAP, wide), bf16),
            pltpu.VMEM((span, CAP, wide), bf16),
            pltpu.VMEM((span, CAP, wide), bf16),
            pltpu.VMEM((span, CAP, wide), bf16),
            pltpu.VMEM((8, 128), jnp.int32),
            pltpu.VMEM((n, 8, 128), jnp.int32),
            pltpu.VMEM((CAP, 128), f32),
            dma((3, 2)), dma((sub + span,)), dma((n,)), dma((n,)), dma((3,)), dma((3,)),
            dma((2, 2, span, 2)), dma((2, span, 2)), dma((2, span, 2)), dma((2, span, 2)),
            dma((2, 1, zs, 2)), dma((1, zs, 2)), dma((1, zs, 2)), dma((1, zs, 2)),
            dma((6,)), dma((6,)), dma((2,)), dma((2,)),
            dma((span,)), dma((span,)), dma((zs,)), dma((zs,)),
            dma((span,)), dma((span,)), dma((span,)), dma((span,)),
        ],
        compiler_params=pltpu.CompilerParams(
            collective_id=0, has_side_effects=True, vmem_limit_bytes=60 * 1024 * 1024
        ),
    )(pos, route_sum, tokens, gate, up, down)


def per_device(tokens, expert_ids, keep_mask, route_weight, gate_weight, up_weight, down_weight):
    matches = (expert_ids == 0) & (keep_mask == 1)
    chosen = jnp.any(matches, axis=1).astype(jnp.int32)
    route_sum = jnp.sum(jnp.where(matches, route_weight, jnp.float32(0.0)), axis=1)
    position = jnp.cumsum(chosen) - chosen
    place = jnp.where(chosen == 1, position, -1)
    y = expert(place[None, :], route_sum[None, :], tokens, gate_weight, up_weight, down_weight)
    slot_ids = jnp.arange(CAP, dtype=jnp.int32)
    pick = (place[:, None] == slot_ids[None, :]).astype(jnp.bfloat16)
    return jnp.dot(pick, y, preferred_element_type=jnp.float32).astype(jnp.bfloat16)


def solution(mesh):
    return jax.shard_map(
        per_device,
        mesh=mesh,
        in_specs=(
            P("wa", None),
            P("wa", None),
            P("wa", None),
            P("wa", None),
            P("wa", "ha"),
            P("wa", "ha"),
            P("wa", "ha"),
        ),
        out_specs=P("wa", "ha"),
        check_vma=False,
    )
```

```python
import functools

import jax
import jax.numpy as jnp
from jax import lax
from jax.experimental import pallas as pl
from jax.experimental.pallas import tpu as pltpu
from jax.sharding import PartitionSpec as P

CAP = 128
MESH = pl.DeviceIdType.MESH


def expert_kernel(
    n,
    pos_ref, route_ref, tok_ref, gate_ref, up_ref, down_ref,
    y_ref,
    w1, w2, stage, tok_buf, guest_out, own_rows, guest_rows, own_acc, guest_acc, part_out, part_in, hidden,
    x_own, x_out, x_in, y_own, y_out, y_in, xy_own, xy_out, xy_in, yx_out, yx_in, count, counts, route,
    load_sem, tok_sem, c_send, c_recv, e_send, e_recv, l1_send, l1_recv, b1_send, b1_recv,
    l2_send, l2_recv, b2_send, b2_recv, g_send, g_recv, p_send, p_recv,
    x_send, x_recv, y_send, y_recv, xy_send, xy_recv, yx_send, yx_recv,
):
    zs = n // 4
    span = zs // 2
    sub = span // 2
    me = lax.axis_index("wa")
    ha = lax.axis_index("ha")
    core = lax.rem(me, 2)
    y = lax.rem(me // 2, 2)
    z = me // 4
    half = z // span
    zl = z - half * span
    sibling = me + 1 - 2 * core
    beside = me + 2 - 4 * y
    mirror = lax.rem(me + n // 2, n)
    q = hidden.shape[2]
    fd = stage.shape[1]
    group = 4 * fd

    def remote(ref, dst, send, recv, **where):
        return pltpu.make_async_remote_copy(
            src_ref=ref, dst_ref=dst, send_sem=send, recv_sem=recv, device_id=where, device_id_type=MESH
        )

    def same(ref, send, recv, **where):
        return remote(ref, ref, send, recv, **where)

    def order(e, at, size):
        low = jnp.where(at < size // 2, 1, 0)
        at = low * at + (1 - low) * (size - 1 - at)
        paired = jnp.where(e % 2 == 1, at + (e + 1) // 2, at - e // 2)
        nth = jnp.where(e <= 2 * at, paired, e)
        return low * nth + (1 - low) * (size - 1 - nth)

    class Line:
        def __init__(self, ref_of, at, size, sems):
            self.ref_of, self.at, self.size = ref_of, at, size
            self.l_send, self.l_recv, self.b_send, self.b_recv = sems

        def hop(self, way, *unit):
            to = me + 4 * (1 - 2 * way)
            return same(self.ref_of(core, *unit), self.l_send.at[(way, *unit)], self.l_recv.at[unit], wa=to)

        def up(self, zi):
            return (zi <= self.at) & (self.at + 1 < self.size)

        def down(self, zi):
            return (zi >= self.at) & (self.at > 0)

        def push(self, t, zi, yy):
            @pl.when(self.up(zi))
            def _():
                self.hop(0, t, zi, yy).start()

            @pl.when(self.down(zi))
            def _():
                self.hop(1, t, zi, yy).start()

        def arrive(self, t, zi, yy):
            self.hop(0, t, zi, yy).wait_recv()

        def give(self, t, zi, yy):
            return same(self.ref_of(core, t, zi, yy), self.b_send.at[t, zi, yy], self.b_recv.at[t, zi, yy], wa=sibling)

        def given(self, t, zi, yy):
            return same(
                self.ref_of(1 - core, t, zi, yy), self.b_send.at[t, zi, yy], self.b_recv.at[t, zi, yy], wa=sibling
            )

        def spread(self, t, zi, yy):
            self.push(t, zi, yy)
            self.give(t, zi, yy).start()

        def serve(self, t, zi, yy):
            self.arrive(t, zi, yy)
            self.spread(t, zi, yy)

        def drain(self, kinds):
            @pl.loop(0, self.size)
            def _(zi):
                for t in kinds:
                    for yy in (0, 1):
                        @pl.when(self.up(zi))
                        def _():
                            self.hop(0, t, zi, yy).wait_send()

                        @pl.when(self.down(zi))
                        def _():
                            self.hop(1, t, zi, yy).wait_send()

                        self.give(t, zi, yy).wait_send()

    first = Line(lambda c, t, zi, yy: w1.at[t, zi, yy, c], zl, span, (l1_send, l1_recv, b1_send, b1_recv))
    second = Line(lambda c, t, zi, yy: w2.at[zi, yy, c], z, zs, (l2_send, l2_recv, b2_send, b2_recv))

    def exchange(t):
        dst, recv = (w2.at[z, y, core], l2_recv.at[0, z, y]) if t == 2 else (w1.at[t, zl, y, core], l1_recv.at[t, zl, y])
        return remote(stage.at[t], dst, e_send.at[t], recv, wa=beside)

    def count_copy(k):
        return remote(count, counts.at[me], c_send.at[k], c_recv.at[k], wa=lax.rem(me + k, n))

    def count_got(k):
        return remote(count, counts.at[lax.rem(me - k + n, n)], c_send.at[k], c_recv.at[k], wa=lax.rem(me + k, n))

    def columns(ref, index):
        return ref.at[:, pl.ds(pl.multiple_of(index * q, 128), q)]

    weights = (gate_ref, up_ref, down_ref)
    homes = (w1.at[0, zl, y, core], w1.at[1, zl, y, core], w2.at[z, y, core])
    loads = []
    for t in range(3):
        loads.append((
            pltpu.make_async_copy(columns(weights[t], 1 - y), stage.at[t], load_sem.at[t, 0]),
            pltpu.make_async_copy(columns(weights[t], y), homes[t], load_sem.at[t, 1]),
        ))

    def tok_load(i):
        column = (1 - half) * span + ha * sub + i if i < sub else half * span + i - sub
        return pltpu.make_async_copy(
            tok_ref.at[:, pl.ds(pl.multiple_of(column * group, 128), group)], tok_buf.at[i], tok_sem.at[i]
        )

    for load in loads[0]:
        load.start()
    for i in range(sub):
        tok_load(i).start()
    for load in (*loads[1], *loads[2]):
        load.start()
    for i in range(sub, sub + span):
        tok_load(i).start()

    place = pos_ref[...]
    chosen = jnp.sum(jnp.where(place >= 0, 1, 0), axis=1, keepdims=True)
    count[...] = jnp.broadcast_to(chosen, count.shape)

    barrier = pltpu.get_barrier_semaphore()

    @pl.loop(1, n)
    def _(k):
        pl.semaphore_signal(barrier, inc=1, device_id={"wa": lax.rem(me + k, n)}, device_id_type=MESH)

    pl.semaphore_signal(barrier, inc=1, device_id={"ha": 1 - ha}, device_id_type=MESH)

    slot_ids = lax.broadcasted_iota(jnp.int32, (CAP, pos_ref.shape[1]), 0)
    table = jnp.where(place == slot_ids, jnp.float32(1.0), jnp.float32(0.0)).astype(jnp.bfloat16)
    slot_route = jnp.sum(jnp.where(place == slot_ids, route_ref[...], jnp.float32(0.0)), axis=1, keepdims=True)
    route[...] = jnp.broadcast_to(slot_route, route.shape)

    pl.semaphore_wait(barrier, n)

    def slots(i):
        tok_load(i).wait()
        return jnp.dot(table, tok_buf[i], preferred_element_type=jnp.float32).astype(jnp.bfloat16)

    def direct(ref, yy, sems, k, **where):
        return same(ref.at[pl.ds(ha * sub, sub), yy], sems[0].at[k], sems[1].at[k], **where)

    def other(ref, yy, sems, k, **where):
        return same(ref.at[pl.ds((1 - ha) * sub, sub), yy], sems[0].at[k], sems[1].at[k], **where)

    g_sems = (g_send, g_recv)
    to_x = {"ha": 1 - ha}
    to_y = {"wa": beside}
    guest_send = remote(guest_out, guest_rows.at[pl.ds(ha * sub, sub), y], g_send.at[0], g_recv.at[0], wa=mirror)
    guest_y, guest_y_got = direct(guest_rows, y, g_sems, 1, **to_y), direct(guest_rows, 1 - y, g_sems, 1, **to_y)
    guest_x, guest_x_got = direct(guest_rows, y, g_sems, 2, **to_x), other(guest_rows, y, g_sems, 2, **to_x)
    guest_d, guest_d_got = direct(guest_rows, 1 - y, g_sems, 3, **to_x), other(guest_rows, 1 - y, g_sems, 3, **to_x)
    own_y, own_y_got = direct(own_rows, y, g_sems, 4, **to_y), direct(own_rows, 1 - y, g_sems, 4, **to_y)
    own_d, own_d_got = direct(own_rows, 1 - y, g_sems, 5, **to_x), other(own_rows, 1 - y, g_sems, 5, **to_x)

    def line_in(e):
        zi = order(e, zl, span)
        for yy in (y, 1 - y):
            for t in (0, 1):
                first.serve(t, zi, yy)

    def line_all(e):
        zi = order(e, zl, span)
        for t in (0, 1):
            for yy in (0, 1):
                first.given(t, zi, yy).wait_recv()

    def line2_in(e):
        zi = order(e, z, zs)
        for yy in (0, 1):
            second.serve(0, zi, yy)

    def project(rows, e, t):
        zi = order(e, zl, span)
        return jnp.dot(rows(zi), w1[t, zi].reshape(group, q), preferred_element_type=jnp.float32)

    def guests(yy):
        return lambda zi: guest_rows[zi, yy]

    def mine(zi):
        return own_rows[zi].reshape(2 * CAP, group)

    def partial(yy):
        return remote(part_out.at[yy], part_in.at[yy], p_send.at[yy], p_recv.at[yy], wa=mirror)

    for load in loads[0]:
        load.wait()
    exchange(0).start()
    first.spread(0, zl, y)
    for i in range(sub):
        guest_out[i] = slots(i)
    guest_send.start()
    for load in loads[1]:
        load.wait()
    exchange(1).start()
    first.spread(1, zl, y)
    for load in loads[2]:
        load.wait()
    exchange(2).start()
    for i in range(span):
        own_rows[i, y] = slots(sub + i)

    @pl.loop(1, n)
    def _(k):
        count_copy(k).start()

    for t in (0, 1):
        first.serve(t, zl, 1 - y)
    second.spread(0, z, y)
    guest_send.wait_recv()
    guest_y.start()
    guest_x.start()
    own_y.start()
    second.serve(0, z, 1 - y)
    line_all(0)
    guest_y_got.wait_recv()
    guest_d.start()
    guest_x_got.wait_recv()
    for t in (0, 1):
        guest_acc[t] = project(guests(y), 0, t)
    for e in range(1, span):
        line_in(e)
        line_all(e)
        if e + 1 < span:
            for t in (0, 1):
                guest_acc[t] = guest_acc[t] + project(guests(y), e, t)
    for t in (0, 1):
        part_out[y, t] = (guest_acc[t] + project(guests(y), span - 1, t)).astype(jnp.bfloat16)
    partial(y).start()
    middle = (z > 0) & (z + 1 < zs)

    @pl.when(middle)
    def _():
        line2_in(1)

    own_y_got.wait_recv()
    own_d.start()
    guest_d_got.wait_recv()
    for t in (0, 1):
        total = project(guests(1 - y), 0, t)
        for e in range(1, span):
            total = total + project(guests(1 - y), e, t)
        part_out[1 - y, t] = total.astype(jnp.bfloat16)
    partial(1 - y).start()

    @pl.when(jnp.logical_not(middle))
    def _():
        line2_in(1)

    @pl.when(middle)
    def _():
        @pl.loop(2, span + 1)
        def _(e):
            line2_in(e)

    own_d_got.wait_recv()
    for t in (0, 1):
        total = project(mine, 0, t)
        for e in range(1, span):
            total = total + project(mine, e, t)
        own_acc[t] = total
    for yy in (0, 1):
        partial(yy).wait_recv()
    for yy in (0, 1):
        gate = own_acc[0, yy * CAP:(yy + 1) * CAP] + part_in[yy, 0].astype(jnp.float32)
        up = own_acc[1, yy * CAP:(yy + 1) * CAP] + part_in[yy, 1].astype(jnp.float32)
        hidden[yy] = (gate / (1.0 + jnp.exp(-gate)) * up).astype(jnp.bfloat16)

    def swap_x(j):
        return remote(x_out.at[j], x_in.at[j], x_send.at[j], x_recv.at[j], ha=1 - ha)

    def swap_y(zi):
        return remote(y_out.at[zi], y_in.at[zi], y_send.at[zi], y_recv.at[zi], wa=beside)

    def swap_xy(j):
        return remote(xy_out.at[j], xy_in.at[j], xy_send.at[j], xy_recv.at[j], wa=beside)

    def swap_yx(j):
        return remote(yx_out.at[j], yx_in.at[j], yx_send.at[j], yx_recv.at[j], ha=1 - ha)

    def mine_rows(v):
        return jnp.where(y == 0, v[:CAP], v[CAP:]), jnp.where(y == 0, v[CAP:], v[:CAP])

    def down(zi, yy):
        return lax.dot_general(
            hidden[...].reshape(2 * CAP, q), w2[zi, yy].reshape(2 * fd, q), (((1,), (1,)), ((), ())),
            preferred_element_type=jnp.float32,
        )

    def finish(e, yy):
        zi = order(e, z, zs)
        out = zi // span
        j = zi - out * span
        second.given(0, zi, yy).wait_recv()
        part = down(zi, yy)
        if yy == 0:
            @pl.when(out == ha)
            def _():
                x_own[j] = part

            @pl.when(out != ha)
            def _():
                x_out[j] = part.astype(jnp.bfloat16)
                swap_x(j).start()
        else:
            keep, leave = mine_rows(part)
            y_out[zi] = leave.astype(jnp.bfloat16)
            swap_y(zi).start()
            y_own[zi] = keep

    def combine(e):
        zi = order(e, z, zs)
        out = zi // span
        j = zi - out * span
        swap_y(zi).wait_recv()
        total = y_own[zi] + y_in[zi].astype(jnp.float32)

        @pl.when(out != ha)
        def _():
            yx_out[j] = total.astype(jnp.bfloat16)
            swap_yx(j).start()

        @pl.when(out == ha)
        def _():
            y_own[zi] = total
            swap_x(j).wait_recv()
            keep, leave = mine_rows(x_own[j] + x_in[j].astype(jnp.float32))
            xy_own[j] = keep
            xy_out[j] = leave.astype(jnp.bfloat16)
            swap_xy(j).start()

    def late(e):
        zi = order(e, z, zs)
        for yy in (0, 1):
            second.serve(0, zi, yy)
            finish(e, yy)

    @pl.loop(0, 2)
    def _(e):
        finish(e, 0)
        finish(e, 1)

    @pl.loop(2, span + 1)
    def _(e):
        @pl.when(jnp.logical_not(middle))
        def _():
            line2_in(e)

        finish(e, 0)
        finish(e, 1)


    @pl.when(middle)
    def _():
        @pl.loop(span + 1, zs)
        def _(e):
            late(e)


    @pl.loop(0, span + 1)
    def _(e):
        combine(e)


    @pl.when(jnp.logical_not(middle))
    def _():
        @pl.loop(span + 1, zs)
        def _(e):
            late(e)


    @pl.loop(span + 1, zs)
    def _(e):
        combine(e)

    @pl.loop(1, n)
    def _(k):
        count_got(k).wait_recv()

    counts[me] = jnp.zeros(counts.shape[1:], jnp.int32)

    def add_count(i, total):
        return total + jnp.where(i < me, counts[i], 0)

    earlier = lax.fori_loop(0, n, add_count, jnp.zeros(counts.shape[1:], jnp.int32))
    slot = lax.broadcasted_iota(jnp.int32, (CAP, 1), 0)
    scale = jnp.where(slot + earlier[0:1, 0:1] < n // 2 * CAP, route[:, 0:1], jnp.float32(0.0))
    wide = 2 * fd

    for j in range(span):
        swap_xy(j).wait_recv()
        total = xy_own[j] + xy_in[j].astype(jnp.float32)
        y_ref[:, 2 * j * wide:(2 * j + 1) * wide] = (total * scale).astype(jnp.bfloat16)
        swap_yx(j).wait_recv()
        total = y_own[ha * span + j] + yx_in[j].astype(jnp.float32)
        y_ref[:, (2 * j + 1) * wide:(2 * j + 2) * wide] = (total * scale).astype(jnp.bfloat16)

    @pl.loop(1, n)
    def _(k):
        count_copy(k).wait_send()

    for t in range(3):
        exchange(t).wait_send()
    for copy in (guest_send, guest_y, guest_x, guest_d, own_y, own_d, partial(0), partial(1)):
        copy.wait_send()
    first.drain((0, 1))
    second.drain((0,))

    @pl.loop(0, span)
    def _(j):
        swap_x(j).wait_send()
        swap_xy(j).wait_send()
        swap_yx(j).wait_send()

    @pl.loop(0, zs)
    def _(zi):
        swap_y(zi).wait_send()


def expert(pos, route_sum, tokens, gate, up, down):
    n = lax.axis_size("wa")
    fd, hid = gate.shape
    q = hid // 2
    zs = n // 4
    span = zs // 2
    sub = span // 2
    group = 4 * fd
    wide = 2 * fd
    any_spec = pl.BlockSpec(memory_space=pl.ANY)
    vmem = pl.BlockSpec(memory_space=pltpu.VMEM)
    dma = pltpu.SemaphoreType.DMA
    bf16, f32 = jnp.bfloat16, jnp.float32
    return pl.pallas_call(
        functools.partial(expert_kernel, n),
        out_shape=jax.ShapeDtypeStruct((CAP, span * group), bf16),
        in_specs=[vmem, vmem, any_spec, any_spec, any_spec, any_spec],
        out_specs=vmem,
        scratch_shapes=[
            pltpu.VMEM((2, span, 2, 2, fd, q), bf16),
            pltpu.VMEM((zs, 2, 2, fd, q), bf16),
            pltpu.VMEM((3, fd, q), bf16),
            pltpu.VMEM((sub + span, tokens.shape[0], group), bf16),
            pltpu.VMEM((sub, CAP, group), bf16),
            pltpu.VMEM((span, 2, CAP, group), bf16),
            pltpu.VMEM((span, 2, CAP, group), bf16),
            pltpu.VMEM((2, 2 * CAP, q), f32),
            pltpu.VMEM((2, CAP, q), f32),
            pltpu.VMEM((2, 2, CAP, q), bf16),
            pltpu.VMEM((2, 2, CAP, q), bf16),
            pltpu.VMEM((2, CAP, q), bf16),
            pltpu.VMEM((span, 2 * CAP, wide), f32),
            pltpu.VMEM((span, 2 * CAP, wide), bf16),
            pltpu.VMEM((span, 2 * CAP, wide), bf16),
            pltpu.VMEM((zs, CAP, wide), f32),
            pltpu.VMEM((zs, CAP, wide), bf16),
            pltpu.VMEM((zs, CAP, wide), bf16),
            pltpu.VMEM((span, CAP, wide), f32),
            pltpu.VMEM((span, CAP, wide), bf16),
            pltpu.VMEM((span, CAP, wide), bf16),
            pltpu.VMEM((span, CAP, wide), bf16),
            pltpu.VMEM((span, CAP, wide), bf16),
            pltpu.VMEM((8, 128), jnp.int32),
            pltpu.VMEM((n, 8, 128), jnp.int32),
            pltpu.VMEM((CAP, 128), f32),
            dma((3, 2)), dma((sub + span,)), dma((n,)), dma((n,)), dma((3,)), dma((3,)),
            dma((2, 2, span, 2)), dma((2, span, 2)), dma((2, span, 2)), dma((2, span, 2)),
            dma((2, 1, zs, 2)), dma((1, zs, 2)), dma((1, zs, 2)), dma((1, zs, 2)),
            dma((6,)), dma((6,)), dma((2,)), dma((2,)),
            dma((span,)), dma((span,)), dma((zs,)), dma((zs,)),
            dma((span,)), dma((span,)), dma((span,)), dma((span,)),
        ],
        compiler_params=pltpu.CompilerParams(
            collective_id=0, has_side_effects=True, vmem_limit_bytes=60 * 1024 * 1024
        ),
    )(pos, route_sum, tokens, gate, up, down)


def per_device(tokens, expert_ids, keep_mask, route_weight, gate_weight, up_weight, down_weight):
    matches = (expert_ids == 0) & (keep_mask == 1)
    chosen = jnp.any(matches, axis=1).astype(jnp.int32)
    route_sum = jnp.sum(jnp.where(matches, route_weight, jnp.float32(0.0)), axis=1)
    position = jnp.cumsum(chosen) - chosen
    place = jnp.where(chosen == 1, position, -1)
    y = expert(place[None, :], route_sum[None, :], tokens, gate_weight, up_weight, down_weight)
    slot_ids = jnp.arange(CAP, dtype=jnp.int32)
    pick = (place[:, None] == slot_ids[None, :]).astype(jnp.bfloat16)
    return jnp.dot(pick, y, preferred_element_type=jnp.float32).astype(jnp.bfloat16)


def solution(mesh):
    return jax.shard_map(
        per_device,
        mesh=mesh,
        in_specs=(
            P("wa", None),
            P("wa", None),
            P("wa", None),
            P("wa", None),
            P("wa", "ha"),
            P("wa", "ha"),
            P("wa", "ha"),
        ),
        out_specs=P("wa", "ha"),
        check_vma=False,
    )
```

```python
import functools

import jax
import jax.numpy as jnp
from jax import lax
from jax.experimental import pallas as pl
from jax.experimental.pallas import tpu as pltpu
from jax.sharding import PartitionSpec as P

CAP = 128
MESH = pl.DeviceIdType.MESH


def expert_kernel(
    n,
    ids_ref, keep_ref, route_ref, tok_ref, gate_ref, up_ref, down_ref,
    y_ref, place_ref,
    ids, keep, weight, w1, w2, stage, tok_buf, guest_out, own_rows, guest_rows, own_acc, guest_acc, part_out, part_in, hidden,
    x_own, x_out, x_in, y_own, y_out, y_in, xy_own, xy_out, xy_in, yx_out, yx_in, y_buf, count, counts, route,
    load_sem, tok_sem, c_send, c_recv, e_send, e_recv, l1_send, l1_recv, b1_send, b1_recv,
    l2_send, l2_recv, b2_send, b2_recv, g_send, g_recv, p_send, p_recv,
    x_send, x_recv, y_send, y_recv, xy_send, xy_recv, yx_send, yx_recv, out_sem, route_sem,
):
    zs = n // 4
    span = zs // 2
    sub = span // 2
    me = lax.axis_index("wa")
    ha = lax.axis_index("ha")
    core = lax.rem(me, 2)
    y = lax.rem(me // 2, 2)
    z = me // 4
    half = z // span
    zl = z - half * span
    sibling = me + 1 - 2 * core
    beside = me + 2 - 4 * y
    mirror = lax.rem(me + n // 2, n)
    q = hidden.shape[2]
    fd = stage.shape[1]
    group = 4 * fd
    wide = 2 * fd

    def remote(ref, dst, send, recv, **where):
        return pltpu.make_async_remote_copy(
            src_ref=ref, dst_ref=dst, send_sem=send, recv_sem=recv, device_id=where, device_id_type=MESH
        )

    def same(ref, send, recv, **where):
        return remote(ref, ref, send, recv, **where)

    def order(e, at, size):
        low = jnp.where(at < size // 2, 1, 0)
        at = low * at + (1 - low) * (size - 1 - at)
        paired = jnp.where(e % 2 == 1, at + (e + 1) // 2, at - e // 2)
        nth = jnp.where(e <= 2 * at, paired, e)
        return low * nth + (1 - low) * (size - 1 - nth)

    def is_late(zi, at, size):
        low = jnp.where(at < size // 2, 1, 0)
        at = low * at + (1 - low) * (size - 1 - at)
        zi = low * zi + (1 - low) * (size - 1 - zi)
        rank = jnp.where(zi > 2 * at, zi, jnp.where(zi > at, 2 * (zi - at) - 1, 2 * (at - zi)))
        return (rank > size // 2) | ((at == 0) & ((rank == 1) | (rank > 2)))

    class Line:
        def __init__(self, ref_of, at, size, sems):
            self.ref_of, self.at, self.size = ref_of, at, size
            self.l_send, self.l_recv, self.b_send, self.b_recv = sems

        def hop(self, way, *unit):
            to = me + 4 * (1 - 2 * way)
            return same(self.ref_of(core, *unit), self.l_send.at[(way, *unit)], self.l_recv.at[unit], wa=to)

        def up(self, zi):
            return (zi <= self.at) & (self.at + 1 < self.size)

        def down(self, zi):
            return (zi >= self.at) & (self.at > 0)

        def push(self, t, zi, yy):
            @pl.when(self.up(zi))
            def _():
                self.hop(0, t, zi, yy).start()

            @pl.when(self.down(zi))
            def _():
                self.hop(1, t, zi, yy).start()

        def arrive(self, t, zi, yy):
            self.hop(0, t, zi, yy).wait_recv()

        def give(self, t, zi, yy):
            return same(self.ref_of(core, t, zi, yy), self.b_send.at[t, zi, yy], self.b_recv.at[t, zi, yy], wa=sibling)

        def given(self, t, zi, yy):
            return same(
                self.ref_of(1 - core, t, zi, yy), self.b_send.at[t, zi, yy], self.b_recv.at[t, zi, yy], wa=sibling
            )

        def spread(self, t, zi, yy):
            self.push(t, zi, yy)
            self.give(t, zi, yy).start()

        def serve(self, t, zi, yy):
            self.arrive(t, zi, yy)
            self.spread(t, zi, yy)

        def drain(self, kinds):
            @pl.loop(0, self.size)
            def _(zi):
                for t in kinds:
                    for yy in (0, 1):
                        @pl.when(self.up(zi))
                        def _():
                            self.hop(0, t, zi, yy).wait_send()

                        @pl.when(self.down(zi))
                        def _():
                            self.hop(1, t, zi, yy).wait_send()

                        self.give(t, zi, yy).wait_send()

    first = Line(lambda c, t, zi, yy: w1.at[t, zi, yy, c], zl, span, (l1_send, l1_recv, b1_send, b1_recv))
    second = Line(lambda c, t, zi, yy: w2.at[zi, yy, c], z, zs, (l2_send, l2_recv, b2_send, b2_recv))

    def exchange(t):
        dst, recv = (w2.at[z, y, core], l2_recv.at[0, z, y]) if t == 2 else (w1.at[t, zl, y, core], l1_recv.at[t, zl, y])
        return remote(stage.at[t], dst, e_send.at[t], recv, wa=beside)

    def count_copy(k):
        return remote(count, counts.at[me], c_send.at[k], c_recv.at[k], wa=lax.rem(me + k, n))

    def count_got(k):
        return remote(count, counts.at[lax.rem(me - k + n, n)], c_send.at[k], c_recv.at[k], wa=lax.rem(me + k, n))

    def columns(ref, index):
        return ref.at[:, pl.ds(pl.multiple_of(index * q, 128), q)]

    weights = (gate_ref, up_ref, down_ref)
    homes = (w1.at[0, zl, y, core], w1.at[1, zl, y, core], w2.at[z, y, core])
    loads = []
    for t in range(3):
        loads.append((
            pltpu.make_async_copy(columns(weights[t], 1 - y), stage.at[t], load_sem.at[t, 0]),
            pltpu.make_async_copy(columns(weights[t], y), homes[t], load_sem.at[t, 1]),
        ))

    def tok_load(i):
        column = (1 - half) * span + ha * sub + i if i < sub else half * span + i - sub
        return pltpu.make_async_copy(
            tok_ref.at[:, pl.ds(pl.multiple_of(column * group, 128), group)], tok_buf.at[i], tok_sem.at[i]
        )

    routing = [
        pltpu.make_async_copy(ref, buf, route_sem.at[k])
        for k, (ref, buf) in enumerate(((ids_ref, ids), (keep_ref, keep), (route_ref, weight)))
    ]
    for copy in (*loads[0], *routing):
        copy.start()
    for i in range(sub):
        tok_load(i).start()
    for load in (*loads[1], *loads[2]):
        load.start()
    for i in range(sub, sub + span):
        tok_load(i).start()

    barrier = pltpu.get_barrier_semaphore()

    @pl.loop(1, n)
    def _(k):
        pl.semaphore_signal(barrier, inc=1, device_id={"wa": lax.rem(me + k, n)}, device_id_type=MESH)

    pl.semaphore_signal(barrier, inc=1, device_id={"ha": 1 - ha}, device_id_type=MESH)

    pl.semaphore_wait(barrier, n)

    def direct(ref, yy, sems, k, **where):
        return same(ref.at[pl.ds(ha * sub, sub), yy], sems[0].at[k], sems[1].at[k], **where)

    def other(ref, yy, sems, k, **where):
        return same(ref.at[pl.ds((1 - ha) * sub, sub), yy], sems[0].at[k], sems[1].at[k], **where)

    g_sems = (g_send, g_recv)
    to_x = {"ha": 1 - ha}
    to_y = {"wa": beside}
    guest_send = remote(guest_out, guest_rows.at[pl.ds(ha * sub, sub), y], g_send.at[0], g_recv.at[0], wa=mirror)
    guest_y, guest_y_got = direct(guest_rows, y, g_sems, 1, **to_y), direct(guest_rows, 1 - y, g_sems, 1, **to_y)
    guest_x, guest_x_got = direct(guest_rows, y, g_sems, 2, **to_x), other(guest_rows, y, g_sems, 2, **to_x)
    guest_d, guest_d_got = direct(guest_rows, 1 - y, g_sems, 3, **to_x), other(guest_rows, 1 - y, g_sems, 3, **to_x)
    own_y, own_y_got = direct(own_rows, y, g_sems, 4, **to_y), direct(own_rows, 1 - y, g_sems, 4, **to_y)
    own_d, own_d_got = direct(own_rows, 1 - y, g_sems, 5, **to_x), other(own_rows, 1 - y, g_sems, 5, **to_x)

    def line_in(e):
        zi = order(e, zl, span)
        for yy in (y, 1 - y):
            for t in (0, 1):
                first.serve(t, zi, yy)

    def line_all(e):
        zi = order(e, zl, span)
        for t in (0, 1):
            for yy in (0, 1):
                first.given(t, zi, yy).wait_recv()

    def line2_in(e):
        zi = order(e, z, zs)
        for yy in (0, 1):
            second.serve(0, zi, yy)

    def project(rows, e, t):
        zi = order(e, zl, span)
        return jnp.dot(rows(zi), w1[t, zi].reshape(group, q), preferred_element_type=jnp.float32)

    def guests(yy):
        return lambda zi: guest_rows[zi, yy]

    def mine(zi):
        return own_rows[zi].reshape(2 * CAP, group)

    def partial(yy):
        return remote(part_out.at[yy], part_in.at[yy], p_send.at[yy], p_recv.at[yy], wa=mirror)

    for load in loads[0]:
        load.wait()
    exchange(0).start()
    first.spread(0, zl, y)
    for copy in routing:
        copy.wait()
    matches = (ids[...] == 0) & (keep[...] == 1)
    chosen = jnp.minimum(jnp.sum(jnp.where(matches, 1, 0), axis=0, keepdims=True), 1)
    route_sum = jnp.sum(jnp.where(matches, weight[...], jnp.float32(0.0)), axis=0, keepdims=True)
    length = chosen.shape[1]
    lane = lax.broadcasted_iota(jnp.int32, (8, length), 1)
    running = jnp.broadcast_to(chosen, (8, length))
    shift = 1
    while shift < length:
        running = running + jnp.where(lane >= shift, pltpu.roll(running, shift, 1), 0)
        shift *= 2
    place = jnp.where(chosen == 1, running[0:1] - 1, -1)
    place_ref[...] = place
    count[...] = jnp.broadcast_to(jnp.sum(chosen, axis=1, keepdims=True), count.shape)
    slot_ids = lax.broadcasted_iota(jnp.int32, (CAP, length), 0)
    hit = place == slot_ids
    table = jnp.where(hit, jnp.float32(1.0), jnp.float32(0.0)).astype(jnp.bfloat16)
    for i in range(sub):
        tok_load(i).wait()
        guest_out[i] = jnp.dot(table, tok_buf[i], preferred_element_type=jnp.float32).astype(jnp.bfloat16)
    guest_send.start()
    for load in loads[1]:
        load.wait()
    exchange(1).start()
    first.spread(1, zl, y)
    for load in loads[2]:
        load.wait()
    exchange(2).start()
    slot_route = jnp.sum(jnp.where(hit, route_sum, jnp.float32(0.0)), axis=1, keepdims=True)
    route[...] = jnp.broadcast_to(slot_route, route.shape)
    for i in range(span):
        tok_load(sub + i).wait()
        own_rows[i, y] = jnp.dot(
            table, tok_buf[sub + i], preferred_element_type=jnp.float32
        ).astype(jnp.bfloat16)

    @pl.loop(1, n)
    def _(k):
        count_copy(k).start()

    for t in (0, 1):
        first.serve(t, zl, 1 - y)
    second.spread(0, z, y)
    guest_send.wait_recv()
    guest_y.start()
    guest_x.start()
    own_y.start()
    second.serve(0, z, 1 - y)
    line_all(0)
    guest_y_got.wait_recv()
    guest_d.start()
    guest_x_got.wait_recv()
    for t in (0, 1):
        guest_acc[t] = project(guests(y), 0, t)
    for e in range(1, span):
        line_in(e)
        line_all(e)
        if e + 1 < span:
            for t in (0, 1):
                guest_acc[t] = guest_acc[t] + project(guests(y), e, t)
    for t in (0, 1):
        part_out[y, t] = (guest_acc[t] + project(guests(y), span - 1, t)).astype(jnp.bfloat16)
    partial(y).start()
    middle = (z > 0) & (z + 1 < zs)

    @pl.when(middle)
    def _():
        line2_in(1)

    own_y_got.wait_recv()
    own_d.start()
    guest_d_got.wait_recv()
    for t in (0, 1):
        total = project(guests(1 - y), 0, t)
        for e in range(1, span):
            total = total + project(guests(1 - y), e, t)
        part_out[1 - y, t] = total.astype(jnp.bfloat16)
    partial(1 - y).start()

    @pl.when(jnp.logical_not(middle))
    def _():
        line2_in(1)

    @pl.when(middle)
    def _():
        @pl.loop(2, span + 1)
        def _(e):
            line2_in(e)

    own_d_got.wait_recv()
    for t in (0, 1):
        total = project(mine, 0, t)
        for e in range(1, span):
            total = total + project(mine, e, t)
        own_acc[t] = total
    for yy in (0, 1):
        partial(yy).wait_recv()
    for yy in (0, 1):
        gate = own_acc[0, yy * CAP:(yy + 1) * CAP] + part_in[yy, 0].astype(jnp.float32)
        up = own_acc[1, yy * CAP:(yy + 1) * CAP] + part_in[yy, 1].astype(jnp.float32)
        hidden[yy] = (gate / (1.0 + jnp.exp(-gate)) * up).astype(jnp.bfloat16)

    def swap_x(j):
        return remote(x_out.at[j], x_in.at[j], x_send.at[j], x_recv.at[j], ha=1 - ha)

    def swap_y(zi, yy):
        return remote(y_out.at[yy, zi], y_in.at[yy, zi], y_send.at[yy, zi], y_recv.at[yy, zi], wa=beside)

    def swap_xy(j):
        return remote(xy_out.at[j], xy_in.at[j], xy_send.at[j], xy_recv.at[j], wa=beside)

    def swap_yx(j, yy):
        return remote(yx_out.at[yy, j], yx_in.at[yy, j], yx_send.at[yy, j], yx_recv.at[yy, j], ha=1 - ha)

    def mine_rows(v):
        return jnp.where(y == 0, v[:CAP], v[CAP:]), jnp.where(y == 0, v[CAP:], v[:CAP])

    def down(zi, yy):
        return lax.dot_general(
            hidden[...].reshape(2 * CAP, q), w2[zi, yy].reshape(2 * fd, q), (((1,), (1,)), ((), ())),
            preferred_element_type=jnp.float32,
        )

    def place_of(e):
        zi = order(e, z, zs)
        out = zi // span
        return zi, out, zi - out * span

    def finish_x(e):
        zi, out, j = place_of(e)
        second.given(0, zi, 0).wait_recv()
        part = down(zi, 0)

        @pl.when(out == ha)
        def _():
            x_own[j] = part

        @pl.when(out != ha)
        def _():
            x_out[j] = part.astype(jnp.bfloat16)
            swap_x(j).start()

    def finish_y(e, yy):
        zi, out, j = place_of(e)
        second.given(0, zi, yy).wait_recv()
        keep, leave = mine_rows(down(zi, yy))
        y_out[yy, zi] = leave.astype(jnp.bfloat16)
        swap_y(zi, yy).start()
        y_own[yy, zi] = keep

    def combine_x(e):
        zi, out, j = place_of(e)

        @pl.when(out == ha)
        def _():
            swap_x(j).wait_recv()
            keep, leave = mine_rows(x_own[j] + x_in[j].astype(jnp.float32))
            xy_own[j] = keep
            xy_out[j] = leave.astype(jnp.bfloat16)
            swap_xy(j).start()

    def combine_y(e, yy):
        zi, out, j = place_of(e)
        swap_y(zi, yy).wait_recv()
        total = y_own[yy, zi] + y_in[yy, zi].astype(jnp.float32)

        @pl.when(out != ha)
        def _():
            yx_out[yy, j] = total.astype(jnp.bfloat16)
            swap_yx(j, yy).start()

        @pl.when(out == ha)
        def _():
            y_own[yy, zi] = total

    def late(e, yy):
        second.serve(0, order(e, z, zs), yy)
        finish_y(e, yy)

    @pl.when(middle)
    def _():
        @pl.loop(0, span + 1)
        def _(e):
            finish_x(e)
            finish_y(e, 1)

        @pl.loop(span + 1, zs)
        def _(e):
            late(e, 0)
            late(e, 1)

        @pl.loop(0, span + 1)
        def _(e):
            combine_y(e, 1)
            combine_x(e)

        @pl.loop(span + 1, zs)
        def _(e):
            combine_y(e, 0)
            combine_y(e, 1)

    @pl.when(jnp.logical_not(middle))
    def _():
        finish_y(0, 1)
        finish_x(0)
        finish_y(1, 0)
        finish_y(1, 1)
        second.serve(0, order(2, z, zs), 0)
        finish_x(2)
        late(2, 1)
        combine_y(0, 1)
        combine_x(0)
        combine_y(1, 0)
        combine_y(1, 1)

        @pl.loop(3, zs - 1)
        def _(e):
            late(e, 0)
            late(e, 1)
            combine_y(e, 0)
            combine_y(e, 1)

        late(zs - 1, 0)
        combine_y(2, 1)
        combine_x(2)
        late(zs - 1, 1)
        combine_y(zs - 1, 0)
        combine_y(zs - 1, 1)

    @pl.loop(1, n)
    def _(k):
        count_got(k).wait_recv()

    counts[me] = jnp.zeros(counts.shape[1:], jnp.int32)

    def add_count(i, total):
        return total + jnp.where(i < me, counts[i], 0)

    earlier = lax.fori_loop(0, n, add_count, jnp.zeros(counts.shape[1:], jnp.int32))
    slot = lax.broadcasted_iota(jnp.int32, (CAP, 1), 0)
    scale = jnp.where(slot + earlier[0:1, 0:1] < n // 2 * CAP, route[:, 0:1], jnp.float32(0.0))
    width = 2 * span * wide
    cut = wide if wide % 128 == 0 else width

    def out_copy(u):
        return pltpu.make_async_copy(y_buf.at[:, u * cut:(u + 1) * cut], y_ref.at[:, u * cut:(u + 1) * cut], out_sem.at[u])

    for yy in (1, 0):
        for j in range(span):
            zi = ha * span + j
            u = 2 * j + yy
            if yy == 0:
                behind = is_late(zi, z, zs)

                @pl.when(behind)
                def _():
                    swap_yx(j, 0).wait_recv()
                    y_buf[:, u * wide:(u + 1) * wide] = ((y_own[0, zi] + yx_in[0, j].astype(jnp.float32)) * scale).astype(jnp.bfloat16)

                @pl.when(jnp.logical_not(behind))
                def _():
                    swap_xy(j).wait_recv()
                    y_buf[:, u * wide:(u + 1) * wide] = ((xy_own[j] + xy_in[j].astype(jnp.float32)) * scale).astype(jnp.bfloat16)
            else:
                swap_yx(j, 1).wait_recv()
                y_buf[:, u * wide:(u + 1) * wide] = ((y_own[1, zi] + yx_in[1, j].astype(jnp.float32)) * scale).astype(jnp.bfloat16)
            if cut == wide:
                out_copy(u).start()

    if cut != wide:
        out_copy(0).start()

    @pl.loop(1, n)
    def _(k):
        count_copy(k).wait_send()

    for t in range(3):
        exchange(t).wait_send()
    for copy in (guest_send, guest_y, guest_x, guest_d, own_y, own_d, partial(0), partial(1)):
        copy.wait_send()
    first.drain((0, 1))
    second.drain((0,))

    @pl.loop(0, zs)
    def _(e):
        zi, out, j = place_of(e)
        swap_y(zi, 1).wait_send()

        @pl.when(out != ha)
        def _():
            swap_yx(j, 1).wait_send()

        behind = is_late(zi, z, zs)

        @pl.when(behind)
        def _():
            swap_y(zi, 0).wait_send()

            @pl.when(out != ha)
            def _():
                swap_yx(j, 0).wait_send()

        @pl.when(jnp.logical_not(behind))
        def _():
            @pl.when(out != ha)
            def _():
                swap_x(j).wait_send()

            @pl.when(out == ha)
            def _():
                swap_xy(j).wait_send()

    for u in range(width // cut):
        out_copy(u).wait()


def expert(ids, keep, weight, tokens, gate, up, down):
    n = lax.axis_size("wa")
    fd, hid = gate.shape
    q = hid // 2
    zs = n // 4
    span = zs // 2
    sub = span // 2
    group = 4 * fd
    wide = 2 * fd
    any_spec = pl.BlockSpec(memory_space=pl.ANY)
    vmem = pl.BlockSpec(memory_space=pltpu.VMEM)
    dma = pltpu.SemaphoreType.DMA
    bf16, f32 = jnp.bfloat16, jnp.float32
    return pl.pallas_call(
        functools.partial(expert_kernel, n),
        out_shape=(
            jax.ShapeDtypeStruct((CAP, span * group), bf16), jax.ShapeDtypeStruct((1, tokens.shape[0]), jnp.int32)
        ),
        in_specs=[any_spec] * 7,
        out_specs=(any_spec, vmem),
        scratch_shapes=[
            pltpu.VMEM(ids.shape, jnp.int32),
            pltpu.VMEM(ids.shape, jnp.int32),
            pltpu.VMEM(ids.shape, f32),
            pltpu.VMEM((2, span, 2, 2, fd, q), bf16),
            pltpu.VMEM((zs, 2, 2, fd, q), bf16),
            pltpu.VMEM((3, fd, q), bf16),
            pltpu.VMEM((sub + span, tokens.shape[0], group), bf16),
            pltpu.VMEM((sub, CAP, group), bf16),
            pltpu.VMEM((span, 2, CAP, group), bf16),
            pltpu.VMEM((span, 2, CAP, group), bf16),
            pltpu.VMEM((2, 2 * CAP, q), f32),
            pltpu.VMEM((2, CAP, q), f32),
            pltpu.VMEM((2, 2, CAP, q), bf16),
            pltpu.VMEM((2, 2, CAP, q), bf16),
            pltpu.VMEM((2, CAP, q), bf16),
            pltpu.VMEM((span, 2 * CAP, wide), f32),
            pltpu.VMEM((span, 2 * CAP, wide), bf16),
            pltpu.VMEM((span, 2 * CAP, wide), bf16),
            pltpu.VMEM((2, zs, CAP, wide), f32),
            pltpu.VMEM((2, zs, CAP, wide), bf16),
            pltpu.VMEM((2, zs, CAP, wide), bf16),
            pltpu.VMEM((span, CAP, wide), f32),
            pltpu.VMEM((span, CAP, wide), bf16),
            pltpu.VMEM((span, CAP, wide), bf16),
            pltpu.VMEM((2, span, CAP, wide), bf16),
            pltpu.VMEM((2, span, CAP, wide), bf16),
            pltpu.VMEM((CAP, 2 * span * wide), bf16),
            pltpu.VMEM((8, 128), jnp.int32),
            pltpu.VMEM((n, 8, 128), jnp.int32),
            pltpu.VMEM((CAP, 128), f32),
            dma((3, 2)), dma((sub + span,)), dma((n,)), dma((n,)), dma((3,)), dma((3,)),
            dma((2, 2, span, 2)), dma((2, span, 2)), dma((2, span, 2)), dma((2, span, 2)),
            dma((2, 1, zs, 2)), dma((1, zs, 2)), dma((1, zs, 2)), dma((1, zs, 2)),
            dma((6,)), dma((6,)), dma((2,)), dma((2,)),
            dma((span,)), dma((span,)), dma((2, zs)), dma((2, zs)),
            dma((span,)), dma((span,)), dma((2, span)), dma((2, span)), dma((2 * span,)), dma((3,)),
        ],
        compiler_params=pltpu.CompilerParams(
            collective_id=0, has_side_effects=True, vmem_limit_bytes=60 * 1024 * 1024
        ),
    )(ids, keep, weight, tokens, gate, up, down)


def per_device(tokens, expert_ids, keep_mask, route_weight, gate_weight, up_weight, down_weight):
    y, place = expert(expert_ids.T, keep_mask.T, route_weight.T, tokens, gate_weight, up_weight, down_weight)
    place = place[0]
    slot_ids = jnp.arange(CAP, dtype=jnp.int32)
    pick = (place[:, None] == slot_ids[None, :]).astype(jnp.bfloat16)
    return jnp.dot(pick, y, preferred_element_type=jnp.float32).astype(jnp.bfloat16)


def solution(mesh):
    return jax.shard_map(
        per_device,
        mesh=mesh,
        in_specs=(
            P("wa", None),
            P("wa", None),
            P("wa", None),
            P("wa", None),
            P("wa", "ha"),
            P("wa", "ha"),
            P("wa", "ha"),
        ),
        out_specs=P("wa", "ha"),
        check_vma=False,
    )
```

```python
import functools

import jax
import jax.numpy as jnp
from jax import lax
from jax.experimental import pallas as pl
from jax.experimental.pallas import tpu as pltpu
from jax.sharding import PartitionSpec as P

CAP = 128
MESH = pl.DeviceIdType.MESH


def expert_kernel(
    n,
    ids_ref, keep_ref, route_ref, tok_ref, gate_ref, up_ref, down_ref,
    y_ref, place_ref,
    ids, keep, weight, place_buf, w1, w2, stage, tok_buf, guest_out, own_rows, guest_rows, own_acc, guest_acc, part_out, part_in, hidden,
    x_own, x_out, x_in, y_own, y_out, y_in, xy_own, xy_out, xy_in, yx_out, yx_in, y_buf, count, counts, route,
    load_sem, tok_sem, c_sem, e_send, l1_send, l1_recv, b1_send, b1_recv, l2_send, l2_recv, b2_send, b2_recv,
    g_send, g_recv, p_send, p_recv, x_send, x_recv, y_send, y_recv, xy_send, xy_recv, yx_send, yx_recv,
    part_send, part_recv, out_sem, route_sem,
):
    zs = n // 4
    span = zs // 2
    sub = span // 2
    me = lax.axis_index("wa")
    ha = lax.axis_index("ha")
    core = lax.rem(me, 2)
    y = lax.rem(me // 2, 2)
    z = me // 4
    half = z // span
    zl = z - half * span
    sibling = me + 1 - 2 * core
    beside = me + 2 - 4 * y
    mirror = lax.rem(me + n // 2, n)
    q = hidden.shape[2]
    fd = stage.shape[1]
    group = 4 * fd
    wide = 2 * fd

    def remote(ref, dst, send, recv, **where):
        return pltpu.make_async_remote_copy(
            src_ref=ref, dst_ref=dst, send_sem=send, recv_sem=recv, device_id=where, device_id_type=MESH
        )

    def same(ref, send, recv, **where):
        return remote(ref, ref, send, recv, **where)

    def order(e, at, size):
        low = jnp.where(at < size // 2, 1, 0)
        at = low * at + (1 - low) * (size - 1 - at)
        paired = jnp.where(e % 2 == 1, at + (e + 1) // 2, at - e // 2)
        nth = jnp.where(e <= 2 * at, paired, e)
        return low * nth + (1 - low) * (size - 1 - nth)

    def rank_of(zi, at, size):
        low = jnp.where(at < size // 2, 1, 0)
        at = low * at + (1 - low) * (size - 1 - at)
        zi = low * zi + (1 - low) * (size - 1 - zi)
        return jnp.where(zi > 2 * at, zi, jnp.where(zi > at, 2 * (zi - at) - 1, 2 * (at - zi)))

    def is_late(zi, at, size):
        rank = rank_of(zi, at, size)
        edge = (at == 0) | (at + 1 == size)
        return (rank > size // 2) | (edge & ((rank == 1) | (rank > 2)))

    def settle(sem, elements):
        rows = elements // group
        tokens = tok_buf.shape[1]
        for size in [tokens] * (rows // tokens) + [rows % tokens] * (rows % tokens > 0):
            same(tok_buf.at[0, 0:size], sem, sem, wa=sibling).wait_send()

    class Line:
        def __init__(self, ref_of, at, size, sems):
            self.ref_of, self.at, self.size = ref_of, at, size
            self.l_send, self.l_recv, self.b_send, self.b_recv = sems

        def hop(self, way, *unit):
            to = me + 4 * (1 - 2 * way)
            return same(self.ref_of(core, *unit), self.l_send, self.l_recv.at[unit], wa=to)

        def up(self, zi):
            return (zi <= self.at) & (self.at + 1 < self.size)

        def down(self, zi):
            return (zi >= self.at) & (self.at > 0)

        def push(self, t, zi, yy):
            @pl.when(self.up(zi))
            def _():
                self.hop(0, t, zi, yy).start()

            @pl.when(self.down(zi))
            def _():
                self.hop(1, t, zi, yy).start()

        def arrive(self, t, zi, yy):
            self.hop(0, t, zi, yy).wait_recv()

        def give(self, t, zi, yy):
            return same(self.ref_of(core, t, zi, yy), self.b_send, self.b_recv(t, zi, yy), wa=sibling)

        def given(self, t, zi, yy):
            return same(self.ref_of(1 - core, t, zi, yy), self.b_send, self.b_recv(t, zi, yy), wa=sibling)

        def spread(self, t, zi, yy):
            self.push(t, zi, yy)
            self.give(t, zi, yy).start()

        def serve(self, t, zi, yy):
            self.arrive(t, zi, yy)
            self.spread(t, zi, yy)

        def drain(self, kinds):
            edge = (self.at == 0) | (self.at + 1 == self.size)
            unit = 2 * kinds * fd * q

            @pl.when(edge)
            def _():
                settle(self.l_send, unit)

            @pl.when(jnp.logical_not(edge))
            def _():
                settle(self.l_send, (self.size + 1) * unit)

            settle(self.b_send, self.size * unit)

    first = Line(lambda c, t, zi, yy: w1.at[t, zi, yy, c], zl, span, (l1_send, l1_recv, b1_send, lambda t, zi, yy: b1_recv.at[zi]))
    second = Line(lambda c, t, zi, yy: w2.at[zi, yy, c], z, zs, (l2_send, l2_recv, b2_send, lambda t, zi, yy: b2_recv.at[zi, yy]))

    def exchange(t):
        dst, recv = (w2.at[z, y, core], l2_recv.at[0, z, y]) if t == 2 else (w1.at[t, zl, y, core], l1_recv.at[t, zl, y])
        return remote(stage.at[t], dst, e_send, recv, wa=beside)

    def count_copy(k):
        return remote(count, counts.at[me], c_sem.at[0], c_sem.at[1], wa=lax.rem(me + k, n))

    def all_counts():
        return same(counts.at[pl.ds(0, n - 1)], c_sem.at[0], c_sem.at[1], wa=sibling)

    def columns(ref, index):
        return ref.at[:, pl.ds(pl.multiple_of(index * q, 128), q)]

    weights = (gate_ref, up_ref, down_ref)
    homes = (w1.at[0, zl, y, core], w1.at[1, zl, y, core], w2.at[z, y, core])
    loads = []
    for t in range(3):
        loads.append((
            pltpu.make_async_copy(columns(weights[t], 1 - y), stage.at[t], load_sem.at[t]),
            pltpu.make_async_copy(columns(weights[t], y), homes[t], load_sem.at[t]),
        ))

    def loaded(t):
        pltpu.make_async_copy(w1.at[0, 0, 0], w1.at[0, 0, 0], load_sem.at[t]).wait()

    def tok_load(i):
        column = (1 - half) * span + ha * sub + i if i < sub else half * span + i - sub
        return pltpu.make_async_copy(
            tok_ref.at[:, pl.ds(pl.multiple_of(column * group, 128), group)], tok_buf.at[i], tok_sem.at[i]
        )

    routing = [
        pltpu.make_async_copy(ref, buf, route_sem.at[k])
        for k, (ref, buf) in enumerate(((ids_ref, ids), (keep_ref, keep), (route_ref, weight)))
    ]
    for copy in (*loads[0], *routing):
        copy.start()
    for i in range(sub):
        tok_load(i).start()
    for load in (*loads[1], *loads[2]):
        load.start()
    for i in range(sub, sub + span):
        tok_load(i).start()

    barrier = pltpu.get_barrier_semaphore()

    @pl.loop(1, n)
    def _(k):
        pl.semaphore_signal(barrier, inc=1, device_id={"wa": lax.rem(me + k, n)}, device_id_type=MESH)

    pl.semaphore_signal(barrier, inc=1, device_id={"ha": 1 - ha}, device_id_type=MESH)

    pl.semaphore_wait(barrier, n)

    def direct(ref, yy, sems, k, **where):
        return same(ref.at[pl.ds(ha * sub, sub), yy], sems[0], sems[1].at[k], **where)

    def other(ref, yy, sems, k, **where):
        return same(ref.at[pl.ds((1 - ha) * sub, sub), yy], sems[0], sems[1].at[k], **where)

    g_sems = (g_send, g_recv)
    to_x = {"ha": 1 - ha}
    to_y = {"wa": beside}
    guest_send = remote(guest_out, guest_rows.at[pl.ds(ha * sub, sub), y], g_send, g_recv.at[0], wa=mirror)
    guest_y, guest_y_got = direct(guest_rows, y, g_sems, 1, **to_y), direct(guest_rows, 1 - y, g_sems, 1, **to_y)
    guest_x, guest_x_got = direct(guest_rows, y, g_sems, 2, **to_x), other(guest_rows, y, g_sems, 2, **to_x)
    guest_d, guest_d_got = direct(guest_rows, 1 - y, g_sems, 3, **to_x), other(guest_rows, 1 - y, g_sems, 3, **to_x)
    own_y, own_y_got = direct(own_rows, y, g_sems, 4, **to_y), direct(own_rows, 1 - y, g_sems, 4, **to_y)
    own_d, own_d_got = direct(own_rows, 1 - y, g_sems, 5, **to_x), other(own_rows, 1 - y, g_sems, 5, **to_x)

    def line_in(e):
        zi = order(e, zl, span)
        for yy in (y, 1 - y):
            for t in (0, 1):
                first.serve(t, zi, yy)

    def line_all(e):
        zi = order(e, zl, span)
        same(w1.at[:, zi, :, 1 - core], b1_send, b1_recv.at[zi], wa=sibling).wait_recv()

    def line2_in(e):
        zi = order(e, z, zs)
        for yy in (0, 1):
            second.serve(0, zi, yy)

    def project(rows, e, t):
        zi = order(e, zl, span)
        return jnp.dot(rows(zi), w1[t, zi].reshape(group, q), preferred_element_type=jnp.float32)

    def guests(yy):
        return lambda zi: guest_rows[zi, yy]

    def mine(zi):
        return own_rows[zi].reshape(2 * CAP, group)

    def partial(yy):
        return remote(part_out.at[yy], part_in.at[yy], p_send, p_recv.at[yy], wa=mirror)

    loaded(0)
    exchange(0).start()
    first.spread(0, zl, y)
    for copy in routing:
        copy.wait()
    matches = (ids[...] == 0) & (keep[...] == 1)
    chosen = jnp.minimum(jnp.sum(jnp.where(matches, 1, 0), axis=0, keepdims=True), 1)
    route_sum = jnp.sum(jnp.where(matches, weight[...], jnp.float32(0.0)), axis=0, keepdims=True)
    length = chosen.shape[1]
    lane = lax.broadcasted_iota(jnp.int32, (8, length), 1)
    running = jnp.broadcast_to(chosen, (8, length))
    shift = 1
    while shift < length:
        running = running + jnp.where(lane >= shift, pltpu.roll(running, shift, 1), 0)
        shift *= 2
    place = jnp.where(chosen == 1, running[0:1] - 1, -1)
    place_buf[...] = place
    place_copy = pltpu.make_async_copy(place_buf, place_ref, route_sem.at[3])
    place_copy.start()
    count[...] = jnp.broadcast_to(jnp.sum(chosen, axis=1, keepdims=True), count.shape)
    slot_ids = lax.broadcasted_iota(jnp.int32, (CAP, length), 0)
    hit = place == slot_ids
    table = jnp.where(hit, jnp.float32(1.0), jnp.float32(0.0)).astype(jnp.bfloat16)
    for i in range(sub):
        tok_load(i).wait()
        guest_out[i] = jnp.dot(table, tok_buf[i], preferred_element_type=jnp.float32).astype(jnp.bfloat16)
    guest_send.start()
    loaded(1)
    exchange(1).start()
    first.spread(1, zl, y)
    loaded(2)
    exchange(2).start()
    slot_route = jnp.sum(jnp.where(hit, route_sum, jnp.float32(0.0)), axis=1, keepdims=True)
    route[...] = jnp.broadcast_to(slot_route, route.shape)
    for i in range(span):
        tok_load(sub + i).wait()
        own_rows[i, y] = jnp.dot(
            table, tok_buf[sub + i], preferred_element_type=jnp.float32
        ).astype(jnp.bfloat16)

    @pl.loop(1, n)
    def _(k):
        count_copy(k).start()

    for t in (0, 1):
        first.serve(t, zl, 1 - y)
    second.spread(0, z, y)
    guest_send.wait_recv()
    guest_y.start()
    guest_x.start()
    own_y.start()
    second.serve(0, z, 1 - y)
    line_all(0)
    guest_y_got.wait_recv()
    guest_d.start()
    guest_x_got.wait_recv()
    for t in (0, 1):
        guest_acc[t] = project(guests(y), 0, t)
    for e in range(1, span):
        line_in(e)
        line_all(e)
        if e + 1 < span:
            for t in (0, 1):
                guest_acc[t] = guest_acc[t] + project(guests(y), e, t)
    for t in (0, 1):
        part_out[y, t] = (guest_acc[t] + project(guests(y), span - 1, t)).astype(jnp.bfloat16)
    partial(y).start()
    middle = (z > 0) & (z + 1 < zs)

    @pl.when(middle)
    def _():
        line2_in(1)

    own_y_got.wait_recv()
    own_d.start()
    guest_d_got.wait_recv()
    for t in (0, 1):
        total = project(guests(1 - y), 0, t)
        for e in range(1, span):
            total = total + project(guests(1 - y), e, t)
        part_out[1 - y, t] = total.astype(jnp.bfloat16)
    partial(1 - y).start()

    @pl.when(jnp.logical_not(middle))
    def _():
        line2_in(1)

    @pl.when(middle)
    def _():
        @pl.loop(2, span + 1)
        def _(e):
            line2_in(e)

    own_d_got.wait_recv()
    for t in (0, 1):
        total = project(mine, 0, t)
        for e in range(1, span):
            total = total + project(mine, e, t)
        own_acc[t] = total
    for yy in (0, 1):
        partial(yy).wait_recv()
    for yy in (0, 1):
        gate = own_acc[0, yy * CAP:(yy + 1) * CAP] + part_in[yy, 0].astype(jnp.float32)
        up = own_acc[1, yy * CAP:(yy + 1) * CAP] + part_in[yy, 1].astype(jnp.float32)
        hidden[yy] = (gate / (1.0 + jnp.exp(-gate)) * up).astype(jnp.bfloat16)

    def swap_x(j):
        return remote(x_out.at[j], x_in.at[j], x_send.at[j], x_recv.at[j], ha=1 - ha)

    def swap_y(zi, yy):
        return remote(y_out.at[yy, zi], y_in.at[yy, zi], y_send, y_recv.at[yy, zi], wa=beside)

    def swap_part(zi, yy, c):
        return remote(y_out.at[yy, zi, c], y_in.at[yy, zi, c], y_send, part_recv.at[0, yy, c], wa=beside)

    def swap_part_x(j, yy, c):
        return remote(
            yx_out.at[yy, j, c], yx_in.at[yy, j, c], part_send.at[yy, c], part_recv.at[1, yy, c], ha=1 - ha
        )

    def swap_xy(j):
        return remote(xy_out.at[j], xy_in.at[j], xy_send.at[j], xy_recv.at[j], wa=beside)

    def swap_yx(j, yy):
        return remote(yx_out.at[yy, j], yx_in.at[yy, j], yx_send.at[yy, j], yx_recv.at[yy, j], ha=1 - ha)

    def mine_rows(v):
        return jnp.where(y == 0, v[:CAP], v[CAP:]), jnp.where(y == 0, v[CAP:], v[:CAP])

    def down(zi, yy):
        return lax.dot_general(
            hidden[...].reshape(2 * CAP, q), w2[zi, yy].reshape(2 * fd, q), (((1,), (1,)), ((), ())),
            preferred_element_type=jnp.float32,
        )

    def place_of(e):
        zi = order(e, z, zs)
        out = zi // span
        return zi, out, zi - out * span

    def finish_x(e):
        zi, out, j = place_of(e)
        second.given(0, zi, 0).wait_recv()
        part = down(zi, 0)

        @pl.when(out == ha)
        def _():
            x_own[j] = part

        @pl.when(out != ha)
        def _():
            x_out[j] = part.astype(jnp.bfloat16)
            swap_x(j).start()

    def finish_y(e, yy):
        zi, out, j = place_of(e)
        second.given(0, zi, yy).wait_recv()
        keep, leave = mine_rows(down(zi, yy))
        for c in (0, 1):
            y_out[yy, zi, c] = leave[:, c * fd:(c + 1) * fd].astype(jnp.bfloat16)
        swap_y(zi, yy).start()
        for c in (0, 1):
            y_own[yy, zi, c] = keep[:, c * fd:(c + 1) * fd]

    def combine_x(e):
        zi, out, j = place_of(e)

        @pl.when(out == ha)
        def _():
            swap_x(j).wait_recv()
            keep, leave = mine_rows(x_own[j] + x_in[j].astype(jnp.float32))
            xy_own[j] = keep
            xy_out[j] = leave.astype(jnp.bfloat16)
            swap_xy(j).start()

    def combine_y(e, yy):
        zi, out, j = place_of(e)
        swap_y(zi, yy).wait_recv()
        total = y_own[yy, zi] + y_in[yy, zi].astype(jnp.float32)

        @pl.when(out != ha)
        def _():
            yx_out[yy, j] = total.astype(jnp.bfloat16)
            swap_yx(j, yy).start()

        @pl.when(out == ha)
        def _():
            y_own[yy, zi] = total

    def finish_last(yy):
        zi, out, j = place_of(zs - 1)
        second.serve(0, zi, yy)
        for c in (core, 1 - core):
            if c is not core:
                second.given(0, zi, yy).wait_recv()
            keep, leave = mine_rows(lax.dot_general(
                hidden[...].reshape(2 * CAP, q), w2[zi, yy, c], (((1,), (1,)), ((), ())),
                preferred_element_type=jnp.float32,
            ))
            y_out[yy, zi, c] = leave.astype(jnp.bfloat16)
            swap_part(zi, yy, c).start()
            y_own[yy, zi, c] = keep

    def combine_last(yy):
        zi, out, j = place_of(zs - 1)
        for c in (core, 1 - core):
            swap_part(zi, yy, c).wait_recv()
            total = y_own[yy, zi, c] + y_in[yy, zi, c].astype(jnp.float32)

            @pl.when(out != ha)
            def _():
                yx_out[yy, j, c] = total.astype(jnp.bfloat16)
                swap_part_x(j, yy, c).start()

            @pl.when(out == ha)
            def _():
                y_own[yy, zi, c] = total

    def late(e, yy):
        second.serve(0, order(e, z, zs), yy)
        finish_y(e, yy)

    @pl.when(middle)
    def _():
        @pl.loop(0, span + 1)
        def _(e):
            finish_x(e)
            finish_y(e, 1)

        @pl.loop(span + 1, zs - 1)
        def _(e):
            late(e, 0)
            late(e, 1)

        finish_last(0)
        finish_last(1)

        @pl.loop(0, span + 1)
        def _(e):
            combine_y(e, 1)
            combine_x(e)

        @pl.loop(span + 1, zs - 1)
        def _(e):
            combine_y(e, 0)
            combine_y(e, 1)

        combine_last(0)
        combine_last(1)

    @pl.when(jnp.logical_not(middle))
    def _():
        finish_y(0, 1)
        finish_x(0)
        finish_y(1, 0)
        finish_y(1, 1)
        second.serve(0, order(2, z, zs), 0)
        finish_x(2)
        late(2, 1)
        combine_y(0, 1)
        combine_x(0)
        combine_y(1, 0)

        @pl.loop(3, zs - 1)
        def _(e):
            late(e, 0)
            late(e, 1)
            combine_y(e, 0)
            combine_y(e, 1)

        finish_last(0)
        combine_y(1, 1)
        combine_y(2, 1)
        combine_x(2)
        finish_last(1)
        combine_last(0)
        combine_last(1)

    all_counts().wait_recv()

    counts[me] = jnp.zeros(counts.shape[1:], jnp.int32)

    def add_count(i, total):
        return total + jnp.where(i < me, counts[i], 0)

    earlier = lax.fori_loop(0, n, add_count, jnp.zeros(counts.shape[1:], jnp.int32))
    slot = lax.broadcasted_iota(jnp.int32, (CAP, 1), 0)
    scale = jnp.where(slot + earlier[0:1, 0:1] < n // 2 * CAP, route[:, 0:1], jnp.float32(0.0))
    width = 2 * span * wide
    cut = wide if wide % 128 == 0 else width

    def out_copy(u):
        return pltpu.make_async_copy(y_buf.at[:, u * cut:(u + 1) * cut], y_ref.at[:, u * cut:(u + 1) * cut], out_sem)

    def put(u, total):
        y_buf[:, u * wide:(u + 1) * wide] = (total * scale).astype(jnp.bfloat16)

    def put_y(u, zi, yy, j):
        for c in (0, 1):
            total = y_own[yy, zi, c] + yx_in[yy, j, c].astype(jnp.float32)
            y_buf[:, u * wide + c * fd:u * wide + (c + 1) * fd] = (total * scale).astype(jnp.bfloat16)

    for yy in (1, 0):
        for j in range(span):
            zi = ha * span + j
            u = 2 * j + yy
            final = rank_of(zi, z, zs) == zs - 1
            split = is_late(zi, z, zs) if yy == 0 else final | True

            @pl.when(final)
            def _():
                for c in (core, 1 - core):
                    swap_part_x(j, yy, c).wait_recv()

            @pl.when(split & jnp.logical_not(final))
            def _():
                swap_yx(j, yy).wait_recv()

            @pl.when(split)
            def _():
                put_y(u, zi, yy, j)

            if yy == 0:
                @pl.when(jnp.logical_not(split))
                def _():
                    swap_xy(j).wait_recv()
                    put(u, xy_own[j] + xy_in[j].astype(jnp.float32))

            if cut == wide:
                out_copy(u).start()

    if cut != wide:
        out_copy(0).start()

    all_counts().wait_send()

    place_copy.wait()
    settle(e_send, 3 * fd * q)
    settle(g_send, 6 * sub * CAP * group)
    settle(p_send, 4 * CAP * q)
    first.drain(2)
    second.drain(1)

    @pl.when(middle)
    def _():
        settle(y_send, (zs + zs - 1 - span) * CAP * wide)

    @pl.when(jnp.logical_not(middle))
    def _():
        settle(y_send, (2 * zs - 2) * CAP * wide)

    @pl.loop(0, zs)
    def _(e):
        zi, out, j = place_of(e)
        split = is_late(zi, z, zs)

        @pl.when((out != ha) & (e < zs - 1))
        def _():
            swap_yx(j, 1).wait_send()

        @pl.when((out != ha) & (e < zs - 1) & split)
        def _():
            swap_yx(j, 0).wait_send()

        @pl.when((out != ha) & (e == zs - 1))
        def _():
            for yy in (0, 1):
                for c in (0, 1):
                    swap_part_x(j, yy, c).wait_send()

        @pl.when((out != ha) & jnp.logical_not(split))
        def _():
            swap_x(j).wait_send()

        @pl.when((out == ha) & jnp.logical_not(split))
        def _():
            swap_xy(j).wait_send()

    pltpu.make_async_copy(y_buf, y_ref, out_sem).wait()


def expert(ids, keep, weight, tokens, gate, up, down):
    n = lax.axis_size("wa")
    fd, hid = gate.shape
    q = hid // 2
    zs = n // 4
    span = zs // 2
    sub = span // 2
    group = 4 * fd
    wide = 2 * fd
    any_spec = pl.BlockSpec(memory_space=pl.ANY)
    dma = pltpu.SemaphoreType.DMA
    bf16, f32 = jnp.bfloat16, jnp.float32
    return pl.pallas_call(
        functools.partial(expert_kernel, n),
        out_shape=(
            jax.ShapeDtypeStruct((CAP, span * group), bf16), jax.ShapeDtypeStruct((1, tokens.shape[0]), jnp.int32)
        ),
        in_specs=[any_spec] * 7,
        out_specs=(any_spec, any_spec),
        scratch_shapes=[
            pltpu.VMEM(ids.shape, jnp.int32),
            pltpu.VMEM(ids.shape, jnp.int32),
            pltpu.VMEM(ids.shape, f32),
            pltpu.VMEM((1, tokens.shape[0]), jnp.int32),
            pltpu.VMEM((2, span, 2, 2, fd, q), bf16),
            pltpu.VMEM((zs, 2, 2, fd, q), bf16),
            pltpu.VMEM((3, fd, q), bf16),
            pltpu.VMEM((sub + span, tokens.shape[0], group), bf16),
            pltpu.VMEM((sub, CAP, group), bf16),
            pltpu.VMEM((span, 2, CAP, group), bf16),
            pltpu.VMEM((span, 2, CAP, group), bf16),
            pltpu.VMEM((2, 2 * CAP, q), f32),
            pltpu.VMEM((2, CAP, q), f32),
            pltpu.VMEM((2, 2, CAP, q), bf16),
            pltpu.VMEM((2, 2, CAP, q), bf16),
            pltpu.VMEM((2, CAP, q), bf16),
            pltpu.VMEM((span, 2 * CAP, wide), f32),
            pltpu.VMEM((span, 2 * CAP, wide), bf16),
            pltpu.VMEM((span, 2 * CAP, wide), bf16),
            pltpu.VMEM((2, zs, 2, CAP, fd), f32),
            pltpu.VMEM((2, zs, 2, CAP, fd), bf16),
            pltpu.VMEM((2, zs, 2, CAP, fd), bf16),
            pltpu.VMEM((span, CAP, wide), f32),
            pltpu.VMEM((span, CAP, wide), bf16),
            pltpu.VMEM((span, CAP, wide), bf16),
            pltpu.VMEM((2, span, 2, CAP, fd), bf16),
            pltpu.VMEM((2, span, 2, CAP, fd), bf16),
            pltpu.VMEM((CAP, 2 * span * wide), bf16),
            pltpu.VMEM((8, 128), jnp.int32),
            pltpu.VMEM((n, 8, 128), jnp.int32),
            pltpu.VMEM((CAP, 128), f32),
            dma((3,)), dma((sub + span,)), dma((2,)), dma,
            dma, dma((2, span, 2)), dma, dma((span,)),
            dma, dma((1, zs, 2)), dma, dma((zs, 2)),
            dma, dma((6,)), dma, dma((2,)),
            dma((span,)), dma((span,)), dma, dma((2, zs)),
            dma((span,)), dma((span,)), dma((2, span)), dma((2, span)), dma((2, 2)), dma((2, 2, 2)), dma, dma((4,)),
        ],
        compiler_params=pltpu.CompilerParams(
            collective_id=0, has_side_effects=True, vmem_limit_bytes=60 * 1024 * 1024
        ),
    )(ids, keep, weight, tokens, gate, up, down)


def combine_kernel(place_ref, y_ref, out_ref, rows, block, in_sem, out_sem):
    count, tokens, wide = block.shape
    loads = [
        pltpu.make_async_copy(y_ref.at[:, k * wide:(k + 1) * wide], rows.at[k], in_sem.at[k]) for k in range(count)
    ]
    for load in loads:
        load.start()
    slots = lax.broadcasted_iota(jnp.int32, (CAP, tokens), 0)
    pick = jnp.where(place_ref[...] == slots, jnp.float32(1.0), jnp.float32(0.0)).astype(jnp.bfloat16).T
    stores = []
    for k in range(count):
        loads[k].wait()
        block[k] = jnp.dot(pick, rows[k], preferred_element_type=jnp.float32).astype(jnp.bfloat16)
        stores.append(pltpu.make_async_copy(block.at[k], out_ref.at[:, k * wide:(k + 1) * wide], out_sem.at[k]))
        stores[k].start()
    for store in stores:
        store.wait()


def combine(place, y):
    tokens, width = place.shape[1], y.shape[1]
    wide = 512 if width % 512 == 0 else width
    count = width // wide
    any_spec = pl.BlockSpec(memory_space=pl.ANY)
    dma = pltpu.SemaphoreType.DMA
    return pl.pallas_call(
        combine_kernel,
        out_shape=jax.ShapeDtypeStruct((tokens, width), jnp.bfloat16),
        in_specs=[pl.BlockSpec(memory_space=pltpu.VMEM), any_spec],
        out_specs=any_spec,
        scratch_shapes=[
            pltpu.VMEM((count, CAP, wide), jnp.bfloat16),
            pltpu.VMEM((count, tokens, wide), jnp.bfloat16),
            dma((count,)), dma((count,)),
        ],
    )(place, y)


def per_device(tokens, expert_ids, keep_mask, route_weight, gate_weight, up_weight, down_weight):
    y, place = expert(expert_ids.T, keep_mask.T, route_weight.T, tokens, gate_weight, up_weight, down_weight)
    return combine(place, y)


def solution(mesh):
    return jax.shard_map(
        per_device,
        mesh=mesh,
        in_specs=(
            P("wa", None),
            P("wa", None),
            P("wa", None),
            P("wa", None),
            P("wa", "ha"),
            P("wa", "ha"),
            P("wa", "ha"),
        ),
        out_specs=P("wa", "ha"),
        check_vma=False,
    )
```

```python
import functools

import jax
import jax.numpy as jnp
from jax import lax
from jax.experimental import pallas as pl
from jax.experimental.pallas import tpu as pltpu
from jax.sharding import PartitionSpec as P

CAP = 128
MESH = pl.DeviceIdType.MESH


def expert_kernel(
    n,
    ids_ref, keep_ref, route_ref, tok_ref, gate_ref, up_ref, down_ref,
    y_ref, place_ref,
    ids, keep, weight, place_buf, w1, w2, stage, tok_buf, guest_out, own_rows, guest_rows, own_acc, guest_acc, part_out, part_in, hidden,
    x_own, x_out, x_in, y_own, y_out, y_in, xy_own, xy_out, xy_in, yx_out, yx_in, y_buf, count, counts, route,
    load_sem, tok_sem, c_sem, e_send, l1_send, l1_recv, b1_send, b1_recv, l2_send, l2_recv, b2_send, b2_recv,
    g_send, g_recv, p_send, p_recv, x_send, x_recv, y_send, y_recv, xy_send, xy_recv, yx_send, yx_recv,
    part_send, part_recv, out_sem, route_sem,
):
    zs = n // 4
    span = zs // 2
    sub = span // 2
    me = lax.axis_index("wa")
    ha = lax.axis_index("ha")
    core = lax.rem(me, 2)
    y = lax.rem(me // 2, 2)
    z = me // 4
    half = z // span
    zl = z - half * span
    sibling = me + 1 - 2 * core
    beside = me + 2 - 4 * y
    mirror = lax.rem(me + n // 2, n)
    q = hidden.shape[2]
    fd = stage.shape[1]
    group = 4 * fd
    wide = 2 * fd

    def remote(ref, dst, send, recv, **where):
        return pltpu.make_async_remote_copy(
            src_ref=ref, dst_ref=dst, send_sem=send, recv_sem=recv, device_id=where, device_id_type=MESH
        )

    def same(ref, send, recv, **where):
        return remote(ref, ref, send, recv, **where)

    def order(e, at, size):
        low = jnp.where(at < size // 2, 1, 0)
        at = low * at + (1 - low) * (size - 1 - at)
        paired = jnp.where(e % 2 == 1, at + (e + 1) // 2, at - e // 2)
        nth = jnp.where(e <= 2 * at, paired, e)
        return low * nth + (1 - low) * (size - 1 - nth)

    def rank_of(zi, at, size):
        low = jnp.where(at < size // 2, 1, 0)
        at = low * at + (1 - low) * (size - 1 - at)
        zi = low * zi + (1 - low) * (size - 1 - zi)
        return jnp.where(zi > 2 * at, zi, jnp.where(zi > at, 2 * (zi - at) - 1, 2 * (at - zi)))

    def y_first(zi, yy):
        rank = rank_of(zi, z, zs)
        edge = (z == 0) | (z + 1 == zs)
        if yy == 1:
            return jnp.logical_not(edge & (rank == 2))
        return (rank > span) | (edge & ((rank == 1) | (rank > 2)))

    def settle(sem, elements):
        rows = elements // group
        tokens = tok_buf.shape[1]
        for size in [tokens] * (rows // tokens) + [rows % tokens] * (rows % tokens > 0):
            same(tok_buf.at[0, 0:size], sem, sem, wa=sibling).wait_send()

    class Line:
        def __init__(self, ref_of, at, size, sems):
            self.ref_of, self.at, self.size = ref_of, at, size
            self.l_send, self.l_recv, self.b_send, self.b_recv = sems

        def hop(self, way, *unit):
            to = me + 4 * (1 - 2 * way)
            return same(self.ref_of(core, *unit), self.l_send, self.l_recv.at[unit], wa=to)

        def up(self, zi):
            return (zi <= self.at) & (self.at + 1 < self.size)

        def down(self, zi):
            return (zi >= self.at) & (self.at > 0)

        def push(self, t, zi, yy):
            @pl.when(self.up(zi))
            def _():
                self.hop(0, t, zi, yy).start()

            @pl.when(self.down(zi))
            def _():
                self.hop(1, t, zi, yy).start()

        def arrive(self, t, zi, yy):
            self.hop(0, t, zi, yy).wait_recv()

        def give(self, t, zi, yy):
            return same(self.ref_of(core, t, zi, yy), self.b_send, self.b_recv(t, zi, yy), wa=sibling)

        def given(self, t, zi, yy):
            return same(self.ref_of(1 - core, t, zi, yy), self.b_send, self.b_recv(t, zi, yy), wa=sibling)

        def spread(self, t, zi, yy):
            self.push(t, zi, yy)
            self.give(t, zi, yy).start()

        def serve(self, t, zi, yy):
            self.arrive(t, zi, yy)
            self.spread(t, zi, yy)

        def drain(self, kinds):
            edge = (self.at == 0) | (self.at + 1 == self.size)
            unit = 2 * kinds * fd * q

            @pl.when(edge)
            def _():
                settle(self.l_send, unit)

            @pl.when(jnp.logical_not(edge))
            def _():
                settle(self.l_send, (self.size + 1) * unit)

            settle(self.b_send, self.size * unit)

    first = Line(lambda c, t, zi, yy: w1.at[t, zi, yy, c], zl, span, (l1_send, l1_recv, b1_send, lambda t, zi, yy: b1_recv.at[zi]))
    second = Line(lambda c, t, zi, yy: w2.at[zi, yy, c], z, zs, (l2_send, l2_recv, b2_send, lambda t, zi, yy: b2_recv.at[zi, yy]))

    def exchange(t):
        dst, recv = (w2.at[z, y, core], l2_recv.at[0, z, y]) if t == 2 else (w1.at[t, zl, y, core], l1_recv.at[t, zl, y])
        return remote(stage.at[t], dst, e_send, recv, wa=beside)

    def count_copy(k):
        return remote(count, counts.at[me], c_sem.at[0], c_sem.at[1], wa=lax.rem(me + k, n))

    def all_counts():
        return same(counts.at[pl.ds(0, n - 1)], c_sem.at[0], c_sem.at[1], wa=sibling)

    def columns(ref, index):
        return ref.at[:, pl.ds(pl.multiple_of(index * q, 128), q)]

    weights = (gate_ref, up_ref, down_ref)
    homes = (w1.at[0, zl, y, core], w1.at[1, zl, y, core], w2.at[z, y, core])
    loads = []
    for t in range(3):
        loads.append((
            pltpu.make_async_copy(columns(weights[t], 1 - y), stage.at[t], load_sem.at[t]),
            pltpu.make_async_copy(columns(weights[t], y), homes[t], load_sem.at[t]),
        ))

    def loaded(t):
        pltpu.make_async_copy(w1.at[0, 0, 0], w1.at[0, 0, 0], load_sem.at[t]).wait()

    def tok_load(i):
        column = (1 - half) * span + ha * sub + i if i < sub else half * span + i - sub
        return pltpu.make_async_copy(
            tok_ref.at[:, pl.ds(pl.multiple_of(column * group, 128), group)], tok_buf.at[i], tok_sem.at[i]
        )

    routing = [
        pltpu.make_async_copy(ref, buf, route_sem.at[k])
        for k, (ref, buf) in enumerate(((ids_ref, ids), (keep_ref, keep), (route_ref, weight)))
    ]
    for copy in (*loads[0], *routing):
        copy.start()
    for i in range(sub):
        tok_load(i).start()
    for load in (*loads[1], *loads[2]):
        load.start()
    for i in range(sub, sub + span):
        tok_load(i).start()

    barrier = pltpu.get_barrier_semaphore()

    @pl.loop(1, n)
    def _(k):
        pl.semaphore_signal(barrier, inc=1, device_id={"wa": lax.rem(me + k, n)}, device_id_type=MESH)

    pl.semaphore_signal(barrier, inc=1, device_id={"ha": 1 - ha}, device_id_type=MESH)

    pl.semaphore_wait(barrier, n)

    def direct(ref, yy, sems, k, **where):
        return same(ref.at[pl.ds(ha * sub, sub), yy], sems[0], sems[1].at[k], **where)

    def other(ref, yy, sems, k, **where):
        return same(ref.at[pl.ds((1 - ha) * sub, sub), yy], sems[0], sems[1].at[k], **where)

    g_sems = (g_send, g_recv)
    to_x = {"ha": 1 - ha}
    to_y = {"wa": beside}
    guest_send = remote(guest_out, guest_rows.at[pl.ds(ha * sub, sub), y], g_send, g_recv.at[0], wa=mirror)
    guest_y, guest_y_got = direct(guest_rows, y, g_sems, 1, **to_y), direct(guest_rows, 1 - y, g_sems, 1, **to_y)
    guest_x, guest_x_got = direct(guest_rows, y, g_sems, 2, **to_x), other(guest_rows, y, g_sems, 2, **to_x)
    guest_d, guest_d_got = direct(guest_rows, 1 - y, g_sems, 3, **to_x), other(guest_rows, 1 - y, g_sems, 3, **to_x)
    own_y, own_y_got = direct(own_rows, y, g_sems, 4, **to_y), direct(own_rows, 1 - y, g_sems, 4, **to_y)
    own_d, own_d_got = direct(own_rows, 1 - y, g_sems, 5, **to_x), other(own_rows, 1 - y, g_sems, 5, **to_x)

    def line_in(e):
        zi = order(e, zl, span)
        for yy in (y, 1 - y):
            for t in (0, 1):
                first.serve(t, zi, yy)

    def line_all(e):
        zi = order(e, zl, span)
        same(w1.at[:, zi, :, 1 - core], b1_send, b1_recv.at[zi], wa=sibling).wait_recv()

    def line2_in(e):
        zi = order(e, z, zs)
        for yy in (0, 1):
            second.serve(0, zi, yy)

    def project(rows, e, t):
        zi = order(e, zl, span)
        return jnp.dot(rows(zi), w1[t, zi].reshape(group, q), preferred_element_type=jnp.float32)

    def guests(yy):
        return lambda zi: guest_rows[zi, yy]

    def mine(zi):
        return own_rows[zi].reshape(2 * CAP, group)

    def partial(yy):
        return remote(part_out.at[yy], part_in.at[yy], p_send, p_recv.at[yy], wa=mirror)

    loaded(0)
    exchange(0).start()
    first.spread(0, zl, y)
    for copy in routing:
        copy.wait()
    matches = (ids[...] == 0) & (keep[...] == 1)
    chosen = jnp.minimum(jnp.sum(jnp.where(matches, 1, 0), axis=0, keepdims=True), 1)
    route_sum = jnp.sum(jnp.where(matches, weight[...], jnp.float32(0.0)), axis=0, keepdims=True)
    length = chosen.shape[1]
    lane = lax.broadcasted_iota(jnp.int32, (8, length), 1)
    running = jnp.broadcast_to(chosen, (8, length))
    shift = 1
    while shift < length:
        running = running + jnp.where(lane >= shift, pltpu.roll(running, shift, 1), 0)
        shift *= 2
    place = jnp.where(chosen == 1, running[0:1] - 1, -1)
    place_buf[...] = place
    place_copy = pltpu.make_async_copy(place_buf, place_ref, route_sem.at[3])
    place_copy.start()
    count[...] = jnp.broadcast_to(jnp.sum(chosen, axis=1, keepdims=True), count.shape)
    slot_ids = lax.broadcasted_iota(jnp.int32, (CAP, length), 0)
    hit = place == slot_ids
    table = jnp.where(hit, jnp.float32(1.0), jnp.float32(0.0)).astype(jnp.bfloat16)
    for i in range(sub):
        tok_load(i).wait()
        guest_out[i] = jnp.dot(table, tok_buf[i], preferred_element_type=jnp.float32).astype(jnp.bfloat16)
    guest_send.start()
    loaded(1)
    exchange(1).start()
    first.spread(1, zl, y)
    loaded(2)
    exchange(2).start()
    slot_route = jnp.sum(jnp.where(hit, route_sum, jnp.float32(0.0)), axis=1, keepdims=True)
    route[...] = jnp.broadcast_to(slot_route, route.shape)
    for i in range(span):
        tok_load(sub + i).wait()
        own_rows[i, y] = jnp.dot(
            table, tok_buf[sub + i], preferred_element_type=jnp.float32
        ).astype(jnp.bfloat16)

    @pl.loop(1, n)
    def _(k):
        count_copy(k).start()

    for t in (0, 1):
        first.serve(t, zl, 1 - y)
    second.spread(0, z, y)
    guest_send.wait_recv()
    guest_y.start()
    guest_x.start()
    own_y.start()
    second.serve(0, z, 1 - y)
    line_all(0)
    guest_y_got.wait_recv()
    guest_d.start()
    guest_x_got.wait_recv()
    for t in (0, 1):
        guest_acc[t] = project(guests(y), 0, t)
    for e in range(1, span):
        line_in(e)
        line_all(e)
        if e + 1 < span:
            for t in (0, 1):
                guest_acc[t] = guest_acc[t] + project(guests(y), e, t)
    for t in (0, 1):
        part_out[y, t] = (guest_acc[t] + project(guests(y), span - 1, t)).astype(jnp.bfloat16)
    partial(y).start()
    middle = (z > 0) & (z + 1 < zs)

    @pl.when(middle)
    def _():
        line2_in(1)

    own_y_got.wait_recv()
    own_d.start()
    guest_d_got.wait_recv()
    for t in (0, 1):
        total = project(guests(1 - y), 0, t)
        for e in range(1, span):
            total = total + project(guests(1 - y), e, t)
        part_out[1 - y, t] = total.astype(jnp.bfloat16)
    partial(1 - y).start()

    @pl.when(jnp.logical_not(middle))
    def _():
        line2_in(1)

    @pl.when(middle)
    def _():
        @pl.loop(2, span + 1)
        def _(e):
            line2_in(e)

    own_d_got.wait_recv()
    for t in (0, 1):
        total = project(mine, 0, t)
        for e in range(1, span):
            total = total + project(mine, e, t)
        own_acc[t] = total
    for yy in (0, 1):
        partial(yy).wait_recv()
    for yy in (0, 1):
        gate = own_acc[0, yy * CAP:(yy + 1) * CAP] + part_in[yy, 0].astype(jnp.float32)
        up = own_acc[1, yy * CAP:(yy + 1) * CAP] + part_in[yy, 1].astype(jnp.float32)
        hidden[yy] = (gate / (1.0 + jnp.exp(-gate)) * up).astype(jnp.bfloat16)

    def swap_x(j, yy):
        return remote(x_out.at[yy, j], x_in.at[yy, j], x_send.at[yy, j], x_recv.at[yy, j], ha=1 - ha)

    def swap_y(zi, yy):
        return remote(y_out.at[yy, zi], y_in.at[yy, zi], y_send, y_recv.at[yy, zi], wa=beside)

    def swap_part(zi, yy, c):
        return remote(y_out.at[yy, zi, c], y_in.at[yy, zi, c], y_send, part_recv.at[0, yy, c], wa=beside)

    def swap_part_x(j, yy, c):
        return remote(
            yx_out.at[yy, j, c], yx_in.at[yy, j, c], part_send.at[yy, c], part_recv.at[1, yy, c], ha=1 - ha
        )

    def swap_xy(j, yy):
        return remote(xy_out.at[yy, j], xy_in.at[yy, j], xy_send.at[yy, j], xy_recv.at[yy, j], wa=beside)

    def swap_yx(j, yy):
        return remote(yx_out.at[yy, j], yx_in.at[yy, j], yx_send.at[yy, j], yx_recv.at[yy, j], ha=1 - ha)

    def mine_rows(v):
        return jnp.where(y == 0, v[:CAP], v[CAP:]), jnp.where(y == 0, v[CAP:], v[:CAP])

    def down(zi, yy):
        return lax.dot_general(
            hidden[...].reshape(2 * CAP, q), w2[zi, yy].reshape(2 * fd, q), (((1,), (1,)), ((), ())),
            preferred_element_type=jnp.float32,
        )

    def place_of(e):
        zi = order(e, z, zs)
        out = zi // span
        return zi, out, zi - out * span

    def finish_x(e, yy):
        zi, out, j = place_of(e)
        second.given(0, zi, yy).wait_recv()
        part = down(zi, yy)

        @pl.when(out == ha)
        def _():
            x_own[yy, j] = part

        @pl.when(out != ha)
        def _():
            x_out[yy, j] = part.astype(jnp.bfloat16)
            swap_x(j, yy).start()

    def finish_y(e, yy):
        zi, out, j = place_of(e)
        second.given(0, zi, yy).wait_recv()
        keep, leave = mine_rows(down(zi, yy))
        for c in (0, 1):
            y_out[yy, zi, c] = leave[:, c * fd:(c + 1) * fd].astype(jnp.bfloat16)
        swap_y(zi, yy).start()
        for c in (0, 1):
            y_own[yy, zi, c] = keep[:, c * fd:(c + 1) * fd]

    def combine_x(e, yy):
        zi, out, j = place_of(e)

        @pl.when(out == ha)
        def _():
            swap_x(j, yy).wait_recv()
            keep, leave = mine_rows(x_own[yy, j] + x_in[yy, j].astype(jnp.float32))
            xy_own[yy, j] = keep
            xy_out[yy, j] = leave.astype(jnp.bfloat16)
            swap_xy(j, yy).start()

    def combine_y(e, yy):
        zi, out, j = place_of(e)
        swap_y(zi, yy).wait_recv()
        total = y_own[yy, zi] + y_in[yy, zi].astype(jnp.float32)

        @pl.when(out != ha)
        def _():
            yx_out[yy, j] = total.astype(jnp.bfloat16)
            swap_yx(j, yy).start()

        @pl.when(out == ha)
        def _():
            y_own[yy, zi] = total

    def part_last(yy, c):
        zi, out, j = place_of(zs - 1)
        keep, leave = mine_rows(lax.dot_general(
            hidden[...].reshape(2 * CAP, q), w2[zi, yy, c], (((1,), (1,)), ((), ())),
            preferred_element_type=jnp.float32,
        ))
        y_out[yy, zi, c] = leave.astype(jnp.bfloat16)
        swap_part(zi, yy, c).start()
        y_own[yy, zi, c] = keep

    def start_last(yy):
        second.serve(0, order(zs - 1, z, zs), yy)
        part_last(yy, core)

    def end_last(yy):
        second.given(0, order(zs - 1, z, zs), yy).wait_recv()
        part_last(yy, 1 - core)

    def combine_last(yy):
        zi, out, j = place_of(zs - 1)
        for c in (core, 1 - core):
            swap_part(zi, yy, c).wait_recv()
            total = y_own[yy, zi, c] + y_in[yy, zi, c].astype(jnp.float32)

            @pl.when(out != ha)
            def _():
                yx_out[yy, j, c] = total.astype(jnp.bfloat16)
                swap_part_x(j, yy, c).start()

            @pl.when(out == ha)
            def _():
                y_own[yy, zi, c] = total

    def late(e, yy):
        second.serve(0, order(e, z, zs), yy)
        finish_y(e, yy)

    @pl.when(middle)
    def _():
        @pl.loop(0, span + 1)
        def _(e):
            finish_x(e, 0)
            finish_y(e, 1)

        @pl.loop(span + 1, zs - 1)
        def _(e):
            late(e, 0)
            late(e, 1)

        start_last(0)
        end_last(0)
        start_last(1)
        end_last(1)

        @pl.loop(0, span + 1)
        def _(e):
            combine_y(e, 1)
            combine_x(e, 0)

        @pl.loop(span + 1, zs - 1)
        def _(e):
            combine_y(e, 0)
            combine_y(e, 1)

        combine_last(0)
        combine_last(1)

    @pl.when(jnp.logical_not(middle))
    def _():
        finish_y(0, 1)
        finish_x(0, 0)
        finish_y(1, 0)
        finish_y(1, 1)
        second.serve(0, order(2, z, zs), 0)
        finish_x(2, 0)
        second.serve(0, order(2, z, zs), 1)
        finish_x(2, 1)
        combine_y(0, 1)
        combine_y(1, 0)

        @pl.loop(3, zs - 1)
        def _(e):
            late(e, 0)
            late(e, 1)
            combine_y(e, 0)
            combine_y(e, 1)

        start_last(0)
        combine_y(1, 1)
        end_last(0)
        combine_x(2, 0)
        start_last(1)
        end_last(1)
        combine_x(0, 0)
        combine_last(0)
        combine_last(1)
        combine_x(2, 1)

    all_counts().wait_recv()

    counts[me] = jnp.zeros(counts.shape[1:], jnp.int32)

    def add_count(i, total):
        return total + jnp.where(i < me, counts[i], 0)

    earlier = lax.fori_loop(0, n, add_count, jnp.zeros(counts.shape[1:], jnp.int32))
    slot = lax.broadcasted_iota(jnp.int32, (CAP, 1), 0)
    scale = jnp.where(slot + earlier[0:1, 0:1] < n // 2 * CAP, route[:, 0:1], jnp.float32(0.0))
    width = 2 * span * wide
    cut = wide if wide % 128 == 0 else width

    def out_copy(u):
        return pltpu.make_async_copy(y_buf.at[:, u * cut:(u + 1) * cut], y_ref.at[:, u * cut:(u + 1) * cut], out_sem)

    def put(u, total):
        y_buf[:, u * wide:(u + 1) * wide] = (total * scale).astype(jnp.bfloat16)

    def put_y(u, zi, yy, j):
        for c in (0, 1):
            total = y_own[yy, zi, c] + yx_in[yy, j, c].astype(jnp.float32)
            y_buf[:, u * wide + c * fd:u * wide + (c + 1) * fd] = (total * scale).astype(jnp.bfloat16)

    for yy in (1, 0):
        for j in range(span):
            zi = ha * span + j
            u = 2 * j + yy
            final = rank_of(zi, z, zs) == zs - 1
            split = y_first(zi, yy)

            @pl.when(final)
            def _():
                for c in (core, 1 - core):
                    swap_part_x(j, yy, c).wait_recv()

            @pl.when(split & jnp.logical_not(final))
            def _():
                swap_yx(j, yy).wait_recv()

            @pl.when(split)
            def _():
                put_y(u, zi, yy, j)

            @pl.when(jnp.logical_not(split))
            def _():
                swap_xy(j, yy).wait_recv()
                put(u, xy_own[yy, j] + xy_in[yy, j].astype(jnp.float32))

            if cut == wide:
                out_copy(u).start()

    if cut != wide:
        out_copy(0).start()

    all_counts().wait_send()

    place_copy.wait()
    settle(e_send, 3 * fd * q)
    settle(g_send, 6 * sub * CAP * group)
    settle(p_send, 4 * CAP * q)
    first.drain(2)
    second.drain(1)

    @pl.when(middle)
    def _():
        settle(y_send, (zs + zs - 1 - span) * CAP * wide)

    @pl.when(jnp.logical_not(middle))
    def _():
        settle(y_send, (2 * zs - 3) * CAP * wide)

    @pl.loop(0, zs)
    def _(e):
        zi, out, j = place_of(e)
        for yy in (0, 1):
            split = y_first(zi, yy)

            @pl.when((out != ha) & (e < zs - 1) & split)
            def _():
                swap_yx(j, yy).wait_send()

            @pl.when((out != ha) & (e == zs - 1))
            def _():
                for c in (0, 1):
                    swap_part_x(j, yy, c).wait_send()

            @pl.when((out != ha) & jnp.logical_not(split))
            def _():
                swap_x(j, yy).wait_send()

            @pl.when((out == ha) & jnp.logical_not(split))
            def _():
                swap_xy(j, yy).wait_send()

    pltpu.make_async_copy(y_buf, y_ref, out_sem).wait()


def expert(ids, keep, weight, tokens, gate, up, down):
    n = lax.axis_size("wa")
    fd, hid = gate.shape
    q = hid // 2
    zs = n // 4
    span = zs // 2
    sub = span // 2
    group = 4 * fd
    wide = 2 * fd
    any_spec = pl.BlockSpec(memory_space=pl.ANY)
    dma = pltpu.SemaphoreType.DMA
    bf16, f32 = jnp.bfloat16, jnp.float32
    return pl.pallas_call(
        functools.partial(expert_kernel, n),
        out_shape=(
            jax.ShapeDtypeStruct((CAP, span * group), bf16), jax.ShapeDtypeStruct((1, tokens.shape[0]), jnp.int32)
        ),
        in_specs=[any_spec] * 7,
        out_specs=(any_spec, any_spec),
        scratch_shapes=[
            pltpu.VMEM(ids.shape, jnp.int32),
            pltpu.VMEM(ids.shape, jnp.int32),
            pltpu.VMEM(ids.shape, f32),
            pltpu.VMEM((1, tokens.shape[0]), jnp.int32),
            pltpu.VMEM((2, span, 2, 2, fd, q), bf16),
            pltpu.VMEM((zs, 2, 2, fd, q), bf16),
            pltpu.VMEM((3, fd, q), bf16),
            pltpu.VMEM((sub + span, tokens.shape[0], group), bf16),
            pltpu.VMEM((sub, CAP, group), bf16),
            pltpu.VMEM((span, 2, CAP, group), bf16),
            pltpu.VMEM((span, 2, CAP, group), bf16),
            pltpu.VMEM((2, 2 * CAP, q), f32),
            pltpu.VMEM((2, CAP, q), f32),
            pltpu.VMEM((2, 2, CAP, q), bf16),
            pltpu.VMEM((2, 2, CAP, q), bf16),
            pltpu.VMEM((2, CAP, q), bf16),
            pltpu.VMEM((2, span, 2 * CAP, wide), f32),
            pltpu.VMEM((2, span, 2 * CAP, wide), bf16),
            pltpu.VMEM((2, span, 2 * CAP, wide), bf16),
            pltpu.VMEM((2, zs, 2, CAP, fd), f32),
            pltpu.VMEM((2, zs, 2, CAP, fd), bf16),
            pltpu.VMEM((2, zs, 2, CAP, fd), bf16),
            pltpu.VMEM((2, span, CAP, wide), f32),
            pltpu.VMEM((2, span, CAP, wide), bf16),
            pltpu.VMEM((2, span, CAP, wide), bf16),
            pltpu.VMEM((2, span, 2, CAP, fd), bf16),
            pltpu.VMEM((2, span, 2, CAP, fd), bf16),
            pltpu.VMEM((CAP, 2 * span * wide), bf16),
            pltpu.VMEM((8, 128), jnp.int32),
            pltpu.VMEM((n, 8, 128), jnp.int32),
            pltpu.VMEM((CAP, 128), f32),
            dma((3,)), dma((sub + span,)), dma((2,)), dma,
            dma, dma((2, span, 2)), dma, dma((span,)),
            dma, dma((1, zs, 2)), dma, dma((zs, 2)),
            dma, dma((6,)), dma, dma((2,)),
            dma((2, span)), dma((2, span)), dma, dma((2, zs)),
            dma((2, span)), dma((2, span)), dma((2, span)), dma((2, span)), dma((2, 2)), dma((2, 2, 2)), dma, dma((4,)),
        ],
        compiler_params=pltpu.CompilerParams(
            collective_id=0, has_side_effects=True, vmem_limit_bytes=60 * 1024 * 1024
        ),
    )(ids, keep, weight, tokens, gate, up, down)


def combine_kernel(place_ref, y_ref, out_ref, place, rows, block, in_sem, out_sem):
    steps, tall, _ = block.shape
    count, _, wide = rows.shape
    loads = [pltpu.make_async_copy(place_ref, place, in_sem.at[count])]
    for k in range(count):
        loads.append(pltpu.make_async_copy(y_ref.at[:, k * wide:(k + 1) * wide], rows.at[k], in_sem.at[k]))
    for load in loads:
        load.start()
    loads[0].wait()
    slots = lax.broadcasted_iota(jnp.int32, (CAP, steps * tall), 0)
    pick = jnp.where(place[...] == slots, jnp.float32(1.0), jnp.float32(0.0)).astype(jnp.bfloat16).T
    for load in loads[1:]:
        load.wait()
    stores = []
    for i in range(steps):
        for k in range(count):
            block[i, :, k * wide:(k + 1) * wide] = jnp.dot(
                pick[i * tall:(i + 1) * tall], rows[k], preferred_element_type=jnp.float32
            ).astype(jnp.bfloat16)
        stores.append(pltpu.make_async_copy(block.at[i], out_ref.at[i * tall:(i + 1) * tall], out_sem.at[i]))
        stores[i].start()
    for store in stores:
        store.wait()


def combine(place, y):
    tokens, width = place.shape[1], y.shape[1]
    wide = 512 if width % 512 == 0 else width
    tall = CAP if tokens % CAP == 0 else tokens
    count, steps = width // wide, tokens // tall
    any_spec = pl.BlockSpec(memory_space=pl.ANY)
    dma = pltpu.SemaphoreType.DMA
    return pl.pallas_call(
        combine_kernel,
        out_shape=jax.ShapeDtypeStruct((tokens, width), jnp.bfloat16),
        in_specs=[any_spec, any_spec],
        out_specs=any_spec,
        scratch_shapes=[
            pltpu.VMEM((1, tokens), jnp.int32),
            pltpu.VMEM((count, CAP, wide), jnp.bfloat16),
            pltpu.VMEM((steps, tall, width), jnp.bfloat16),
            dma((count + 1,)), dma((steps,)),
        ],
    )(place, y)


def per_device(tokens, expert_ids, keep_mask, route_weight, gate_weight, up_weight, down_weight):
    y, place = expert(expert_ids.T, keep_mask.T, route_weight.T, tokens, gate_weight, up_weight, down_weight)
    return combine(place, y)


def solution(mesh):
    return jax.shard_map(
        per_device,
        mesh=mesh,
        in_specs=(
            P("wa", None),
            P("wa", None),
            P("wa", None),
            P("wa", None),
            P("wa", "ha"),
            P("wa", "ha"),
            P("wa", "ha"),
        ),
        out_specs=P("wa", "ha"),
        check_vma=False,
    )
```

```python
import functools

import jax
import jax.numpy as jnp
from jax import lax
from jax.experimental import pallas as pl
from jax.experimental.pallas import tpu as pltpu
from jax.sharding import PartitionSpec as P

CAP = 128
MESH = pl.DeviceIdType.MESH


def expert_kernel(
    n,
    ids_ref, keep_ref, route_ref, tok_ref, gate_ref, up_ref, down_ref,
    y_ref, place_ref,
    ids, keep, weight, place_buf, w1, w2, stage, tok_buf, guest_out, own_rows, guest_rows, own_acc, part_out, part_in, hidden,
    x_own, x_out, x_in, y_own, y_out, y_in, xy_own, xy_out, xy_in, yx_out, yx_in, y_buf, count, counts, route,
    load_sem, tok_sem, c_sem, e_send, l1_send, l1_recv, b1_send, b1_recv, l2_send, l2_recv, b2_send, b2_recv,
    g_send, g_recv, p_send, p_recv, x_recv, y_send, y_recv, xy_recv, yx_recv,
    part_recv, out_sem, route_sem,
):
    zs = n // 4
    span = zs // 2
    sub = span // 2
    me = lax.axis_index("wa")
    ha = lax.axis_index("ha")
    core = lax.rem(me, 2)
    y = lax.rem(me // 2, 2)
    z = me // 4
    half = z // span
    zl = z - half * span
    sibling = me + 1 - 2 * core
    beside = me + 2 - 4 * y
    mirror = lax.rem(me + n // 2, n)
    q = hidden.shape[2]
    fd = stage.shape[1]
    group = 4 * fd
    wide = 2 * fd

    def remote(ref, dst, send, recv, **where):
        return pltpu.make_async_remote_copy(
            src_ref=ref, dst_ref=dst, send_sem=send, recv_sem=recv, device_id=where, device_id_type=MESH
        )

    def same(ref, send, recv, **where):
        return remote(ref, ref, send, recv, **where)

    def order(e, at, size):
        low = jnp.where(at < size // 2, 1, 0)
        at = low * at + (1 - low) * (size - 1 - at)
        paired = jnp.where(e % 2 == 1, at + (e + 1) // 2, at - e // 2)
        nth = jnp.where(e <= 2 * at, paired, e)
        return low * nth + (1 - low) * (size - 1 - nth)

    def rank_of(zi, at, size):
        low = jnp.where(at < size // 2, 1, 0)
        at = low * at + (1 - low) * (size - 1 - at)
        zi = low * zi + (1 - low) * (size - 1 - zi)
        return jnp.where(zi > 2 * at, zi, jnp.where(zi > at, 2 * (zi - at) - 1, 2 * (at - zi)))

    def y_first(zi, yy):
        rank = rank_of(zi, z, zs)
        edge = (z == 0) | (z + 1 == zs)
        if yy == 1:
            return rank >= 0
        return (rank > span) | (edge & ((rank == 1) | (rank > 2)))

    def settle(sem, elements):
        rows = elements // group
        tokens = tok_buf.shape[1]
        for size in [tokens] * (rows // tokens) + [rows % tokens] * (rows % tokens > 0):
            same(tok_buf.at[0, 0:size], sem, sem, wa=sibling).wait_send()

    class Line:
        def __init__(self, ref_of, at, size, sems):
            self.ref_of, self.at, self.size = ref_of, at, size
            self.l_send, self.l_recv, self.b_send, self.b_recv = sems

        def hop(self, way, *unit):
            to = me + 4 * (1 - 2 * way)
            return same(self.ref_of(core, *unit), self.l_send, self.l_recv.at[unit], wa=to)

        def up(self, zi):
            return (zi <= self.at) & (self.at + 1 < self.size)

        def down(self, zi):
            return (zi >= self.at) & (self.at > 0)

        def push(self, t, zi, yy):
            @pl.when(self.up(zi))
            def _():
                self.hop(0, t, zi, yy).start()

            @pl.when(self.down(zi))
            def _():
                self.hop(1, t, zi, yy).start()

        def arrive(self, t, zi, yy):
            self.hop(0, t, zi, yy).wait_recv()

        def give(self, t, zi, yy):
            return same(self.ref_of(core, t, zi, yy), self.b_send, self.b_recv(t, zi, yy), wa=sibling)

        def given(self, t, zi, yy):
            return same(self.ref_of(1 - core, t, zi, yy), self.b_send, self.b_recv(t, zi, yy), wa=sibling)

        def spread(self, t, zi, yy):
            self.push(t, zi, yy)
            self.give(t, zi, yy).start()

        def serve(self, t, zi, yy):
            self.arrive(t, zi, yy)
            self.spread(t, zi, yy)

        def drain(self, kinds):
            edge = (self.at == 0) | (self.at + 1 == self.size)
            unit = 2 * kinds * fd * q

            @pl.when(edge)
            def _():
                settle(self.l_send, unit)

            @pl.when(jnp.logical_not(edge))
            def _():
                settle(self.l_send, (self.size + 1) * unit)

            settle(self.b_send, self.size * unit)

    first = Line(lambda c, t, zi, yy: w1.at[t, zi, yy, c], zl, span, (l1_send, l1_recv, b1_send, lambda t, zi, yy: b1_recv.at[t, zi]))
    second = Line(lambda c, t, zi, yy: w2.at[zi, yy, c], z, zs, (l2_send, l2_recv, b2_send, lambda t, zi, yy: b2_recv.at[zi, yy]))

    def exchange(t):
        dst, recv = (w2.at[z, y, core], l2_recv.at[0, z, y]) if t == 2 else (w1.at[t, zl, y, core], l1_recv.at[t, zl, y])
        return remote(stage.at[t], dst, e_send, recv, wa=beside)

    def count_copy(k):
        return remote(count, counts.at[me], c_sem.at[0], c_sem.at[1], wa=lax.rem(me + k, n))

    def all_counts():
        return same(counts.at[pl.ds(0, n - 1)], c_sem.at[0], c_sem.at[1], wa=sibling)

    def columns(ref, index):
        return ref.at[:, pl.ds(pl.multiple_of(index * q, 128), q)]

    weights = (gate_ref, up_ref, down_ref)
    homes = (w1.at[0, zl, y, core], w1.at[1, zl, y, core], w2.at[z, y, core])
    loads = []
    for t in range(3):
        loads.append((
            pltpu.make_async_copy(columns(weights[t], 1 - y), stage.at[t], load_sem.at[t]),
            pltpu.make_async_copy(columns(weights[t], y), homes[t], load_sem.at[t]),
        ))

    def loaded(t):
        pltpu.make_async_copy(w1.at[0, 0, 0], w1.at[0, 0, 0], load_sem.at[t]).wait()

    def tok_load(i):
        column = (1 - half) * span + ha * sub + i if i < sub else half * span + i - sub
        return pltpu.make_async_copy(
            tok_ref.at[:, pl.ds(pl.multiple_of(column * group, 128), group)], tok_buf.at[i], tok_sem.at[i]
        )

    routing = [
        pltpu.make_async_copy(ref, buf, route_sem.at[k])
        for k, (ref, buf) in enumerate(((ids_ref, ids), (keep_ref, keep), (route_ref, weight)))
    ]
    for copy in (*loads[0], *routing):
        copy.start()
    for i in range(sub):
        tok_load(i).start()
    for load in (*loads[1], *loads[2]):
        load.start()
    for i in range(sub, sub + span):
        tok_load(i).start()

    barrier = pltpu.get_barrier_semaphore()

    @pl.loop(1, n)
    def _(k):
        pl.semaphore_signal(barrier, inc=1, device_id={"wa": lax.rem(me + k, n)}, device_id_type=MESH)

    pl.semaphore_signal(barrier, inc=1, device_id={"ha": 1 - ha}, device_id_type=MESH)

    pl.semaphore_wait(barrier, n)

    def direct(ref, yy, sems, k, **where):
        return same(ref.at[pl.ds(ha * sub, sub), yy], sems[0], sems[1].at[k], **where)

    def other(ref, yy, sems, k, **where):
        return same(ref.at[pl.ds((1 - ha) * sub, sub), yy], sems[0], sems[1].at[k], **where)

    g_sems = (g_send, g_recv)
    to_x = {"ha": 1 - ha}
    to_y = {"wa": beside}
    guest_send = remote(guest_out, guest_rows.at[pl.ds(ha * sub, sub), y], g_send, g_recv.at[0], wa=mirror)
    guest_y, guest_y_got = direct(guest_rows, y, g_sems, 1, **to_y), direct(guest_rows, 1 - y, g_sems, 1, **to_y)
    guest_x, guest_x_got = direct(guest_rows, y, g_sems, 2, **to_x), other(guest_rows, y, g_sems, 2, **to_x)
    guest_d, guest_d_got = direct(guest_rows, 1 - y, g_sems, 3, **to_x), other(guest_rows, 1 - y, g_sems, 3, **to_x)
    own_y, own_y_got = direct(own_rows, y, g_sems, 4, **to_y), direct(own_rows, 1 - y, g_sems, 4, **to_y)
    own_d, own_d_got = direct(own_rows, 1 - y, g_sems, 5, **to_x), other(own_rows, 1 - y, g_sems, 5, **to_x)

    def given_all(t, e):
        zi = order(e, zl, span)
        same(w1.at[t, zi, :, 1 - core], b1_send, b1_recv.at[t, zi], wa=sibling).wait_recv()

    def line2_in(e):
        zi = order(e, z, zs)
        for yy in (0, 1):
            second.serve(0, zi, yy)

    def project(rows, e, t):
        zi = order(e, zl, span)
        return jnp.dot(rows(zi), w1[t, zi].reshape(group, q), preferred_element_type=jnp.float32)

    def guests(yy):
        return lambda zi: guest_rows[zi, yy]

    def mine(zi):
        return own_rows[zi].reshape(2 * CAP, group)

    def partial(yy, t):
        return remote(part_out.at[yy, t], part_in.at[yy, t], p_send, p_recv.at[yy, t], wa=mirror)

    def serve_guest(yy, t):
        total = None
        for e in range(span):
            term = project(guests(yy), e, t)
            total = term if total is None else total + term
        part_out[yy, t] = total.astype(jnp.bfloat16)
        partial(yy, t).start()

    loaded(0)
    exchange(0).start()
    first.spread(0, zl, y)
    for copy in routing:
        copy.wait()
    matches = (ids[...] == 0) & (keep[...] == 1)
    chosen = jnp.minimum(jnp.sum(jnp.where(matches, 1, 0), axis=0, keepdims=True), 1)
    route_sum = jnp.sum(jnp.where(matches, weight[...], jnp.float32(0.0)), axis=0, keepdims=True)
    length = chosen.shape[1]
    lane = lax.broadcasted_iota(jnp.int32, (8, length), 1)
    running = jnp.broadcast_to(chosen, (8, length))
    shift = 1
    while shift < length:
        running = running + jnp.where(lane >= shift, pltpu.roll(running, shift, 1), 0)
        shift *= 2
    place = jnp.where(chosen == 1, running[0:1] - 1, -1)
    place_buf[...] = place
    place_copy = pltpu.make_async_copy(place_buf, place_ref, route_sem.at[3])
    place_copy.start()
    count[...] = jnp.broadcast_to(jnp.sum(chosen, axis=1, keepdims=True), count.shape)
    slot_ids = lax.broadcasted_iota(jnp.int32, (CAP, length), 0)
    hit = place == slot_ids
    table = jnp.where(hit, jnp.float32(1.0), jnp.float32(0.0)).astype(jnp.bfloat16)
    for i in range(sub):
        tok_load(i).wait()
        guest_out[i] = jnp.dot(table, tok_buf[i], preferred_element_type=jnp.float32).astype(jnp.bfloat16)
    guest_send.start()
    loaded(1)
    exchange(1).start()
    first.spread(1, zl, y)
    loaded(2)
    exchange(2).start()
    slot_route = jnp.sum(jnp.where(hit, route_sum, jnp.float32(0.0)), axis=1, keepdims=True)
    route[...] = jnp.broadcast_to(slot_route, route.shape)
    for i in range(span):
        tok_load(sub + i).wait()
        own_rows[i, y] = jnp.dot(
            table, tok_buf[sub + i], preferred_element_type=jnp.float32
        ).astype(jnp.bfloat16)

    @pl.loop(1, n)
    def _(k):
        count_copy(k).start()

    for t in (0, 1):
        first.serve(t, zl, 1 - y)
    second.spread(0, z, y)
    guest_send.wait_recv()
    guest_y.start()
    guest_x.start()
    own_y.start()
    second.serve(0, z, 1 - y)
    for t in (0, 1):
        given_all(t, 0)
    guest_y_got.wait_recv()
    guest_d.start()
    guest_x_got.wait_recv()
    for e in range(1, span):
        zi = order(e, zl, span)
        for t in (0, 1):
            first.serve(t, zi, y)
        first.serve(0, zi, 1 - y)
        given_all(0, e)
    serve_guest(y, 0)
    for e in range(1, span):
        first.serve(1, order(e, zl, span), 1 - y)
        given_all(1, e)
    serve_guest(y, 1)
    middle = (z > 0) & (z + 1 < zs)

    @pl.when(middle)
    def _():
        line2_in(1)

    own_y_got.wait_recv()
    own_d.start()
    guest_d_got.wait_recv()
    for t in (0, 1):
        serve_guest(1 - y, t)

    @pl.when(jnp.logical_not(middle))
    def _():
        line2_in(1)

    @pl.when(middle)
    def _():
        @pl.loop(2, span + 1)
        def _(e):
            line2_in(e)

    own_d_got.wait_recv()
    for t in (0, 1):
        total = project(mine, 0, t)
        for e in range(1, span):
            total = total + project(mine, e, t)
        own_acc[t] = total
    for yy in (0, 1):
        for t in (0, 1):
            partial(yy, t).wait_recv()
    for yy in (0, 1):
        gate = own_acc[0, yy * CAP:(yy + 1) * CAP] + part_in[yy, 0].astype(jnp.float32)
        up = own_acc[1, yy * CAP:(yy + 1) * CAP] + part_in[yy, 1].astype(jnp.float32)
        hidden[yy] = (gate / (1.0 + jnp.exp(-gate)) * up).astype(jnp.bfloat16)

    def swap_x(j, yy):
        return remote(x_out.at[yy, j], x_in.at[yy, j], y_send, x_recv.at[yy, j], ha=1 - ha)

    def swap_y(zi, yy):
        return remote(y_out.at[yy, zi], y_in.at[yy, zi], y_send, y_recv.at[yy, zi], wa=beside)

    def swap_part(zi, yy, c):
        return remote(y_out.at[yy, zi, c], y_in.at[yy, zi, c], y_send, part_recv.at[0, yy, c], wa=beside)

    def swap_part_x(j, yy, c):
        return remote(
            yx_out.at[yy, j, c], yx_in.at[yy, j, c], y_send, part_recv.at[1, yy, c], ha=1 - ha
        )

    def swap_xy(j, yy):
        return remote(xy_out.at[yy, j], xy_in.at[yy, j], y_send, xy_recv.at[yy, j], wa=beside)

    def swap_yx(j, yy):
        return remote(yx_out.at[yy, j], yx_in.at[yy, j], y_send, yx_recv.at[yy, j], ha=1 - ha)

    def mine_rows(v):
        return jnp.where(y == 0, v[:CAP], v[CAP:]), jnp.where(y == 0, v[CAP:], v[:CAP])

    def down(zi, yy):
        return lax.dot_general(
            hidden[...].reshape(2 * CAP, q), w2[zi, yy].reshape(2 * fd, q), (((1,), (1,)), ((), ())),
            preferred_element_type=jnp.float32,
        )

    def place_of(e):
        zi = order(e, z, zs)
        out = zi // span
        return zi, out, zi - out * span

    def finish_x(e, yy):
        zi, out, j = place_of(e)
        second.given(0, zi, yy).wait_recv()
        part = down(zi, yy)

        @pl.when(out == ha)
        def _():
            x_own[yy, j] = part

        @pl.when(out != ha)
        def _():
            x_out[yy, j] = part.astype(jnp.bfloat16)
            swap_x(j, yy).start()

    def finish_y(e, yy):
        zi, out, j = place_of(e)
        second.given(0, zi, yy).wait_recv()
        keep, leave = mine_rows(down(zi, yy))
        for c in (0, 1):
            y_out[yy, zi, c] = leave[:, c * fd:(c + 1) * fd].astype(jnp.bfloat16)
        swap_y(zi, yy).start()
        for c in (0, 1):
            y_own[yy, zi, c] = keep[:, c * fd:(c + 1) * fd]

    def combine_x(e, yy):
        zi, out, j = place_of(e)

        @pl.when(out == ha)
        def _():
            swap_x(j, yy).wait_recv()
            keep, leave = mine_rows(x_own[yy, j] + x_in[yy, j].astype(jnp.float32))
            xy_own[yy, j] = keep
            xy_out[yy, j] = leave.astype(jnp.bfloat16)
            swap_xy(j, yy).start()

    def combine_y(e, yy):
        zi, out, j = place_of(e)
        swap_y(zi, yy).wait_recv()
        total = y_own[yy, zi] + y_in[yy, zi].astype(jnp.float32)

        @pl.when(out != ha)
        def _():
            yx_out[yy, j] = total.astype(jnp.bfloat16)
            swap_yx(j, yy).start()

        @pl.when(out == ha)
        def _():
            y_own[yy, zi] = total

    def part_last(yy, c):
        zi, out, j = place_of(zs - 1)
        keep, leave = mine_rows(lax.dot_general(
            hidden[...].reshape(2 * CAP, q), w2[zi, yy, c], (((1,), (1,)), ((), ())),
            preferred_element_type=jnp.float32,
        ))
        y_out[yy, zi, c] = leave.astype(jnp.bfloat16)
        swap_part(zi, yy, c).start()
        y_own[yy, zi, c] = keep

    def start_last(yy):
        second.serve(0, order(zs - 1, z, zs), yy)
        part_last(yy, core)

    def end_last(yy):
        second.given(0, order(zs - 1, z, zs), yy).wait_recv()
        part_last(yy, 1 - core)

    def combine_last(yy):
        zi, out, j = place_of(zs - 1)
        for c in (core, 1 - core):
            swap_part(zi, yy, c).wait_recv()
            total = y_own[yy, zi, c] + y_in[yy, zi, c].astype(jnp.float32)

            @pl.when(out != ha)
            def _():
                yx_out[yy, j, c] = total.astype(jnp.bfloat16)
                swap_part_x(j, yy, c).start()

            @pl.when(out == ha)
            def _():
                y_own[yy, zi, c] = total

    def late(e, yy):
        second.serve(0, order(e, z, zs), yy)
        finish_y(e, yy)

    @pl.when(middle)
    def _():
        @pl.loop(0, span + 1)
        def _(e):
            finish_x(e, 0)
            finish_y(e, 1)

        @pl.loop(span + 1, zs - 1)
        def _(e):
            late(e, 0)
            late(e, 1)

        start_last(0)
        end_last(0)
        start_last(1)
        end_last(1)

        @pl.loop(0, span + 1)
        def _(e):
            combine_y(e, 1)
            combine_x(e, 0)

        @pl.loop(span + 1, zs - 1)
        def _(e):
            combine_y(e, 0)
            combine_y(e, 1)

        combine_last(0)
        combine_last(1)

    @pl.when(jnp.logical_not(middle))
    def _():
        finish_y(0, 1)
        finish_x(0, 0)
        finish_y(1, 0)
        finish_y(1, 1)
        second.serve(0, order(2, z, zs), 0)
        finish_x(2, 0)
        late(2, 1)
        combine_y(0, 1)
        combine_y(1, 0)

        @pl.loop(3, zs - 1)
        def _(e):
            late(e, 0)
            late(e, 1)
            combine_y(e, 0)
            combine_y(e, 1)

        start_last(0)
        combine_y(1, 1)
        end_last(0)
        combine_x(2, 0)
        combine_y(2, 1)
        start_last(1)
        end_last(1)
        combine_x(0, 0)
        combine_last(0)
        combine_last(1)

    all_counts().wait_recv()

    counts[me] = jnp.zeros(counts.shape[1:], jnp.int32)

    def add_count(i, total):
        return total + jnp.where(i < me, counts[i], 0)

    earlier = lax.fori_loop(0, n, add_count, jnp.zeros(counts.shape[1:], jnp.int32))
    slot = lax.broadcasted_iota(jnp.int32, (CAP, 1), 0)
    scale = jnp.where(slot + earlier[0:1, 0:1] < n // 2 * CAP, route[:, 0:1], jnp.float32(0.0))
    width = 2 * span * wide
    cut = wide if wide % 128 == 0 else width

    def out_copy(u):
        return pltpu.make_async_copy(y_buf.at[:, u * cut:(u + 1) * cut], y_ref.at[:, u * cut:(u + 1) * cut], out_sem)

    def put(u, total):
        y_buf[:, u * wide:(u + 1) * wide] = (total * scale).astype(jnp.bfloat16)

    def put_y(u, zi, yy, j):
        for c in (0, 1):
            total = y_own[yy, zi, c] + yx_in[yy, j, c].astype(jnp.float32)
            y_buf[:, u * wide + c * fd:u * wide + (c + 1) * fd] = (total * scale).astype(jnp.bfloat16)

    for yy in (1, 0):
        for j in range(span):
            zi = ha * span + j
            u = 2 * j + yy
            final = rank_of(zi, z, zs) == zs - 1
            split = y_first(zi, yy)

            @pl.when(final)
            def _():
                for c in (core, 1 - core):
                    swap_part_x(j, yy, c).wait_recv()

            @pl.when(split & jnp.logical_not(final))
            def _():
                swap_yx(j, yy).wait_recv()

            @pl.when(split)
            def _():
                put_y(u, zi, yy, j)

            @pl.when(jnp.logical_not(split))
            def _():
                swap_xy(j, yy).wait_recv()
                put(u, xy_own[yy, j] + xy_in[yy, j].astype(jnp.float32))

            if cut == wide:
                out_copy(u).start()

    if cut != wide:
        out_copy(0).start()

    all_counts().wait_send()

    place_copy.wait()
    settle(e_send, 3 * fd * q)
    settle(g_send, 6 * sub * CAP * group)
    settle(p_send, 4 * CAP * q)
    first.drain(2)
    second.drain(1)

    unit = CAP * wide

    @pl.when(middle)
    def _():
        settle(y_send, (2 * span + span + 1 + 2 * zs - 1 - span) * unit)

    @pl.when(jnp.logical_not(middle))
    def _():
        settle(y_send, (2 * span + 2 * zs) * unit)

    pltpu.make_async_copy(y_buf, y_ref, out_sem).wait()


def expert(ids, keep, weight, tokens, gate, up, down):
    n = lax.axis_size("wa")
    fd, hid = gate.shape
    q = hid // 2
    zs = n // 4
    span = zs // 2
    sub = span // 2
    group = 4 * fd
    wide = 2 * fd
    any_spec = pl.BlockSpec(memory_space=pl.ANY)
    dma = pltpu.SemaphoreType.DMA
    bf16, f32 = jnp.bfloat16, jnp.float32
    return pl.pallas_call(
        functools.partial(expert_kernel, n),
        out_shape=(
            jax.ShapeDtypeStruct((CAP, span * group), bf16), jax.ShapeDtypeStruct((1, tokens.shape[0]), jnp.int32)
        ),
        in_specs=[any_spec] * 7,
        out_specs=(any_spec, any_spec),
        scratch_shapes=[
            pltpu.VMEM(ids.shape, jnp.int32),
            pltpu.VMEM(ids.shape, jnp.int32),
            pltpu.VMEM(ids.shape, f32),
            pltpu.VMEM((1, tokens.shape[0]), jnp.int32),
            pltpu.VMEM((2, span, 2, 2, fd, q), bf16),
            pltpu.VMEM((zs, 2, 2, fd, q), bf16),
            pltpu.VMEM((3, fd, q), bf16),
            pltpu.VMEM((sub + span, tokens.shape[0], group), bf16),
            pltpu.VMEM((sub, CAP, group), bf16),
            pltpu.VMEM((span, 2, CAP, group), bf16),
            pltpu.VMEM((span, 2, CAP, group), bf16),
            pltpu.VMEM((2, 2 * CAP, q), f32),
            pltpu.VMEM((2, 2, CAP, q), bf16),
            pltpu.VMEM((2, 2, CAP, q), bf16),
            pltpu.VMEM((2, CAP, q), bf16),
            pltpu.VMEM((2, span, 2 * CAP, wide), f32),
            pltpu.VMEM((2, span, 2 * CAP, wide), bf16),
            pltpu.VMEM((2, span, 2 * CAP, wide), bf16),
            pltpu.VMEM((2, zs, 2, CAP, fd), f32),
            pltpu.VMEM((2, zs, 2, CAP, fd), bf16),
            pltpu.VMEM((2, zs, 2, CAP, fd), bf16),
            pltpu.VMEM((2, span, CAP, wide), f32),
            pltpu.VMEM((2, span, CAP, wide), bf16),
            pltpu.VMEM((2, span, CAP, wide), bf16),
            pltpu.VMEM((2, span, 2, CAP, fd), bf16),
            pltpu.VMEM((2, span, 2, CAP, fd), bf16),
            pltpu.VMEM((CAP, 2 * span * wide), bf16),
            pltpu.VMEM((8, 128), jnp.int32),
            pltpu.VMEM((n, 8, 128), jnp.int32),
            pltpu.VMEM((CAP, 128), f32),
            dma((3,)), dma((sub + span,)), dma((2,)), dma,
            dma, dma((2, span, 2)), dma, dma((2, span)),
            dma, dma((1, zs, 2)), dma, dma((zs, 2)),
            dma, dma((6,)), dma, dma((2, 2)),
            dma((2, span)), dma, dma((2, zs)), dma((2, span)), dma((2, span)), dma((2, 2, 2)), dma, dma((4,)),
        ],
        compiler_params=pltpu.CompilerParams(
            collective_id=0, has_side_effects=True, vmem_limit_bytes=60 * 1024 * 1024
        ),
    )(ids, keep, weight, tokens, gate, up, down)


def combine_kernel(place_ref, y_ref, out_ref, place, rows, block, in_sem, out_sem):
    steps, tall, _ = block.shape
    count, _, wide = rows.shape
    loads = [pltpu.make_async_copy(place_ref, place, in_sem.at[count])]
    for k in range(count):
        loads.append(pltpu.make_async_copy(y_ref.at[:, k * wide:(k + 1) * wide], rows.at[k], in_sem.at[k]))
    for load in loads:
        load.start()
    loads[0].wait()
    slots = lax.broadcasted_iota(jnp.int32, (CAP, steps * tall), 0)
    pick = jnp.where(place[...] == slots, jnp.float32(1.0), jnp.float32(0.0)).astype(jnp.bfloat16).T
    for load in loads[1:]:
        load.wait()
    stores = []
    for i in range(steps):
        for k in range(count):
            block[i, :, k * wide:(k + 1) * wide] = jnp.dot(
                pick[i * tall:(i + 1) * tall], rows[k], preferred_element_type=jnp.float32
            ).astype(jnp.bfloat16)
        stores.append(pltpu.make_async_copy(block.at[i], out_ref.at[i * tall:(i + 1) * tall], out_sem.at[i]))
        stores[i].start()
    for store in stores:
        store.wait()


def combine(place, y):
    tokens, width = place.shape[1], y.shape[1]
    wide = 512 if width % 512 == 0 else width
    tall = CAP if tokens % CAP == 0 else tokens
    count, steps = width // wide, tokens // tall
    any_spec = pl.BlockSpec(memory_space=pl.ANY)
    dma = pltpu.SemaphoreType.DMA
    return pl.pallas_call(
        combine_kernel,
        out_shape=jax.ShapeDtypeStruct((tokens, width), jnp.bfloat16),
        in_specs=[any_spec, any_spec],
        out_specs=any_spec,
        scratch_shapes=[
            pltpu.VMEM((1, tokens), jnp.int32),
            pltpu.VMEM((count, CAP, wide), jnp.bfloat16),
            pltpu.VMEM((steps, tall, width), jnp.bfloat16),
            dma((count + 1,)), dma((steps,)),
        ],
    )(place, y)


def per_device(tokens, expert_ids, keep_mask, route_weight, gate_weight, up_weight, down_weight):
    y, place = expert(expert_ids.T, keep_mask.T, route_weight.T, tokens, gate_weight, up_weight, down_weight)
    return combine(place, y)


def solution(mesh):
    return jax.shard_map(
        per_device,
        mesh=mesh,
        in_specs=(
            P("wa", None),
            P("wa", None),
            P("wa", None),
            P("wa", None),
            P("wa", "ha"),
            P("wa", "ha"),
            P("wa", "ha"),
        ),
        out_specs=P("wa", "ha"),
        check_vma=False,
    )
```

```python
import functools

import jax
import jax.numpy as jnp
from jax import lax
from jax.experimental import pallas as pl
from jax.experimental.pallas import tpu as pltpu
from jax.sharding import PartitionSpec as P

CAP = 128
MESH = pl.DeviceIdType.MESH


def expert_kernel(
    n,
    ids_ref, keep_ref, route_ref, tok_ref, gate_ref, up_ref, down_ref,
    y_ref, place_ref,
    ids, keep, weight, w1, w2, stage, tok_buf, guest_out, own_rows, guest_rows, own_acc, part_out, part_in, hidden,
    x_own, x_out, x_in, y_own, y_out, y_in, xy_own, xy_out, xy_in, yx_out, yx_in, count, counts, route,
    load_sem, tok_sem, c_sem, e_send, l1_send, l1_recv, b1_send, b1_recv, l2_send, l2_recv, b2_send, b2_recv,
    g_send, g_recv, p_send, p_recv, x_recv, y_send, y_recv, xy_recv, yx_recv,
    part_recv, route_sem,
):
    zs = n // 4
    span = zs // 2
    sub = span // 2
    me = lax.axis_index("wa")
    ha = lax.axis_index("ha")
    core = lax.rem(me, 2)
    y = lax.rem(me // 2, 2)
    z = me // 4
    half = z // span
    zl = z - half * span
    sibling = me + 1 - 2 * core
    beside = me + 2 - 4 * y
    mirror = lax.rem(me + n // 2, n)
    q = hidden.shape[2]
    fd = stage.shape[1]
    group = 4 * fd
    wide = 2 * fd

    def remote(ref, dst, send, recv, **where):
        return pltpu.make_async_remote_copy(
            src_ref=ref, dst_ref=dst, send_sem=send, recv_sem=recv, device_id=where, device_id_type=MESH
        )

    def same(ref, send, recv, **where):
        return remote(ref, ref, send, recv, **where)

    def order(e, at, size):
        low = jnp.where(at < size // 2, 1, 0)
        at = low * at + (1 - low) * (size - 1 - at)
        paired = jnp.where(e % 2 == 1, at + (e + 1) // 2, at - e // 2)
        nth = jnp.where(e <= 2 * at, paired, e)
        return low * nth + (1 - low) * (size - 1 - nth)

    def rank_of(zi, at, size):
        low = jnp.where(at < size // 2, 1, 0)
        at = low * at + (1 - low) * (size - 1 - at)
        zi = low * zi + (1 - low) * (size - 1 - zi)
        return jnp.where(zi > 2 * at, zi, jnp.where(zi > at, 2 * (zi - at) - 1, 2 * (at - zi)))

    def y_first(zi, yy):
        rank = rank_of(zi, z, zs)
        edge = (z == 0) | (z + 1 == zs)
        if yy == 1:
            return rank >= 0
        return (rank > span) | (edge & ((rank == 1) | (rank > 2)))

    def settle(sem, elements):
        rows = elements // group
        tokens = tok_buf.shape[1]
        for size in [tokens] * (rows // tokens) + [rows % tokens] * (rows % tokens > 0):
            same(tok_buf.at[0, 0:size], sem, sem, wa=sibling).wait_send()

    class Line:
        def __init__(self, ref_of, at, size, sems):
            self.ref_of, self.at, self.size = ref_of, at, size
            self.l_send, self.l_recv, self.b_send, self.b_recv = sems

        def hop(self, way, *unit):
            to = me + 4 * (1 - 2 * way)
            return same(self.ref_of(core, *unit), self.l_send, self.l_recv.at[unit], wa=to)

        def up(self, zi):
            return (zi <= self.at) & (self.at + 1 < self.size)

        def down(self, zi):
            return (zi >= self.at) & (self.at > 0)

        def push(self, t, zi, yy):
            @pl.when(self.up(zi))
            def _():
                self.hop(0, t, zi, yy).start()

            @pl.when(self.down(zi))
            def _():
                self.hop(1, t, zi, yy).start()

        def arrive(self, t, zi, yy):
            self.hop(0, t, zi, yy).wait_recv()

        def give(self, t, zi, yy):
            return same(self.ref_of(core, t, zi, yy), self.b_send, self.b_recv(t, zi, yy), wa=sibling)

        def given(self, t, zi, yy):
            return same(self.ref_of(1 - core, t, zi, yy), self.b_send, self.b_recv(t, zi, yy), wa=sibling)

        def spread(self, t, zi, yy):
            self.push(t, zi, yy)
            self.give(t, zi, yy).start()

        def serve(self, t, zi, yy):
            self.arrive(t, zi, yy)
            self.spread(t, zi, yy)

        def drain(self, kinds):
            edge = (self.at == 0) | (self.at + 1 == self.size)
            unit = 2 * kinds * fd * q

            @pl.when(edge)
            def _():
                settle(self.l_send, unit)

            @pl.when(jnp.logical_not(edge))
            def _():
                settle(self.l_send, (self.size + 1) * unit)

            settle(self.b_send, self.size * unit)

    first = Line(lambda c, t, zi, yy: w1.at[t, zi, yy, c], zl, span, (l1_send, l1_recv, b1_send, lambda t, zi, yy: b1_recv.at[t, zi]))
    second = Line(lambda c, t, zi, yy: w2.at[zi, yy, c], z, zs, (l2_send, l2_recv, b2_send, lambda t, zi, yy: b2_recv.at[zi, yy]))

    def exchange(t):
        dst, recv = (w2.at[z, y, core], l2_recv.at[0, z, y]) if t == 2 else (w1.at[t, zl, y, core], l1_recv.at[t, zl, y])
        return remote(stage.at[t], dst, e_send, recv, wa=beside)

    def count_copy(k):
        return remote(count, counts.at[me], c_sem.at[0], c_sem.at[1], wa=lax.rem(me + k, n))

    def all_counts():
        return same(counts.at[pl.ds(0, n - 1)], c_sem.at[0], c_sem.at[1], wa=sibling)

    def columns(ref, index):
        return ref.at[:, pl.ds(pl.multiple_of(index * q, 128), q)]

    weights = (gate_ref, up_ref, down_ref)
    homes = (w1.at[0, zl, y, core], w1.at[1, zl, y, core], w2.at[z, y, core])
    loads = []
    for t in range(3):
        loads.append((
            pltpu.make_async_copy(columns(weights[t], 1 - y), stage.at[t], load_sem.at[t]),
            pltpu.make_async_copy(columns(weights[t], y), homes[t], load_sem.at[t]),
        ))

    def loaded(t):
        pltpu.make_async_copy(w1.at[0, 0, 0], w1.at[0, 0, 0], load_sem.at[t]).wait()

    def tok_load(i):
        column = (1 - half) * span + ha * sub + i if i < sub else half * span + i - sub
        return pltpu.make_async_copy(
            tok_ref.at[:, pl.ds(pl.multiple_of(column * group, 128), group)], tok_buf.at[i], tok_sem.at[i]
        )

    routing = [
        pltpu.make_async_copy(ref, buf, route_sem.at[k])
        for k, (ref, buf) in enumerate(((ids_ref, ids), (keep_ref, keep), (route_ref, weight)))
    ]
    for copy in (*loads[0], *routing):
        copy.start()
    for i in range(sub):
        tok_load(i).start()
    for load in (*loads[1], *loads[2]):
        load.start()
    for i in range(sub, sub + span):
        tok_load(i).start()

    barrier = pltpu.get_barrier_semaphore()

    @pl.loop(1, n)
    def _(k):
        pl.semaphore_signal(barrier, inc=1, device_id={"wa": lax.rem(me + k, n)}, device_id_type=MESH)

    pl.semaphore_signal(barrier, inc=1, device_id={"ha": 1 - ha}, device_id_type=MESH)

    pl.semaphore_wait(barrier, n)

    def direct(ref, yy, sems, k, **where):
        return same(ref.at[pl.ds(ha * sub, sub), yy], sems[0], sems[1].at[k], **where)

    def other(ref, yy, sems, k, **where):
        return same(ref.at[pl.ds((1 - ha) * sub, sub), yy], sems[0], sems[1].at[k], **where)

    g_sems = (g_send, g_recv)
    to_x = {"ha": 1 - ha}
    to_y = {"wa": beside}
    guest_send = remote(guest_out, guest_rows.at[pl.ds(ha * sub, sub), y], g_send, g_recv.at[0], wa=mirror)
    guest_y, guest_y_got = direct(guest_rows, y, g_sems, 1, **to_y), direct(guest_rows, 1 - y, g_sems, 1, **to_y)
    guest_x, guest_x_got = direct(guest_rows, y, g_sems, 2, **to_x), other(guest_rows, y, g_sems, 2, **to_x)
    guest_d, guest_d_got = direct(guest_rows, 1 - y, g_sems, 3, **to_x), other(guest_rows, 1 - y, g_sems, 3, **to_x)
    own_y, own_y_got = direct(own_rows, y, g_sems, 4, **to_y), direct(own_rows, 1 - y, g_sems, 4, **to_y)
    own_d, own_d_got = direct(own_rows, 1 - y, g_sems, 5, **to_x), other(own_rows, 1 - y, g_sems, 5, **to_x)

    def given_all(t, e):
        zi = order(e, zl, span)
        same(w1.at[t, zi, :, 1 - core], b1_send, b1_recv.at[t, zi], wa=sibling).wait_recv()

    def line2_in(e):
        zi = order(e, z, zs)
        for yy in (0, 1):
            second.serve(0, zi, yy)

    def project(rows, e, t):
        zi = order(e, zl, span)
        return jnp.dot(rows(zi), w1[t, zi].reshape(group, q), preferred_element_type=jnp.float32)

    def guests(yy):
        return lambda zi: guest_rows[zi, yy]

    def mine(zi):
        return own_rows[zi].reshape(2 * CAP, group)

    def partial(yy, t):
        return remote(part_out.at[yy, t], part_in.at[yy, t], p_send, p_recv.at[yy, t], wa=mirror)

    def serve_guest(yy, t):
        total = None
        for e in range(span):
            term = project(guests(yy), e, t)
            total = term if total is None else total + term
        part_out[yy, t] = total.astype(jnp.bfloat16)
        partial(yy, t).start()

    loaded(0)
    exchange(0).start()
    first.spread(0, zl, y)
    for copy in routing:
        copy.wait()
    matches = (ids[...] == 0) & (keep[...] == 1)
    chosen = jnp.minimum(jnp.sum(jnp.where(matches, 1, 0), axis=0, keepdims=True), 1)
    route_sum = jnp.sum(jnp.where(matches, weight[...], jnp.float32(0.0)), axis=0, keepdims=True)
    length = chosen.shape[1]
    lane = lax.broadcasted_iota(jnp.int32, (8, length), 1)
    running = jnp.broadcast_to(chosen, (8, length))
    shift = 1
    while shift < length:
        running = running + jnp.where(lane >= shift, pltpu.roll(running, shift, 1), 0)
        shift *= 2
    place = jnp.where(chosen == 1, running[0:1] - 1, -1)
    place_ref[...] = place
    count[...] = jnp.broadcast_to(jnp.sum(chosen, axis=1, keepdims=True), count.shape)
    slot_ids = lax.broadcasted_iota(jnp.int32, (CAP, length), 0)
    hit = place == slot_ids
    table = jnp.where(hit, jnp.float32(1.0), jnp.float32(0.0)).astype(jnp.bfloat16)
    for i in range(sub):
        tok_load(i).wait()
        guest_out[i] = jnp.dot(table, tok_buf[i], preferred_element_type=jnp.float32).astype(jnp.bfloat16)
    guest_send.start()
    loaded(1)
    exchange(1).start()
    first.spread(1, zl, y)
    loaded(2)
    exchange(2).start()
    slot_route = jnp.sum(jnp.where(hit, route_sum, jnp.float32(0.0)), axis=1, keepdims=True)
    route[...] = jnp.broadcast_to(slot_route, route.shape)
    for i in range(span):
        tok_load(sub + i).wait()
        own_rows[i, y] = jnp.dot(
            table, tok_buf[sub + i], preferred_element_type=jnp.float32
        ).astype(jnp.bfloat16)

    @pl.loop(1, n)
    def _(k):
        count_copy(k).start()

    for t in (0, 1):
        first.serve(t, zl, 1 - y)
    second.spread(0, z, y)
    guest_send.wait_recv()
    guest_y.start()
    guest_x.start()
    own_y.start()
    second.serve(0, z, 1 - y)
    for t in (0, 1):
        given_all(t, 0)
    guest_y_got.wait_recv()
    guest_d.start()
    guest_x_got.wait_recv()
    for e in range(1, span):
        zi = order(e, zl, span)
        for t in (0, 1):
            first.serve(t, zi, y)
        first.serve(0, zi, 1 - y)
        given_all(0, e)
    serve_guest(y, 0)
    for e in range(1, span):
        first.serve(1, order(e, zl, span), 1 - y)
        given_all(1, e)
    serve_guest(y, 1)
    middle = (z > 0) & (z + 1 < zs)

    @pl.when(middle)
    def _():
        line2_in(1)

    own_y_got.wait_recv()
    own_d.start()
    guest_d_got.wait_recv()
    for t in (0, 1):
        serve_guest(1 - y, t)

    @pl.when(jnp.logical_not(middle))
    def _():
        line2_in(1)

    @pl.when(middle)
    def _():
        @pl.loop(2, span + 1)
        def _(e):
            line2_in(e)

    own_d_got.wait_recv()
    for t in (0, 1):
        total = project(mine, 0, t)
        for e in range(1, span):
            total = total + project(mine, e, t)
        own_acc[t] = total
    for yy in (0, 1):
        for t in (0, 1):
            partial(yy, t).wait_recv()
    for yy in (0, 1):
        gate = own_acc[0, yy * CAP:(yy + 1) * CAP] + part_in[yy, 0].astype(jnp.float32)
        up = own_acc[1, yy * CAP:(yy + 1) * CAP] + part_in[yy, 1].astype(jnp.float32)
        hidden[yy] = (gate / (1.0 + jnp.exp(-gate)) * up).astype(jnp.bfloat16)

    def swap_x(j, yy):
        return remote(x_out.at[yy, j], x_in.at[yy, j], y_send, x_recv.at[yy, j], ha=1 - ha)

    def swap_y(zi, yy):
        return remote(y_out.at[yy, zi], y_in.at[yy, zi], y_send, y_recv.at[yy, zi], wa=beside)

    def swap_part(zi, yy, c):
        return remote(y_out.at[yy, zi, c], y_in.at[yy, zi, c], y_send, part_recv.at[0, yy, c], wa=beside)

    def swap_part_x(j, yy, c):
        return remote(
            yx_out.at[yy, j, c], yx_in.at[yy, j, c], y_send, part_recv.at[1, yy, c], ha=1 - ha
        )

    def swap_xy(j, yy):
        return remote(xy_out.at[yy, j], xy_in.at[yy, j], y_send, xy_recv.at[yy, j], wa=beside)

    def swap_yx(j, yy):
        return remote(yx_out.at[yy, j], yx_in.at[yy, j], y_send, yx_recv.at[yy, j], ha=1 - ha)

    def mine_rows(v):
        return jnp.where(y == 0, v[:CAP], v[CAP:]), jnp.where(y == 0, v[CAP:], v[:CAP])

    def down(zi, yy):
        return lax.dot_general(
            hidden[...].reshape(2 * CAP, q), w2[zi, yy].reshape(2 * fd, q), (((1,), (1,)), ((), ())),
            preferred_element_type=jnp.float32,
        )

    def place_of(e):
        zi = order(e, z, zs)
        out = zi // span
        return zi, out, zi - out * span

    def finish_x(e, yy):
        zi, out, j = place_of(e)
        second.given(0, zi, yy).wait_recv()
        part = down(zi, yy)

        @pl.when(out == ha)
        def _():
            x_own[yy, j] = part

        @pl.when(out != ha)
        def _():
            x_out[yy, j] = part.astype(jnp.bfloat16)
            swap_x(j, yy).start()

    def finish_y(e, yy):
        zi, out, j = place_of(e)
        second.given(0, zi, yy).wait_recv()
        keep, leave = mine_rows(down(zi, yy))
        for c in (0, 1):
            y_out[yy, zi, c] = leave[:, c * fd:(c + 1) * fd].astype(jnp.bfloat16)
        swap_y(zi, yy).start()
        for c in (0, 1):
            y_own[yy, zi, c] = keep[:, c * fd:(c + 1) * fd]

    def combine_x(e, yy):
        zi, out, j = place_of(e)

        @pl.when(out == ha)
        def _():
            swap_x(j, yy).wait_recv()
            keep, leave = mine_rows(x_own[yy, j] + x_in[yy, j].astype(jnp.float32))
            xy_own[yy, j] = keep
            xy_out[yy, j] = leave.astype(jnp.bfloat16)
            swap_xy(j, yy).start()

    def combine_y(e, yy):
        zi, out, j = place_of(e)
        swap_y(zi, yy).wait_recv()
        total = y_own[yy, zi] + y_in[yy, zi].astype(jnp.float32)

        @pl.when(out != ha)
        def _():
            yx_out[yy, j] = total.astype(jnp.bfloat16)
            swap_yx(j, yy).start()

        @pl.when(out == ha)
        def _():
            y_own[yy, zi] = total

    def part_last(yy, c):
        zi, out, j = place_of(zs - 1)
        keep, leave = mine_rows(lax.dot_general(
            hidden[...].reshape(2 * CAP, q), w2[zi, yy, c], (((1,), (1,)), ((), ())),
            preferred_element_type=jnp.float32,
        ))
        y_out[yy, zi, c] = leave.astype(jnp.bfloat16)
        swap_part(zi, yy, c).start()
        y_own[yy, zi, c] = keep

    def start_last(yy):
        second.serve(0, order(zs - 1, z, zs), yy)
        part_last(yy, core)

    def end_last(yy):
        second.given(0, order(zs - 1, z, zs), yy).wait_recv()
        part_last(yy, 1 - core)

    def combine_last(yy):
        zi, out, j = place_of(zs - 1)
        for c in (core, 1 - core):
            swap_part(zi, yy, c).wait_recv()
            total = y_own[yy, zi, c] + y_in[yy, zi, c].astype(jnp.float32)

            @pl.when(out != ha)
            def _():
                yx_out[yy, j, c] = total.astype(jnp.bfloat16)
                swap_part_x(j, yy, c).start()

            @pl.when(out == ha)
            def _():
                y_own[yy, zi, c] = total

    def late(e, yy):
        second.serve(0, order(e, z, zs), yy)
        finish_y(e, yy)

    @pl.when(middle)
    def _():
        @pl.loop(0, span + 1)
        def _(e):
            finish_x(e, 0)
            finish_y(e, 1)

        @pl.loop(span + 1, zs - 1)
        def _(e):
            late(e, 0)
            late(e, 1)

        start_last(0)
        end_last(0)
        start_last(1)
        end_last(1)

        @pl.loop(0, span + 1)
        def _(e):
            combine_y(e, 1)
            combine_x(e, 0)

        @pl.loop(span + 1, zs - 1)
        def _(e):
            combine_y(e, 0)
            combine_y(e, 1)

        combine_last(0)
        combine_last(1)

    @pl.when(jnp.logical_not(middle))
    def _():
        finish_y(0, 1)
        finish_x(0, 0)
        finish_y(1, 0)
        finish_y(1, 1)
        second.serve(0, order(2, z, zs), 0)
        finish_x(2, 0)
        late(2, 1)
        combine_y(0, 1)
        combine_y(1, 0)

        @pl.loop(3, zs - 1)
        def _(e):
            late(e, 0)
            late(e, 1)
            combine_y(e, 0)
            combine_y(e, 1)

        start_last(0)
        combine_y(1, 1)
        end_last(0)
        combine_x(2, 0)
        combine_y(2, 1)
        start_last(1)
        end_last(1)
        combine_x(0, 0)
        combine_last(0)
        combine_last(1)

    all_counts().wait_recv()

    counts[me] = jnp.zeros(counts.shape[1:], jnp.int32)

    def add_count(i, total):
        return total + jnp.where(i < me, counts[i], 0)

    earlier = lax.fori_loop(0, n, add_count, jnp.zeros(counts.shape[1:], jnp.int32))
    slot = lax.broadcasted_iota(jnp.int32, (CAP, 1), 0)
    scale = jnp.where(slot + earlier[0:1, 0:1] < n // 2 * CAP, route[:, 0:1], jnp.float32(0.0))
    def put(u, total):
        y_ref[:, u * wide:(u + 1) * wide] = (total * scale).astype(jnp.bfloat16)

    def put_y(u, zi, yy, j):
        for c in (0, 1):
            total = y_own[yy, zi, c] + yx_in[yy, j, c].astype(jnp.float32)
            y_ref[:, u * wide + c * fd:u * wide + (c + 1) * fd] = (total * scale).astype(jnp.bfloat16)

    for yy in (1, 0):
        for j in range(span):
            zi = ha * span + j
            u = 2 * j + yy
            final = rank_of(zi, z, zs) == zs - 1
            split = y_first(zi, yy)

            @pl.when(final)
            def _():
                for c in (core, 1 - core):
                    swap_part_x(j, yy, c).wait_recv()

            @pl.when(split & jnp.logical_not(final))
            def _():
                swap_yx(j, yy).wait_recv()

            @pl.when(split)
            def _():
                put_y(u, zi, yy, j)

            @pl.when(jnp.logical_not(split))
            def _():
                swap_xy(j, yy).wait_recv()
                put(u, xy_own[yy, j] + xy_in[yy, j].astype(jnp.float32))

    all_counts().wait_send()

    settle(e_send, 3 * fd * q)
    settle(g_send, 6 * sub * CAP * group)
    settle(p_send, 4 * CAP * q)
    first.drain(2)
    second.drain(1)

    unit = CAP * wide

    @pl.when(middle)
    def _():
        settle(y_send, (2 * span + span + 1 + 2 * zs - 1 - span) * unit)

    @pl.when(jnp.logical_not(middle))
    def _():
        settle(y_send, (2 * span + 2 * zs) * unit)


def expert(ids, keep, weight, tokens, gate, up, down):
    n = lax.axis_size("wa")
    fd, hid = gate.shape
    q = hid // 2
    zs = n // 4
    span = zs // 2
    sub = span // 2
    group = 4 * fd
    wide = 2 * fd
    any_spec = pl.BlockSpec(memory_space=pl.ANY)
    vmem = pl.BlockSpec(memory_space=pltpu.VMEM)
    dma = pltpu.SemaphoreType.DMA
    bf16, f32 = jnp.bfloat16, jnp.float32
    return pl.pallas_call(
        functools.partial(expert_kernel, n),
        out_shape=(
            pltpu.VMEM((CAP, span * group), bf16), pltpu.VMEM((1, tokens.shape[0]), jnp.int32)
        ),
        in_specs=[any_spec] * 7,
        out_specs=(vmem, vmem),
        scratch_shapes=[
            pltpu.VMEM(ids.shape, jnp.int32),
            pltpu.VMEM(ids.shape, jnp.int32),
            pltpu.VMEM(ids.shape, f32),
            pltpu.VMEM((2, span, 2, 2, fd, q), bf16),
            pltpu.VMEM((zs, 2, 2, fd, q), bf16),
            pltpu.VMEM((3, fd, q), bf16),
            pltpu.VMEM((sub + span, tokens.shape[0], group), bf16),
            pltpu.VMEM((sub, CAP, group), bf16),
            pltpu.VMEM((span, 2, CAP, group), bf16),
            pltpu.VMEM((span, 2, CAP, group), bf16),
            pltpu.VMEM((2, 2 * CAP, q), f32),
            pltpu.VMEM((2, 2, CAP, q), bf16),
            pltpu.VMEM((2, 2, CAP, q), bf16),
            pltpu.VMEM((2, CAP, q), bf16),
            pltpu.VMEM((2, span, 2 * CAP, wide), f32),
            pltpu.VMEM((2, span, 2 * CAP, wide), bf16),
            pltpu.VMEM((2, span, 2 * CAP, wide), bf16),
            pltpu.VMEM((2, zs, 2, CAP, fd), f32),
            pltpu.VMEM((2, zs, 2, CAP, fd), bf16),
            pltpu.VMEM((2, zs, 2, CAP, fd), bf16),
            pltpu.VMEM((2, span, CAP, wide), f32),
            pltpu.VMEM((2, span, CAP, wide), bf16),
            pltpu.VMEM((2, span, CAP, wide), bf16),
            pltpu.VMEM((2, span, 2, CAP, fd), bf16),
            pltpu.VMEM((2, span, 2, CAP, fd), bf16),
            pltpu.VMEM((8, 128), jnp.int32),
            pltpu.VMEM((n, 8, 128), jnp.int32),
            pltpu.VMEM((CAP, 128), f32),
            dma((3,)), dma((sub + span,)), dma((2,)), dma,
            dma, dma((2, span, 2)), dma, dma((2, span)),
            dma, dma((1, zs, 2)), dma, dma((zs, 2)),
            dma, dma((6,)), dma, dma((2, 2)),
            dma((2, span)), dma, dma((2, zs)), dma((2, span)), dma((2, span)), dma((2, 2, 2)), dma((3,)),
        ],
        compiler_params=pltpu.CompilerParams(
            collective_id=0, has_side_effects=True, vmem_limit_bytes=60 * 1024 * 1024
        ),
    )(ids, keep, weight, tokens, gate, up, down)


def combine_kernel(place_ref, y_ref, out_ref, block, out_sem):
    steps, tall, width = block.shape
    wide = 512 if width % 512 == 0 else width
    slots = lax.broadcasted_iota(jnp.int32, (CAP, steps * tall), 0)
    pick = jnp.where(place_ref[...] == slots, jnp.float32(1.0), jnp.float32(0.0)).astype(jnp.bfloat16).T
    stores = []
    for i in range(steps):
        for k in range(0, width, wide):
            block[i, :, k:k + wide] = jnp.dot(
                pick[i * tall:(i + 1) * tall], y_ref[:, k:k + wide], preferred_element_type=jnp.float32
            ).astype(jnp.bfloat16)
        stores.append(pltpu.make_async_copy(block.at[i], out_ref.at[i * tall:(i + 1) * tall], out_sem.at[i]))
        stores[i].start()
    for store in stores:
        store.wait()


def combine(place, y):
    tokens, width = place.shape[1], y.shape[1]
    tall = CAP if tokens % CAP == 0 else tokens
    steps = tokens // tall
    vmem = pl.BlockSpec(memory_space=pltpu.VMEM)
    return pl.pallas_call(
        combine_kernel,
        out_shape=jax.ShapeDtypeStruct((tokens, width), jnp.bfloat16),
        in_specs=[vmem, vmem],
        out_specs=pl.BlockSpec(memory_space=pl.ANY),
        scratch_shapes=[pltpu.VMEM((steps, tall, width), jnp.bfloat16), pltpu.SemaphoreType.DMA((steps,))],
        compiler_params=pltpu.CompilerParams(vmem_limit_bytes=32 * 1024 * 1024),
    )(place, y)


def per_device(tokens, expert_ids, keep_mask, route_weight, gate_weight, up_weight, down_weight):
    y, place = expert(expert_ids.T, keep_mask.T, route_weight.T, tokens, gate_weight, up_weight, down_weight)
    return combine(place, y)


def solution(mesh):
    return jax.shard_map(
        per_device,
        mesh=mesh,
        in_specs=(
            P("wa", None),
            P("wa", None),
            P("wa", None),
            P("wa", None),
            P("wa", "ha"),
            P("wa", "ha"),
            P("wa", "ha"),
        ),
        out_specs=P("wa", "ha"),
        check_vma=False,
    )
```

```python
import functools

import jax
import jax.numpy as jnp
from jax import lax
from jax.experimental import pallas as pl
from jax.experimental.pallas import tpu as pltpu
from jax.sharding import PartitionSpec as P

CAP = 128
MESH = pl.DeviceIdType.MESH


def expert_kernel(
    n,
    ids_ref, keep_ref, route_ref, tok_ref, gate_ref, up_ref, down_ref,
    y_ref, pick_ref,
    ids, keep, weight, w1, w2, stage, tok_buf, guest_out, own_rows, guest_rows, own_acc, part_out, part_in, hidden,
    x_own, x_out, x_in, y_own, y_out, y_in, xy_own, xy_out, xy_in, yx_out, yx_in, count, counts, route,
    load_sem, tok_sem, c_sem, e_send, l1_send, l1_recv, b1_send, b1_recv, l2_send, l2_recv, b2_send, b2_recv,
    g_send, g_recv, p_send, p_recv, x_recv, y_send, y_recv, xy_recv, yx_recv,
    part_recv, route_sem,
):
    zs = n // 4
    span = zs // 2
    sub = span // 2
    me = lax.axis_index("wa")
    ha = lax.axis_index("ha")
    core = lax.rem(me, 2)
    y = lax.rem(me // 2, 2)
    z = me // 4
    half = z // span
    zl = z - half * span
    sibling = me + 1 - 2 * core
    beside = me + 2 - 4 * y
    mirror = lax.rem(me + n // 2, n)
    q = hidden.shape[2]
    fd = stage.shape[1]
    group = 4 * fd
    wide = 2 * fd

    def remote(ref, dst, send, recv, **where):
        return pltpu.make_async_remote_copy(
            src_ref=ref, dst_ref=dst, send_sem=send, recv_sem=recv, device_id=where, device_id_type=MESH
        )

    def same(ref, send, recv, **where):
        return remote(ref, ref, send, recv, **where)

    def order(e, at, size):
        low = jnp.where(at < size // 2, 1, 0)
        at = low * at + (1 - low) * (size - 1 - at)
        paired = jnp.where(e % 2 == 1, at + (e + 1) // 2, at - e // 2)
        nth = jnp.where(e <= 2 * at, paired, e)
        return low * nth + (1 - low) * (size - 1 - nth)

    def rank_of(zi, at, size):
        low = jnp.where(at < size // 2, 1, 0)
        at = low * at + (1 - low) * (size - 1 - at)
        zi = low * zi + (1 - low) * (size - 1 - zi)
        return jnp.where(zi > 2 * at, zi, jnp.where(zi > at, 2 * (zi - at) - 1, 2 * (at - zi)))

    def y_first(zi, yy):
        rank = rank_of(zi, z, zs)
        edge = (z == 0) | (z + 1 == zs)
        if yy == 1:
            return rank >= 0
        return (rank > span) | (edge & ((rank == 1) | (rank > 2)))

    def settle(sem, elements):
        rows = elements // group
        tokens = tok_buf.shape[1]
        for size in [tokens] * (rows // tokens) + [rows % tokens] * (rows % tokens > 0):
            same(tok_buf.at[0, 0:size], sem, sem, wa=sibling).wait_send()

    class Line:
        def __init__(self, ref_of, at, size, sems):
            self.ref_of, self.at, self.size = ref_of, at, size
            self.l_send, self.l_recv, self.b_send, self.b_recv = sems

        def hop(self, way, *unit):
            to = me + 4 * (1 - 2 * way)
            return same(self.ref_of(core, *unit), self.l_send, self.l_recv.at[unit], wa=to)

        def up(self, zi):
            return (zi <= self.at) & (self.at + 1 < self.size)

        def down(self, zi):
            return (zi >= self.at) & (self.at > 0)

        def push(self, t, zi, yy):
            @pl.when(self.up(zi))
            def _():
                self.hop(0, t, zi, yy).start()

            @pl.when(self.down(zi))
            def _():
                self.hop(1, t, zi, yy).start()

        def arrive(self, t, zi, yy):
            self.hop(0, t, zi, yy).wait_recv()

        def give(self, t, zi, yy):
            return same(self.ref_of(core, t, zi, yy), self.b_send, self.b_recv(t, zi, yy), wa=sibling)

        def given(self, t, zi, yy):
            return same(self.ref_of(1 - core, t, zi, yy), self.b_send, self.b_recv(t, zi, yy), wa=sibling)

        def spread(self, t, zi, yy):
            self.push(t, zi, yy)
            self.give(t, zi, yy).start()

        def serve(self, t, zi, yy):
            self.arrive(t, zi, yy)
            self.spread(t, zi, yy)

        def drain(self, kinds):
            edge = (self.at == 0) | (self.at + 1 == self.size)
            unit = 2 * kinds * fd * q

            @pl.when(edge)
            def _():
                settle(self.l_send, unit)

            @pl.when(jnp.logical_not(edge))
            def _():
                settle(self.l_send, (self.size + 1) * unit)

            settle(self.b_send, self.size * unit)

    first = Line(lambda c, t, zi, yy: w1.at[t, zi, yy, c], zl, span, (l1_send, l1_recv, b1_send, lambda t, zi, yy: b1_recv.at[t, zi]))
    second = Line(lambda c, t, zi, yy: w2.at[zi, yy, c], z, zs, (l2_send, l2_recv, b2_send, lambda t, zi, yy: b2_recv.at[zi, yy]))

    def exchange(t):
        dst, recv = (w2.at[z, y, core], l2_recv.at[0, z, y]) if t == 2 else (w1.at[t, zl, y, core], l1_recv.at[t, zl, y])
        return remote(stage.at[t], dst, e_send, recv, wa=beside)

    def count_copy(k):
        return remote(count, counts.at[me], c_sem.at[0], c_sem.at[1], wa=lax.rem(me + k, n))

    def all_counts():
        return same(counts.at[pl.ds(0, n - 1)], c_sem.at[0], c_sem.at[1], wa=sibling)

    def columns(ref, index):
        return ref.at[:, pl.ds(pl.multiple_of(index * q, 128), q)]

    weights = (gate_ref, up_ref, down_ref)
    homes = (w1.at[0, zl, y, core], w1.at[1, zl, y, core], w2.at[z, y, core])
    loads = []
    for t in range(3):
        loads.append((
            pltpu.make_async_copy(columns(weights[t], 1 - y), stage.at[t], load_sem.at[t]),
            pltpu.make_async_copy(columns(weights[t], y), homes[t], load_sem.at[t]),
        ))

    def loaded(t):
        pltpu.make_async_copy(w1.at[0, 0, 0], w1.at[0, 0, 0], load_sem.at[t]).wait()

    def tok_load(i):
        column = (1 - half) * span + ha * sub + i if i < sub else half * span + i - sub
        return pltpu.make_async_copy(
            tok_ref.at[:, pl.ds(pl.multiple_of(column * group, 128), group)], tok_buf.at[i], tok_sem.at[i]
        )

    routing = [
        pltpu.make_async_copy(ref, buf, route_sem.at[k])
        for k, (ref, buf) in enumerate(((ids_ref, ids), (keep_ref, keep), (route_ref, weight)))
    ]
    for copy in (*loads[0], *routing):
        copy.start()
    for i in range(sub):
        tok_load(i).start()
    for load in (*loads[1], *loads[2]):
        load.start()
    for i in range(sub, sub + span):
        tok_load(i).start()

    barrier = pltpu.get_barrier_semaphore()

    @pl.loop(1, n)
    def _(k):
        pl.semaphore_signal(barrier, inc=1, device_id={"wa": lax.rem(me + k, n)}, device_id_type=MESH)

    pl.semaphore_signal(barrier, inc=1, device_id={"ha": 1 - ha}, device_id_type=MESH)

    pl.semaphore_wait(barrier, n)

    def direct(ref, yy, sems, k, **where):
        return same(ref.at[pl.ds(ha * sub, sub), yy], sems[0], sems[1].at[k], **where)

    def other(ref, yy, sems, k, **where):
        return same(ref.at[pl.ds((1 - ha) * sub, sub), yy], sems[0], sems[1].at[k], **where)

    g_sems = (g_send, g_recv)
    to_x = {"ha": 1 - ha}
    to_y = {"wa": beside}
    guest_send = remote(guest_out, guest_rows.at[pl.ds(ha * sub, sub), y], g_send, g_recv.at[0], wa=mirror)
    guest_y, guest_y_got = direct(guest_rows, y, g_sems, 1, **to_y), direct(guest_rows, 1 - y, g_sems, 1, **to_y)
    guest_x, guest_x_got = direct(guest_rows, y, g_sems, 2, **to_x), other(guest_rows, y, g_sems, 2, **to_x)
    guest_d, guest_d_got = direct(guest_rows, 1 - y, g_sems, 3, **to_x), other(guest_rows, 1 - y, g_sems, 3, **to_x)
    own_y, own_y_got = direct(own_rows, y, g_sems, 4, **to_y), direct(own_rows, 1 - y, g_sems, 4, **to_y)
    own_d, own_d_got = direct(own_rows, 1 - y, g_sems, 5, **to_x), other(own_rows, 1 - y, g_sems, 5, **to_x)

    def given_all(t, e):
        zi = order(e, zl, span)
        same(w1.at[t, zi, :, 1 - core], b1_send, b1_recv.at[t, zi], wa=sibling).wait_recv()

    def line2_in(e):
        zi = order(e, z, zs)
        for yy in (0, 1):
            second.serve(0, zi, yy)

    def project(rows, e, t):
        zi = order(e, zl, span)
        return jnp.dot(rows(zi), w1[t, zi].reshape(group, q), preferred_element_type=jnp.float32)

    def guests(yy):
        return lambda zi: guest_rows[zi, yy]

    def mine(zi):
        return own_rows[zi].reshape(2 * CAP, group)

    def partial(yy, t):
        return remote(part_out.at[yy, t], part_in.at[yy, t], p_send, p_recv.at[yy, t], wa=mirror)

    def serve_guest(yy, t):
        total = None
        for e in range(span):
            term = project(guests(yy), e, t)
            total = term if total is None else total + term
        part_out[yy, t] = total.astype(jnp.bfloat16)
        partial(yy, t).start()

    loaded(0)
    exchange(0).start()
    first.spread(0, zl, y)
    for copy in routing:
        copy.wait()
    matches = (ids[...] == 0) & (keep[...] == 1)
    chosen = jnp.minimum(jnp.sum(jnp.where(matches, 1, 0), axis=0, keepdims=True), 1)
    route_sum = jnp.sum(jnp.where(matches, weight[...], jnp.float32(0.0)), axis=0, keepdims=True)
    length = chosen.shape[1]
    lane = lax.broadcasted_iota(jnp.int32, (8, length), 1)
    running = jnp.broadcast_to(chosen, (8, length))
    shift = 1
    while shift < length:
        running = running + jnp.where(lane >= shift, pltpu.roll(running, shift, 1), 0)
        shift *= 2
    place = jnp.where(chosen == 1, running[0:1] - 1, -1)
    count[...] = jnp.broadcast_to(jnp.sum(chosen, axis=1, keepdims=True), count.shape)
    slot_ids = lax.broadcasted_iota(jnp.int32, (CAP, length), 0)
    hit = place == slot_ids
    table = jnp.where(hit, jnp.float32(1.0), jnp.float32(0.0)).astype(jnp.bfloat16)
    for i in range(sub):
        tok_load(i).wait()
        guest_out[i] = jnp.dot(table, tok_buf[i], preferred_element_type=jnp.float32).astype(jnp.bfloat16)
    guest_send.start()
    loaded(1)
    exchange(1).start()
    first.spread(1, zl, y)
    loaded(2)
    exchange(2).start()
    slot_route = jnp.sum(jnp.where(hit, route_sum, jnp.float32(0.0)), axis=1, keepdims=True)
    route[...] = jnp.broadcast_to(slot_route, route.shape)
    for i in range(span):
        tok_load(sub + i).wait()
        own_rows[i, y] = jnp.dot(
            table, tok_buf[sub + i], preferred_element_type=jnp.float32
        ).astype(jnp.bfloat16)

    pick_ref[...] = table.T

    @pl.loop(1, n)
    def _(k):
        count_copy(k).start()

    for t in (0, 1):
        first.serve(t, zl, 1 - y)
    second.spread(0, z, y)
    guest_send.wait_recv()
    guest_y.start()
    guest_x.start()
    own_y.start()
    second.serve(0, z, 1 - y)
    for t in (0, 1):
        given_all(t, 0)
    guest_y_got.wait_recv()
    guest_d.start()
    guest_x_got.wait_recv()
    for e in range(1, span):
        zi = order(e, zl, span)
        for t in (0, 1):
            first.serve(t, zi, y)
        first.serve(0, zi, 1 - y)
        given_all(0, e)
    serve_guest(y, 0)
    for e in range(1, span):
        first.serve(1, order(e, zl, span), 1 - y)
        given_all(1, e)
    serve_guest(y, 1)
    middle = (z > 0) & (z + 1 < zs)

    @pl.when(middle)
    def _():
        line2_in(1)

    own_y_got.wait_recv()
    own_d.start()
    guest_d_got.wait_recv()
    for t in (0, 1):
        serve_guest(1 - y, t)

    @pl.when(jnp.logical_not(middle))
    def _():
        line2_in(1)

    @pl.when(middle)
    def _():
        @pl.loop(2, span + 1)
        def _(e):
            line2_in(e)

    own_d_got.wait_recv()
    for t in (0, 1):
        total = project(mine, 0, t)
        for e in range(1, span):
            total = total + project(mine, e, t)
        own_acc[t] = total
    for yy in (0, 1):
        for t in (0, 1):
            partial(yy, t).wait_recv()
    for yy in (0, 1):
        gate = own_acc[0, yy * CAP:(yy + 1) * CAP] + part_in[yy, 0].astype(jnp.float32)
        up = own_acc[1, yy * CAP:(yy + 1) * CAP] + part_in[yy, 1].astype(jnp.float32)
        hidden[yy] = (gate / (1.0 + jnp.exp(-gate)) * up).astype(jnp.bfloat16)

    def swap_x(j, yy):
        return remote(x_out.at[yy, j], x_in.at[yy, j], y_send, x_recv.at[yy, j], ha=1 - ha)

    def swap_y(zi, yy):
        return remote(y_out.at[yy, zi], y_in.at[yy, zi], y_send, y_recv.at[yy, zi], wa=beside)

    def swap_part(zi, yy, c):
        return remote(y_out.at[yy, zi, c], y_in.at[yy, zi, c], y_send, part_recv.at[0, yy, c], wa=beside)

    def swap_part_x(j, yy, c):
        return remote(
            yx_out.at[yy, j, c], yx_in.at[yy, j, c], y_send, part_recv.at[1, yy, c], ha=1 - ha
        )

    def swap_xy(j, yy):
        return remote(xy_out.at[yy, j], xy_in.at[yy, j], y_send, xy_recv.at[yy, j], wa=beside)

    def swap_yx(j, yy):
        return remote(yx_out.at[yy, j], yx_in.at[yy, j], y_send, yx_recv.at[yy, j], ha=1 - ha)

    def mine_rows(v):
        return jnp.where(y == 0, v[:CAP], v[CAP:]), jnp.where(y == 0, v[CAP:], v[:CAP])

    def down(zi, yy):
        return lax.dot_general(
            hidden[...].reshape(2 * CAP, q), w2[zi, yy].reshape(2 * fd, q), (((1,), (1,)), ((), ())),
            preferred_element_type=jnp.float32,
        )

    def place_of(e):
        zi = order(e, z, zs)
        out = zi // span
        return zi, out, zi - out * span

    def finish_x(e, yy):
        zi, out, j = place_of(e)
        second.given(0, zi, yy).wait_recv()
        part = down(zi, yy)

        @pl.when(out == ha)
        def _():
            x_own[yy, j] = part

        @pl.when(out != ha)
        def _():
            x_out[yy, j] = part.astype(jnp.bfloat16)
            swap_x(j, yy).start()

    def finish_y(e, yy):
        zi, out, j = place_of(e)
        second.given(0, zi, yy).wait_recv()
        keep, leave = mine_rows(down(zi, yy))
        for c in (0, 1):
            y_out[yy, zi, c] = leave[:, c * fd:(c + 1) * fd].astype(jnp.bfloat16)
        swap_y(zi, yy).start()
        for c in (0, 1):
            y_own[yy, zi, c] = keep[:, c * fd:(c + 1) * fd]

    def combine_x(e, yy):
        zi, out, j = place_of(e)

        @pl.when(out == ha)
        def _():
            swap_x(j, yy).wait_recv()
            keep, leave = mine_rows(x_own[yy, j] + x_in[yy, j].astype(jnp.float32))
            xy_own[yy, j] = keep
            xy_out[yy, j] = leave.astype(jnp.bfloat16)
            swap_xy(j, yy).start()

    def combine_y(e, yy):
        zi, out, j = place_of(e)
        swap_y(zi, yy).wait_recv()
        total = y_own[yy, zi] + y_in[yy, zi].astype(jnp.float32)

        @pl.when(out != ha)
        def _():
            yx_out[yy, j] = total.astype(jnp.bfloat16)
            swap_yx(j, yy).start()

        @pl.when(out == ha)
        def _():
            y_own[yy, zi] = total

    def part_last(yy, c):
        zi, out, j = place_of(zs - 1)
        keep, leave = mine_rows(lax.dot_general(
            hidden[...].reshape(2 * CAP, q), w2[zi, yy, c], (((1,), (1,)), ((), ())),
            preferred_element_type=jnp.float32,
        ))
        y_out[yy, zi, c] = leave.astype(jnp.bfloat16)
        swap_part(zi, yy, c).start()
        y_own[yy, zi, c] = keep

    def start_last(yy):
        second.serve(0, order(zs - 1, z, zs), yy)
        part_last(yy, core)

    def end_last(yy):
        second.given(0, order(zs - 1, z, zs), yy).wait_recv()
        part_last(yy, 1 - core)

    def combine_last(yy):
        zi, out, j = place_of(zs - 1)
        for c in (core, 1 - core):
            swap_part(zi, yy, c).wait_recv()
            total = y_own[yy, zi, c] + y_in[yy, zi, c].astype(jnp.float32)

            @pl.when(out != ha)
            def _():
                yx_out[yy, j, c] = total.astype(jnp.bfloat16)
                swap_part_x(j, yy, c).start()

            @pl.when(out == ha)
            def _():
                y_own[yy, zi, c] = total

    def late(e, yy):
        second.serve(0, order(e, z, zs), yy)
        finish_y(e, yy)

    @pl.when(middle)
    def _():
        @pl.loop(0, span + 1)
        def _(e):
            finish_x(e, 0)
            finish_y(e, 1)

        @pl.loop(span + 1, zs - 1)
        def _(e):
            late(e, 0)
            late(e, 1)

        start_last(0)
        end_last(0)
        start_last(1)
        end_last(1)

        @pl.loop(0, span + 1)
        def _(e):
            combine_y(e, 1)
            combine_x(e, 0)

        @pl.loop(span + 1, zs - 1)
        def _(e):
            combine_y(e, 0)
            combine_y(e, 1)

        combine_last(0)
        combine_last(1)

    @pl.when(jnp.logical_not(middle))
    def _():
        finish_y(0, 1)
        finish_x(0, 0)
        finish_y(1, 0)
        finish_y(1, 1)
        second.serve(0, order(2, z, zs), 0)
        finish_x(2, 0)
        late(2, 1)
        combine_y(0, 1)
        combine_y(1, 0)

        @pl.loop(3, zs - 1)
        def _(e):
            late(e, 0)
            late(e, 1)
            combine_y(e, 0)
            combine_y(e, 1)

        start_last(0)
        combine_y(1, 1)
        end_last(0)
        combine_x(2, 0)
        combine_y(2, 1)
        start_last(1)
        end_last(1)
        combine_x(0, 0)
        combine_last(0)
        combine_last(1)

    all_counts().wait_recv()

    counts[me] = jnp.zeros(counts.shape[1:], jnp.int32)

    def add_count(i, total):
        return total + jnp.where(i < me, counts[i], 0)

    earlier = lax.fori_loop(0, n, add_count, jnp.zeros(counts.shape[1:], jnp.int32))
    slot = lax.broadcasted_iota(jnp.int32, (CAP, 1), 0)
    scale = jnp.where(slot + earlier[0:1, 0:1] < n // 2 * CAP, route[:, 0:1], jnp.float32(0.0))
    def put(u, total):
        y_ref[:, u * wide:(u + 1) * wide] = (total * scale).astype(jnp.bfloat16)

    def put_y(u, zi, yy, j):
        for c in (0, 1):
            total = y_own[yy, zi, c] + yx_in[yy, j, c].astype(jnp.float32)
            y_ref[:, u * wide + c * fd:u * wide + (c + 1) * fd] = (total * scale).astype(jnp.bfloat16)

    for yy in (1, 0):
        for j in range(span):
            zi = ha * span + j
            u = 2 * j + yy
            final = rank_of(zi, z, zs) == zs - 1
            split = y_first(zi, yy)

            @pl.when(final)
            def _():
                for c in (core, 1 - core):
                    swap_part_x(j, yy, c).wait_recv()

            @pl.when(split & jnp.logical_not(final))
            def _():
                swap_yx(j, yy).wait_recv()

            @pl.when(split)
            def _():
                put_y(u, zi, yy, j)

            @pl.when(jnp.logical_not(split))
            def _():
                swap_xy(j, yy).wait_recv()
                put(u, xy_own[yy, j] + xy_in[yy, j].astype(jnp.float32))

    all_counts().wait_send()

    settle(e_send, 3 * fd * q)
    settle(g_send, 6 * sub * CAP * group)
    settle(p_send, 4 * CAP * q)
    first.drain(2)
    second.drain(1)

    unit = CAP * wide

    @pl.when(middle)
    def _():
        settle(y_send, (2 * span + span + 1 + 2 * zs - 1 - span) * unit)

    @pl.when(jnp.logical_not(middle))
    def _():
        settle(y_send, (2 * span + 2 * zs) * unit)


def expert(ids, keep, weight, tokens, gate, up, down):
    n = lax.axis_size("wa")
    fd, hid = gate.shape
    q = hid // 2
    zs = n // 4
    span = zs // 2
    sub = span // 2
    group = 4 * fd
    wide = 2 * fd
    any_spec = pl.BlockSpec(memory_space=pl.ANY)
    vmem = pl.BlockSpec(memory_space=pltpu.VMEM)
    dma = pltpu.SemaphoreType.DMA
    bf16, f32 = jnp.bfloat16, jnp.float32
    return pl.pallas_call(
        functools.partial(expert_kernel, n),
        out_shape=(
            pltpu.VMEM((CAP, span * group), bf16), pltpu.VMEM((tokens.shape[0], CAP), bf16)
        ),
        in_specs=[any_spec] * 7,
        out_specs=(vmem, vmem),
        scratch_shapes=[
            pltpu.VMEM(ids.shape, jnp.int32),
            pltpu.VMEM(ids.shape, jnp.int32),
            pltpu.VMEM(ids.shape, f32),
            pltpu.VMEM((2, span, 2, 2, fd, q), bf16),
            pltpu.VMEM((zs, 2, 2, fd, q), bf16),
            pltpu.VMEM((3, fd, q), bf16),
            pltpu.VMEM((sub + span, tokens.shape[0], group), bf16),
            pltpu.VMEM((sub, CAP, group), bf16),
            pltpu.VMEM((span, 2, CAP, group), bf16),
            pltpu.VMEM((span, 2, CAP, group), bf16),
            pltpu.VMEM((2, 2 * CAP, q), f32),
            pltpu.VMEM((2, 2, CAP, q), bf16),
            pltpu.VMEM((2, 2, CAP, q), bf16),
            pltpu.VMEM((2, CAP, q), bf16),
            pltpu.VMEM((2, span, 2 * CAP, wide), f32),
            pltpu.VMEM((2, span, 2 * CAP, wide), bf16),
            pltpu.VMEM((2, span, 2 * CAP, wide), bf16),
            pltpu.VMEM((2, zs, 2, CAP, fd), f32),
            pltpu.VMEM((2, zs, 2, CAP, fd), bf16),
            pltpu.VMEM((2, zs, 2, CAP, fd), bf16),
            pltpu.VMEM((2, span, CAP, wide), f32),
            pltpu.VMEM((2, span, CAP, wide), bf16),
            pltpu.VMEM((2, span, CAP, wide), bf16),
            pltpu.VMEM((2, span, 2, CAP, fd), bf16),
            pltpu.VMEM((2, span, 2, CAP, fd), bf16),
            pltpu.VMEM((8, 128), jnp.int32),
            pltpu.VMEM((n, 8, 128), jnp.int32),
            pltpu.VMEM((CAP, 128), f32),
            dma((3,)), dma((sub + span,)), dma((2,)), dma,
            dma, dma((2, span, 2)), dma, dma((2, span)),
            dma, dma((1, zs, 2)), dma, dma((zs, 2)),
            dma, dma((6,)), dma, dma((2, 2)),
            dma((2, span)), dma, dma((2, zs)), dma((2, span)), dma((2, span)), dma((2, 2, 2)), dma((3,)),
        ],
        compiler_params=pltpu.CompilerParams(
            collective_id=0, has_side_effects=True, vmem_limit_bytes=60 * 1024 * 1024
        ),
    )(ids, keep, weight, tokens, gate, up, down)


def combine_kernel(pick_ref, y_ref, out_ref, block, out_sem):
    steps, tall, width = block.shape
    wide = 512 if width % 512 == 0 else width
    stores = []
    for i in range(steps):
        for k in range(0, width, wide):
            block[i, :, k:k + wide] = jnp.dot(
                pick_ref[i * tall:(i + 1) * tall], y_ref[:, k:k + wide], preferred_element_type=jnp.float32
            ).astype(jnp.bfloat16)
        stores.append(pltpu.make_async_copy(block.at[i], out_ref.at[i * tall:(i + 1) * tall], out_sem.at[i]))
        stores[i].start()
    for store in stores:
        store.wait()


def combine(pick, y):
    tokens, width = pick.shape[0], y.shape[1]
    tall = CAP if tokens % CAP == 0 else tokens
    steps = tokens // tall
    vmem = pl.BlockSpec(memory_space=pltpu.VMEM)
    return pl.pallas_call(
        combine_kernel,
        out_shape=jax.ShapeDtypeStruct((tokens, width), jnp.bfloat16),
        in_specs=[vmem, vmem],
        out_specs=pl.BlockSpec(memory_space=pl.ANY),
        scratch_shapes=[pltpu.VMEM((steps, tall, width), jnp.bfloat16), pltpu.SemaphoreType.DMA((steps,))],
        compiler_params=pltpu.CompilerParams(vmem_limit_bytes=32 * 1024 * 1024),
    )(pick, y)


def per_device(tokens, expert_ids, keep_mask, route_weight, gate_weight, up_weight, down_weight):
    y, pick = expert(expert_ids.T, keep_mask.T, route_weight.T, tokens, gate_weight, up_weight, down_weight)
    return combine(pick, y)


def solution(mesh):
    return jax.shard_map(
        per_device,
        mesh=mesh,
        in_specs=(
            P("wa", None),
            P("wa", None),
            P("wa", None),
            P("wa", None),
            P("wa", "ha"),
            P("wa", "ha"),
            P("wa", "ha"),
        ),
        out_specs=P("wa", "ha"),
        check_vma=False,
    )
```
